256 devices in a mesh: rep: 1, dp: 256 (over x, y, z, core).
Axes of the slice: x: 4, y: 4, z: 8, core: 2. Of those that a mesh axis runs over, the one named last changes fastest.
Arguments:
- x: bfloat16 [256, 1024, 1024], P(('rep', 'dp'))
- dy: bfloat16 [256, 1024, 1024], P(('rep', 'dp'))
- w_gate: bfloat16 [2, 1024, 2560], replicated
- w_up: bfloat16 [2, 1024, 2560], replicated
- w_down: bfloat16 [2, 2560, 1024], replicated
- m_w_gate: float32 [2, 1024, 2560], P(None, 'dp')
- m_w_up: float32 [2, 1024, 2560], P(None, 'dp')
- m_w_down: float32 [2, 2560, 1024], P(None, 'dp')
- v_w_gate: float32 [2, 1024, 2560], P(None, 'dp')
- v_w_up: float32 [2, 1024, 2560], P(None, 'dp')
- v_w_down: float32 [2, 2560, 1024], P(None, 'dp')
Outputs:
- output 1: bfloat16 [2, 1024, 2560], P('rep')
- output 2: bfloat16 [2, 1024, 2560], P('rep')
- output 3: bfloat16 [2, 2560, 1024], P('rep')
- output 4: float32 [2, 1024, 2560], P('rep', 'dp')
- output 5: float32 [2, 1024, 2560], P('rep', 'dp')
- output 6: float32 [2, 2560, 1024], P('rep', 'dp')
- output 7: float32 [2, 1024, 2560], P('rep', 'dp')
- output 8: float32 [2, 1024, 2560], P('rep', 'dp')
- output 9: float32 [2, 2560, 1024], P('rep', 'dp')
All inputs are finite; a program needn't handle non-finite values.
Results may differ from the reference program's by a relative error of at most 0.022.
Values are sent between devices in bfloat16 or wider.
A program may use at most 768 MiB of HBM per device.

```python
import jax
import jax.numpy as jnp
from jax import lax

SEQUENCES = 256
TOKENS = 1024
D = 1024
FF = 2560
LAYERS = 2
NAMES = ("w_gate", "w_up", "w_down")
SHAPES = {"w_gate": (LAYERS, D, FF), "w_up": (LAYERS, D, FF), "w_down": (LAYERS, FF, D)}


def bump(key, n, height):
    away = (jnp.arange(n, dtype=jnp.int32) - jax.random.randint(key, (), 0, n, jnp.int32)) % n
    return jnp.where(away < n // 8, height, 1.0)


def together(key, own, strength):
    shared = jax.random.normal(key, own.shape[1:], jnp.float32)
    return (own + strength * shared) * lax.rsqrt(1 + strength * strength)


def setup_inputs(seed: int = 0, part: int = 0) -> dict:
    kx, kdy, ka, kb, kz, kf, kh, kl, *keys = jax.random.split(jax.random.key(seed), 8 + 3 * len(NAMES))
    kx, kdy, ka, kb = (jax.random.fold_in(k, part) for k in (kx, kdy, ka, kb))
    kw, km, kv = (keys[i::3] for i in range(3))
    shape = (SEQUENCES, TOKENS, D)
    much_x, much_dy = jax.random.uniform(kz, (2,), jnp.float32, 0.0, 1.0)
    loud = 2.0 ** jax.random.uniform(jax.random.fold_in(kz, 1), (), jnp.float32, -1.0, 2.0)
    layers = 2.0 ** jax.random.uniform(kl, (LAYERS, 1, 1), jnp.float32, -1.0, 1.0)
    x = together(ka, jax.random.normal(kx, shape, jnp.float32), much_x) * bump(kf, D, 4.0)
    dy = together(kb, jax.random.normal(kdy, shape, jnp.float32), much_dy)
    drawn = {"x": x.astype(jnp.bfloat16), "dy": (loud * dy * (SEQUENCES * TOKENS) ** -0.5).astype(jnp.bfloat16)}
    for key, name in zip(kw, NAMES, strict=True):
        w = jax.random.normal(key, SHAPES[name], jnp.float32) * SHAPES[name][1] ** -0.5
        drawn[name] = (w * {"w_gate": 1.0, "w_up": bump(kh, FF, 4.0), "w_down": layers}[name]).astype(jnp.bfloat16)
    for key, name in zip(km, NAMES, strict=True):
        drawn[f"m_{name}"] = 0.1 * jax.random.normal(key, SHAPES[name], jnp.float32)
    for key, name in zip(kv, NAMES, strict=True):
        drawn[f"v_{name}"] = loud * loud * jax.random.uniform(key, SHAPES[name], jnp.float32, 0.05, 0.15)
    return drawn


def matmul(a, w):
    return jnp.dot(a, w, preferred_element_type=jnp.float32).astype(jnp.bfloat16)


def normed(h):
    wide = h.astype(jnp.float32)
    scale = lax.rsqrt(jnp.mean(wide**2, -1, keepdims=True) + 1e-6)
    return (wide * scale).astype(jnp.bfloat16)


def layer(h, w):
    a = normed(h)
    gate = jnp.dot(a, w["w_gate"], preferred_element_type=jnp.float32)
    up = jnp.dot(a, w["w_up"], preferred_element_type=jnp.float32)
    return h + matmul((jax.nn.silu(gate) * up).astype(jnp.bfloat16), w["w_down"])


def adamw(w, m, v, g):
    m = 0.9 * m + 0.1 * g
    v = 0.95 * v + 0.05 * g * g
    step = m * lax.rsqrt(v + 1e-8) + 0.1 * w
    return (w - 0.02 * step).astype(jnp.bfloat16), m, v


def stack(weights, h):
    return lax.scan(lambda h, w: (layer(h, w), None), h, weights)[0]


def reference(x, dy, w_gate, w_up, w_down, m_w_gate, m_w_up, m_w_down, v_w_gate, v_w_up, v_w_down):
    weights = dict(zip(NAMES, (w_gate, w_up, w_down), strict=True))

    def take(so_far, sequence):
        h, by_y = sequence
        _, back = jax.vjp(lambda w: stack(w, h), weights)
        return jax.tree.map(lambda total, term: total + term.astype(jnp.float32), so_far, back(by_y)[0]), None

    none_yet = {name: jnp.zeros(w.shape, jnp.float32) for name, w in weights.items()}
    by_weights, _ = lax.scan(take, none_yet, (x, dy))
    gradients = [by_weights[name].astype(jnp.bfloat16).astype(jnp.float32) for name in NAMES]
    new = [
        adamw(w.astype(jnp.float32), m, v, g)
        for w, m, v, g in zip((w_gate, w_up, w_down), (m_w_gate, m_w_up, m_w_down), (v_w_gate, v_w_up, v_w_down), gradients, strict=True)
    ]
    return tuple(one[which] for which in range(3) for one in new)
```

```python
import functools

import jax
import jax.numpy as jnp
from jax import lax
from jax.experimental import pallas as pl
from jax.experimental.pallas import tpu as pltpu
from jax.sharding import PartitionSpec as P

NAMES = ("w_gate", "w_up", "w_down")
MESH = pl.DeviceIdType.MESH
F32, BF16 = jnp.float32, jnp.bfloat16
SIZES = {"x": 4, "y": 4, "z": 8}
VMEM_LIMIT = 64 * 1024 * 1024 - 64 * 1024


RING, DIRECT = "ring", "direct"
COLOURS = (
    (("x", RING), ("y", RING), ("z", DIRECT)),
    (("y", RING), ("x", RING), ("z", DIRECT)),
    (("z", RING), ("x", DIRECT), ("y", DIRECT)),
)
WIDE, TALL = "wide", "tall"
PART = {WIDE: ((0, 384), (384, 384), (768, 512)), TALL: ((0, 16), (16, 16), (32, 8))}
HALF = {WIDE: 1280, TALL: 512}
ROWS = {WIDE: 8, TALL: 40}
ORDER = ((TALL, 1), (WIDE, 1), (WIDE, 3), (TALL, 0), (WIDE, 0), (WIDE, 2))


class Me:
    def __init__(self):
        index = lax.axis_index("dp")
        self.core = lax.rem(index, 2)
        chip = index // 2
        self.at = {
            "z": lax.rem(chip, SIZES["z"]),
            "y": lax.rem(chip // SIZES["z"], SIZES["y"]),
            "x": chip // (SIZES["z"] * SIZES["y"]),
        }
        self.sign = 1 - 2 * self.core

    def off(self, d, by):
        return lax.rem(self.at[d] + by + SIZES[d], SIZES[d])

    def device(self, core=None, **at):
        at = {**self.at, **at}
        core = self.core if core is None else core
        return (0, ((at["x"] * SIZES["y"] + at["y"]) * SIZES["z"] + at["z"]) * 2 + core)

    def barrier(self):
        sem = pltpu.get_barrier_semaphore()

        def signal(peer):
            pl.semaphore_signal(sem, inc=1, device_id=peer, device_id_type=MESH)

        for d, n in SIZES.items():
            each(n - 1, lambda i, d=d: signal(self.device(**{d: self.off(d, i + 1)})))
        signal(self.device(core=1 - self.core))
        signal(self.device(core=1 - self.core, z=self.pair()))
        pl.semaphore_wait(sem, sum(SIZES.values()) - 1)

    def pair(self):
        return self.at["z"] + 1 - 2 * lax.rem(self.at["z"], 2)


def dims(kind, free):
    return tuple(SIZES[d] // (2 if kind == TALL and d == "z" else 1) for d in free)


def view(ref, kind, free, fixed, colour=None, base=0, own=False):
    index = [(fixed[d] // 2 if kind == TALL and d == "z" else fixed[d]) if d in fixed else slice(None) for d in free]
    if own and not (kind == TALL and "z" in free and "z" in fixed):
        return ref.at[(*index, slice(None), slice(None))]
    if kind == WIDE:
        first, size = (0, HALF[WIDE]) if colour is None else PART[WIDE][colour]
        rows, columns = slice(None), pl.ds(_at(base, first), size)
    else:
        rows = slice(None) if own or colour is None else pl.ds(*PART[TALL][colour])
        if "z" in free and "z" in fixed:
            columns = pl.ds(pl.multiple_of(base + lax.rem(fixed["z"], 2) * 256, 256), 256)
        else:
            columns = pl.ds(_at(base, 0), HALF[TALL])
    return ref.at[(*index, rows, columns)]


def _at(base, first):
    return first if isinstance(base, int) and base == 0 else pl.multiple_of(base + first, 128)


def block(kind, colour, free):
    first, size = PART[kind][colour]
    tail = (8, size) if kind == WIDE else (size, HALF[TALL] if "z" in free else HALF[TALL] // 2)
    return dims(kind, free) + tail


def lengths(n):
    return n // 2, (n - 1) // 2


def reduce_buffers(kind):
    shapes = {}
    for c, phases in enumerate(COLOURS):
        free = ["x", "y", "z"]
        for p, (d, how) in enumerate(phases):
            free.remove(d)
            shape = block(kind, c, tuple(free))
            count = SIZES[d] - 1
            shapes[c, p] = (count, *shape)
    return shapes


class Copies:
    def __init__(self, send, recv):
        self.send, self.recv, self.all, self.used = send, recv, {}, 0

    def start(self, key, src, dst, to):
        self.start_all(key, 1, lambda i: (src, dst, to))

    def start_all(self, key, count, make):
        first = self.used
        self.used += count

        def copy(i):
            src, dst, to = make(i)
            return pltpu.make_async_remote_copy(
                src_ref=src, dst_ref=dst, send_sem=self.send.at[first + i], recv_sem=self.recv.at[first + i], device_id=to, device_id_type=MESH
            )

        self.all[key] = count, copy
        each(count, lambda i: copy(i).start())

    def arrived(self, key):
        count, copy = self.all[key]
        each(count, lambda i: copy(i).wait_recv())

    def sent(self):
        for count, copy in self.all.values():
            each(count, lambda i, copy=copy: copy(i).wait_send())


def each(count, do):
    if count == 1:
        do(0)
    else:

        @pl.loop(0, count)
        def _(i):
            do(i)


def total(parts):
    return functools.reduce(jnp.add, [p[...].astype(F32) for p in parts])


def reduce_colour(me, copies, key, kind, colour, grads, received, last):
    free, fixed = ("x", "y", "z"), {}
    parts = [lambda at, r=r: view(r, kind, ("x", "y", "z"), at, colour) for r in grads]
    out = parts[0]

    def add(at, more):
        rest = [d for d in free if d not in at]
        if len(rest) >= 2:
            first = rest[0]

            @pl.loop(0, SIZES[first])
            def _(i):
                now = {**at, first: i}
                out(now)[...] = total([p(now) for p in parts + more]).astype(BF16)
        else:
            out(at)[...] = total([p(at) for p in parts + more]).astype(BF16)

    for phase, (d, how) in enumerate(COLOURS[colour]):
        n, buffer = SIZES[d], received(colour, phase)
        left = tuple(e for e in ("x", "y", "z") if e not in fixed and e != d)

        def slot(i, buffer=buffer, left=left):
            return lambda at: view(buffer.at[i], kind, left, {e: v for e, v in at.items() if e in left}, colour, own=True)

        if how == RING:
            long, short = lengths(n)
            ways = ((me.sign, long, 0, "l"), (-me.sign, short, long, "s"))
            for s in range(long):
                for sign, length, base, name in ways:
                    if s >= length:
                        continue
                    to = me.off(d, sign * (length - s))
                    at = {**fixed, d: to}
                    if s:
                        copies.arrived((key, colour, phase, name, s - 1))
                    add(at, [slot(base + s - 1)] if s else [])
                    copies.start(
                        (key, colour, phase, name, s), out(at), buffer.at[base + s], me.device(**{d: me.off(d, sign)})
                    )
                yield
            for sign, length, base, name in ways:
                if length:
                    copies.arrived((key, colour, phase, name, length - 1))
            parts = parts + [slot(base + length - 1) for sign, length, base, name in ways if length]
        else:

            def make(i, d=d, fixed=fixed, buffer=buffer, add=add, out=out):
                to = me.off(d, i + 1)
                return out({**fixed, d: to}), buffer.at[i], me.device(**{d: to})

            each(n - 1, lambda i: add({**fixed, d: me.off(d, i + 1)}, []))
            copies.start_all((key, colour, phase), n - 1, make)
            yield
            copies.arrived((key, colour, phase))
            parts = parts + [slot(i) for i in range(n - 1)]
        fixed = {**fixed, d: me.at[d]}
    last(colour, total([p(fixed) for p in parts]).astype(BF16).astype(F32))


def reduce_kernel(*refs):
    ins, outs, rest = refs[:6], refs[6:8], list(refs[8:])
    own = {WIDE: rest[0], TALL: rest[1]}
    other = {WIDE: rest[2], TALL: rest[3]}
    sums = {WIDE: rest[4], TALL: rest[5]}
    cross = {WIDE: rest[6], TALL: rest[7]}
    shares = rest[8]
    load, send, recv = rest[9:12]
    bufs = {}
    for kind in (WIDE, TALL):
        for k in reduce_buffers(kind):
            bufs[kind, k] = rest[12 + len(bufs)]
    me = Me()
    me.barrier()
    copies = Copies(send, recv)
    loads = []
    for i, (kind, j) in enumerate(ORDER):
        half = HALF[kind]
        src = ins[i].at[..., pl.ds(pl.multiple_of(me.core * half, 256), half)]
        copy = pltpu.make_async_copy(src, own[kind].at[j], load.at[i])
        copy.start()
        loads.append(copy)
        src = ins[i].at[..., pl.ds(pl.multiple_of((1 - me.core) * half, 256), half)]
        copies.start((i, "half"), src, other[kind].at[j], me.device(core=1 - me.core))

    def colours(i):
        kind, j = ORDER[i]
        loads[i].wait()
        copies.arrived((i, "half"))

        def last(colour, value):
            first, size = PART[kind][colour]
            if kind == WIDE:
                sums[WIDE][j, 0, :, first : first + size] = value[:4]
                sums[WIDE][j, 1, :, first : first + size] = value[4:]
            else:
                sums[TALL][j, first : first + size, :] = value

        gens = [
            reduce_colour(me, copies, i, kind, c, (own[kind].at[j], other[kind].at[j]), lambda c, p: bufs[kind, (c, p)].at[j], last)
            for c in range(3)
        ]
        while gens:
            gens = [g for g in gens if next(g, 0) is None]
            yield
        if kind == WIDE:
            copies.start((i, "rows"), sums[WIDE].at[j, 1 - me.core], cross[WIDE].at[j], me.device(core=1 - me.core))
        else:
            for q in range(4):
                shares[j, q] = sums[TALL][j, 10 * q : 10 * q + 10, :]
            b = lax.rem(me.at["z"], 2)
            mine = 2 * b + me.core
            for o, (z, core) in enumerate(((me.at["z"], 1 - me.core), (me.pair(), me.core), (me.pair(), 1 - me.core))):
                q = 2 * lax.rem(z, 2) + core
                copies.start((i, "rows", o), shares.at[j, q], cross[TALL].at[j, mine], me.device(core=core, z=z))
        yield
        if kind == WIDE:
            copies.arrived((i, "rows"))
            outs[0][j, me.core] = sums[WIDE][j, me.core]
            outs[0][j, 1 - me.core] = cross[WIDE][j]
        else:
            for o in range(3):
                copies.arrived((i, "rows", o))
            for q in range(4):
                outs[1][j, q] = jnp.where(q == mine, shares[j, q], cross[TALL][j, q])

    run([colours(i) for i in range(6)], 3)
    copies.sent()


def run(gens, apart):
    steps = [(i * apart, i, g) for i, g in enumerate(gens)]
    t = 0
    live = set(range(len(gens)))
    while live:
        for start, i, g in steps:
            if i in live and t >= start and next(g, 0) == 0:
                live.discard(i)
        t += 1


def full_shape(kind):
    return dims(kind, ("x", "y", "z")) + (ROWS[kind], HALF[kind])


def reduce_scatter(grads):
    scratch = [
        pltpu.VMEM((4, *full_shape(WIDE)), BF16),
        pltpu.VMEM((2, *full_shape(TALL)), BF16),
        pltpu.VMEM((4, *full_shape(WIDE)), BF16),
        pltpu.VMEM((2, *full_shape(TALL)), BF16),
        pltpu.VMEM((4, 2, 4, 1280), F32),
        pltpu.VMEM((2, 40, 256), F32),
        pltpu.VMEM((4, 4, 1280), F32),
        pltpu.VMEM((2, 4, 10, 256), F32),
        pltpu.VMEM((2, 4, 10, 256), F32),
        pltpu.SemaphoreType.DMA((6,)),
        pltpu.SemaphoreType.DMA((256,)),
        pltpu.SemaphoreType.DMA((256,)),
    ]
    for kind, many in ((WIDE, 4), (TALL, 2)):
        scratch += [pltpu.VMEM((many, *shape), BF16) for shape in reduce_buffers(kind).values()]
    return pl.pallas_call(
        reduce_kernel,
        out_shape=(jax.ShapeDtypeStruct((4, 2, 4, 1280), F32), jax.ShapeDtypeStruct((2, 4, 10, 256), F32)),
        in_specs=[pl.BlockSpec(memory_space=pl.ANY)] * 6,
        out_specs=(pl.BlockSpec(memory_space=pltpu.VMEM), pl.BlockSpec(memory_space=pltpu.VMEM)),
        scratch_shapes=scratch,
        compiler_params=pltpu.CompilerParams(collective_id=0, has_side_effects=True, vmem_limit_bytes=VMEM_LIMIT),
        name="reduce_scatter",
    )(*grads)


def gather_colour(me, copies, key, kind, colour, ref):
    base = me.core * HALF[kind]
    fixed = dict(me.at)

    def part(at):
        return view(ref, kind, ("x", "y", "z"), at, colour, base)

    phases = COLOURS[colour][::-1]
    for phase, (d, how) in enumerate(phases):
        n, lastly = SIZES[d], phase == len(phases) - 1
        rest = {e: v for e, v in fixed.items() if e != d}
        here = part(fixed)

        def across(name, at):
            if lastly:
                copies.start((key, colour, "across", name), part(at), part(at), me.device(core=1 - me.core))

        if how == RING:
            long, short = lengths(n)
            ways = ((me.sign, long, "l"), (-me.sign, short, "s"))
            for s in range(long):
                for sign, length, name in ways:
                    if s >= length:
                        continue
                    at = {**rest, d: me.off(d, -sign * s)}
                    if s:
                        copies.arrived((key, colour, phase, name, s - 1))
                    copies.start((key, colour, phase, name, s), part(at), part(at), me.device(**{d: me.off(d, sign)}))
                    if s:
                        across((name, s - 1), at)
                if s == 0:
                    across("own", fixed)
                yield
            for sign, length, name in ways:
                if length:
                    copies.arrived((key, colour, phase, name, length - 1))
                    across((name, length - 1), {**rest, d: me.off(d, -sign * length)})
        else:
            copies.start_all(
                (key, colour, phase), n - 1, lambda i, d=d, here=here: (here, here, me.device(**{d: me.off(d, i + 1)}))
            )
            yield
            copies.arrived((key, colour, phase))
        fixed = rest
    yield
    names = ["own"]
    d, how = phases[-1]
    long, short = lengths(SIZES[d])
    names += [("l", s) for s in range(long)] + [("s", s) for s in range(short)]
    for name in names:
        copies.arrived((key, colour, "across", name))


def gather_kernel(*refs):
    wide, tall, outs, rest = refs[0], refs[1], refs[2:8], refs[8:]
    cross = {WIDE: rest[0], TALL: rest[1]}
    stage = {WIDE: rest[2], TALL: rest[3]}
    forty, put, send, recv = rest[4:8]
    me = Me()
    me.barrier()
    copies = Copies(send, recv)
    mine = 2 * lax.rem(me.at["z"], 2) + me.core

    for i, (kind, j) in enumerate(ORDER):
        if kind == WIDE:
            copies.start((i, "rows"), wide.at[j, 1 - me.core], cross[WIDE].at[j], me.device(core=1 - me.core))
        else:
            for o, (z, core) in enumerate(((me.at["z"], 1 - me.core), (me.pair(), me.core), (me.pair(), 1 - me.core))):
                q = 2 * lax.rem(z, 2) + core
                copies.start((i, "rows", o), tall.at[j, q], cross[TALL].at[j, mine], me.device(core=core, z=z))

    def colours(i):
        kind, j = ORDER[i]
        if kind == WIDE:
            copies.arrived((i, "rows"))
            own, theirs = wide[j, me.core], cross[WIDE][j]
            first = me.core == 0
            rows = [jnp.where(first, own, theirs), jnp.where(first, theirs, own)]
            stage[WIDE][j] = jnp.concatenate(rows, axis=0).astype(BF16)
        else:
            for o in range(3):
                copies.arrived((i, "rows", o))
            for q in range(4):
                forty[10 * q : 10 * q + 10, :] = jnp.where(q == mine, tall[j, q], cross[TALL][j, q])
            stage[TALL][j] = forty[...].astype(BF16)
        copy = pltpu.make_async_copy(
            stage[kind].at[j], view(outs[i], kind, ("x", "y", "z"), me.at, None, me.core * HALF[kind]), put.at[i]
        )
        copy.start()
        copy.wait()
        gens = [gather_colour(me, copies, i, kind, c, outs[i]) for c in range(3)]
        while gens:
            gens = [g for g in gens if next(g, 0) is None]
            yield

    run([colours(i) for i in range(6)], 3)
    copies.sent()


def all_gather(wide, tall):
    scratch = [
        pltpu.VMEM((4, 4, 1280), F32),
        pltpu.VMEM((2, 4, 10, 256), F32),
        pltpu.VMEM((4, 8, 1280), BF16),
        pltpu.VMEM((2, 40, 256), BF16),
        pltpu.VMEM((40, 256), F32),
        pltpu.SemaphoreType.DMA((6,)),
        pltpu.SemaphoreType.DMA((384,)),
        pltpu.SemaphoreType.DMA((384,)),
    ]
    return pl.pallas_call(
        gather_kernel,
        out_shape=tuple(
            jax.ShapeDtypeStruct((*dims(kind, ("x", "y", "z")), ROWS[kind], 2 * HALF[kind]), BF16) for kind, _ in ORDER
        ),
        in_specs=[pl.BlockSpec(memory_space=pltpu.VMEM)] * 2,
        out_specs=(pl.BlockSpec(memory_space=pl.ANY),) * 6,
        scratch_shapes=scratch,
        compiler_params=pltpu.CompilerParams(collective_id=1, has_side_effects=True),
        name="all_gather",
    )(wide, tall)


def matmul(a, w):
    return jnp.dot(a, w, preferred_element_type=F32).astype(BF16)


def normed(h):
    wide = h.astype(F32)
    scale = lax.rsqrt(jnp.mean(wide**2, -1, keepdims=True) + 1e-6)
    return (wide * scale).astype(BF16)


def layer(h, w):
    a = normed(h)
    gate = jnp.dot(a, w["w_gate"], preferred_element_type=F32)
    up = jnp.dot(a, w["w_up"], preferred_element_type=F32)
    return h + matmul((jax.nn.silu(gate) * up).astype(BF16), w["w_down"])


def adamw(w, m, v, g):
    m = 0.9 * m + 0.1 * g
    v = 0.95 * v + 0.05 * g * g
    step = m * lax.rsqrt(v + 1e-8) + 0.1 * w
    return (w - 0.02 * step).astype(BF16), m, v


def stack(weights, h):
    for w in weights:
        h = layer(h, w)
    return h


def split(g, kind):
    return g.reshape(*dims(kind, ("x", "y", "z")), ROWS[kind], 2 * HALF[kind])


def reduced(grads):
    ordered = []
    for kind, j in ORDER:
        name = "w_down" if kind == TALL else NAMES[j // 2]
        ordered.append(split(grads[j % 2][name], kind))
    wide, tall = reduce_scatter(ordered)
    wide = wide.transpose(0, 2, 1, 3).reshape(2, 2, 4, 2560)
    tall = tall.reshape(2, 2, 2, 10, 256).transpose(0, 3, 2, 1, 4).reshape(2, 10, 1024)
    return wide[0], wide[1], tall


def gathered(gate, up, down):
    wide = jnp.stack([gate, up]).reshape(4, 4, 2, 1280).transpose(0, 2, 1, 3).astype(F32)
    tall = down.reshape(2, 10, 2, 2, 256).transpose(0, 3, 2, 1, 4).reshape(2, 4, 10, 256).astype(F32)
    new = all_gather(wide, tall)
    by = {key: w.reshape(-1, w.shape[-1]) for key, w in zip(ORDER, new, strict=True)}
    return (
        jnp.stack([by[WIDE, 0], by[WIDE, 1]]),
        jnp.stack([by[WIDE, 2], by[WIDE, 3]]),
        jnp.stack([by[TALL, 0], by[TALL, 1]]),
    )


def solution(mesh):
    def step(x, dy, *arrays):
        weights, m, v = (arrays[i : i + 3] for i in (0, 3, 6))
        layers = [{name: w[l] for name, w in zip(NAMES, weights, strict=True)} for l in range(2)]
        _, back = jax.vjp(lambda w: stack(w, x[0]), layers)
        gradients = reduced(back(dy[0])[0])
        index = lax.axis_index("dp")
        news = []
        for w, mm, vv, g in zip(weights, m, v, gradients, strict=True):
            rows = mm.shape[1]
            mine = lax.dynamic_slice_in_dim(w, index * rows, rows, 1)
            news.append(adamw(mine.astype(F32), mm, vv, g))
        new = gathered(*(n[0] for n in news))
        return (*new, *(n[1] for n in news), *(n[2] for n in news))

    batch, whole, rows = P(("rep", "dp")), P(), P(None, "dp")
    return jax.shard_map(
        step,
        mesh=mesh,
        in_specs=(batch, batch, *(whole,) * 3, *(rows,) * 6),
        out_specs=(*(P("rep"),) * 3, *(P("rep", "dp"),) * 6),
        check_vma=False,
    )
```

```python
import functools

import jax
import jax.numpy as jnp
from jax import lax
from jax.experimental import pallas as pl
from jax.experimental.pallas import tpu as pltpu
from jax.sharding import PartitionSpec as P

NAMES = ("w_gate", "w_up", "w_down")
MESH = pl.DeviceIdType.MESH
F32, BF16 = jnp.float32, jnp.bfloat16
SIZES = {"x": 4, "y": 4, "z": 8}
VMEM_LIMIT = 64 * 1024 * 1024 - 64 * 1024

REDUCE_ORDER = "020100021211100201220012210220113210312230120100024232414021522022515012111042323130520001220241402112205110423250115231000230220141204240325110213052201240503000110103123122414232102131224103203240301113425150521321233123335141425040334352435152505353"
GATHER_ORDER = "020100121110222120023231301242412240013202525150004211125210220121002032104211003120300110215241110240203051501200310122321011214240413050520220511201110122001132213140500010414210522102302112203151222032414042525002021231302212323140514230223252414050425241515051"


RING, DIRECT = "ring", "direct"
COLOURS = (
    (("x", RING), ("y", RING), ("z", DIRECT)),
    (("y", RING), ("x", RING), ("z", DIRECT)),
    (("z", RING), ("x", DIRECT), ("y", DIRECT)),
)
WIDE, TALL = "wide", "tall"
PART = {WIDE: ((0, 384), (384, 384), (768, 512)), TALL: ((0, 16), (16, 16), (32, 8))}
HALF = {WIDE: 1280, TALL: 512}
ROWS = {WIDE: 8, TALL: 40}
ORDER = ((TALL, 1), (WIDE, 1), (WIDE, 3), (TALL, 0), (WIDE, 0), (WIDE, 2))


class Me:
    def __init__(self):
        index = lax.axis_index("dp")
        self.core = lax.rem(index, 2)
        chip = index // 2
        self.at = {
            "z": lax.rem(chip, SIZES["z"]),
            "y": lax.rem(chip // SIZES["z"], SIZES["y"]),
            "x": chip // (SIZES["z"] * SIZES["y"]),
        }
        self.sign = 1 - 2 * self.core

    def off(self, d, by):
        return lax.rem(self.at[d] + by + SIZES[d], SIZES[d])

    def device(self, core=None, **at):
        at = {**self.at, **at}
        core = self.core if core is None else core
        return (0, ((at["x"] * SIZES["y"] + at["y"]) * SIZES["z"] + at["z"]) * 2 + core)

    def barrier(self):
        sem = pltpu.get_barrier_semaphore()

        def signal(peer):
            pl.semaphore_signal(sem, inc=1, device_id=peer, device_id_type=MESH)

        for d, n in SIZES.items():
            each(n - 1, lambda i, d=d: signal(self.device(**{d: self.off(d, i + 1)})))
        signal(self.device(core=1 - self.core))
        signal(self.device(core=1 - self.core, z=self.pair()))
        pl.semaphore_wait(sem, sum(SIZES.values()) - 1)

    def pair(self):
        return self.at["z"] + 1 - 2 * lax.rem(self.at["z"], 2)


def dims(kind, free):
    return tuple(SIZES[d] // (2 if kind == TALL and d == "z" else 1) for d in free)


def view(ref, kind, free, fixed, colour=None, base=0, own=False):
    index = [(fixed[d] // 2 if kind == TALL and d == "z" else fixed[d]) if d in fixed else slice(None) for d in free]
    if own and not (kind == TALL and "z" in free and "z" in fixed):
        return ref.at[(*index, slice(None), slice(None))]
    if kind == WIDE:
        first, size = (0, HALF[WIDE]) if colour is None else PART[WIDE][colour]
        rows, columns = slice(None), pl.ds(_at(base, first), size)
    else:
        rows = slice(None) if own or colour is None else pl.ds(*PART[TALL][colour])
        if "z" in free and "z" in fixed:
            columns = pl.ds(pl.multiple_of(base + lax.rem(fixed["z"], 2) * 256, 256), 256)
        else:
            columns = pl.ds(_at(base, 0), HALF[TALL])
    return ref.at[(*index, rows, columns)]


def _at(base, first):
    return first if isinstance(base, int) and base == 0 else pl.multiple_of(base + first, 128)


def block(kind, colour, free):
    first, size = PART[kind][colour]
    tail = (8, size) if kind == WIDE else (size, HALF[TALL] if "z" in free else HALF[TALL] // 2)
    return dims(kind, free) + tail


def lengths(n):
    return n // 2, (n - 1) // 2


def reduce_buffers(kind):
    shapes = {}
    for c, phases in enumerate(COLOURS):
        free = ["x", "y", "z"]
        for p, (d, how) in enumerate(phases):
            free.remove(d)
            shape = block(kind, c, tuple(free))
            count = SIZES[d] - 1
            shapes[c, p] = (count, *shape)
    return shapes


class Copies:
    def __init__(self, send, recv):
        self.send, self.recv, self.all, self.used = send, recv, {}, 0

    def start(self, key, src, dst, to):
        self.start_all(key, 1, lambda i: (src, dst, to))

    def start_all(self, key, count, make):
        first = self.used
        self.used += count

        def copy(i):
            src, dst, to = make(i)
            return pltpu.make_async_remote_copy(
                src_ref=src, dst_ref=dst, send_sem=self.send.at[first + i], recv_sem=self.recv.at[first + i], device_id=to, device_id_type=MESH
            )

        self.all[key] = count, copy
        each(count, lambda i: copy(i).start())

    def arrived(self, key):
        count, copy = self.all[key]
        each(count, lambda i: copy(i).wait_recv())

    def sent(self):
        for count, copy in self.all.values():
            each(count, lambda i, copy=copy: copy(i).wait_send())


def each(count, do):
    if count == 1:
        do(0)
    else:

        @pl.loop(0, count)
        def _(i):
            do(i)


def total(parts):
    return functools.reduce(jnp.add, [p[...].astype(F32) for p in parts])


def reduce_colour(me, copies, key, kind, colour, grads, received, last):
    free, fixed = ("x", "y", "z"), {}
    parts = [lambda at, r=r: view(r, kind, ("x", "y", "z"), at, colour) for r in grads]
    out = parts[0]

    def add(at, more):
        rest = [d for d in free if d not in at]
        if len(rest) >= 2:
            first = rest[0]

            @pl.loop(0, SIZES[first])
            def _(i):
                now = {**at, first: i}
                out(now)[...] = total([p(now) for p in parts + more]).astype(BF16)
        else:
            out(at)[...] = total([p(at) for p in parts + more]).astype(BF16)

    for phase, (d, how) in enumerate(COLOURS[colour]):
        n, buffer = SIZES[d], received(colour, phase)
        left = tuple(e for e in ("x", "y", "z") if e not in fixed and e != d)

        def slot(i, buffer=buffer, left=left):
            return lambda at: view(buffer.at[i], kind, left, {e: v for e, v in at.items() if e in left}, colour, own=True)

        if how == RING:
            long, short = lengths(n)
            ways = ((me.sign, long, 0, "l"), (-me.sign, short, long, "s"))
            for s in range(long):
                for sign, length, base, name in ways:
                    if s >= length:
                        continue
                    to = me.off(d, sign * (length - s))
                    at = {**fixed, d: to}
                    if s:
                        copies.arrived((key, colour, phase, name, s - 1))
                    add(at, [slot(base + s - 1)] if s else [])
                    copies.start(
                        (key, colour, phase, name, s), out(at), buffer.at[base + s], me.device(**{d: me.off(d, sign)})
                    )
                yield
            for sign, length, base, name in ways:
                if length:
                    copies.arrived((key, colour, phase, name, length - 1))
            parts = parts + [slot(base + length - 1) for sign, length, base, name in ways if length]
        else:

            def make(i, d=d, fixed=fixed, buffer=buffer, add=add, out=out):
                to = me.off(d, i + 1)
                return out({**fixed, d: to}), buffer.at[i], me.device(**{d: to})

            each(n - 1, lambda i: add({**fixed, d: me.off(d, i + 1)}, []))
            copies.start_all((key, colour, phase), n - 1, make)
            yield
            copies.arrived((key, colour, phase))
            parts = parts + [slot(i) for i in range(n - 1)]
        fixed = {**fixed, d: me.at[d]}
    last(colour, total([p(fixed) for p in parts]).astype(BF16).astype(F32))


def reduce_kernel(*refs):
    ins, outs, rest = refs[:6], refs[6:8], list(refs[8:])
    own = {WIDE: rest[0], TALL: rest[1]}
    other = {WIDE: rest[2], TALL: rest[3]}
    sums = {WIDE: rest[4], TALL: rest[5]}
    cross = {WIDE: rest[6], TALL: rest[7]}
    shares = rest[8]
    load, send, recv = rest[9:12]
    bufs = {}
    for kind in (WIDE, TALL):
        for k in reduce_buffers(kind):
            bufs[kind, k] = rest[12 + len(bufs)]
    me = Me()
    me.barrier()
    copies = Copies(send, recv)
    loads = []
    for i, (kind, j) in enumerate(ORDER):
        half = HALF[kind]
        src = ins[i].at[..., pl.ds(pl.multiple_of(me.core * half, 256), half)]
        copy = pltpu.make_async_copy(src, own[kind].at[j], load.at[i])
        copy.start()
        loads.append(copy)
        src = ins[i].at[..., pl.ds(pl.multiple_of((1 - me.core) * half, 256), half)]
        copies.start((i, "half"), src, other[kind].at[j], me.device(core=1 - me.core))

    def begin(i):
        loads[i].wait()
        copies.arrived((i, "half"))

    def colour(i, c):
        kind, j = ORDER[i]
        if i in waiting:
            waiting.discard(i)
            begin(i)

        def last(colour, value):
            first, size = PART[kind][colour]
            if kind == WIDE:
                sums[WIDE][j, 0, :, first : first + size] = value[:4]
                sums[WIDE][j, 1, :, first : first + size] = value[4:]
            else:
                sums[TALL][j, first : first + size, :] = value

        yield from reduce_colour(
            me, copies, i, kind, c, (own[kind].at[j], other[kind].at[j]), lambda c, p: bufs[kind, (c, p)].at[j], last
        )

    def finish(i):
        kind, j = ORDER[i]
        if kind == WIDE:
            copies.start((i, "rows"), sums[WIDE].at[j, 1 - me.core], cross[WIDE].at[j], me.device(core=1 - me.core))
        else:
            for q in range(4):
                shares[j, q] = sums[TALL][j, 10 * q : 10 * q + 10, :]
            b = lax.rem(me.at["z"], 2)
            mine = 2 * b + me.core
            for o, (z, core) in enumerate(((me.at["z"], 1 - me.core), (me.pair(), me.core), (me.pair(), 1 - me.core))):
                q = 2 * lax.rem(z, 2) + core
                copies.start((i, "rows", o), shares.at[j, q], cross[TALL].at[j, mine], me.device(core=core, z=z))
        yield
        if kind == WIDE:
            copies.arrived((i, "rows"))
            outs[0][j, me.core] = sums[WIDE][j, me.core]
            outs[0][j, 1 - me.core] = cross[WIDE][j]
        else:
            for o in range(3):
                copies.arrived((i, "rows", o))
            for q in range(4):
                outs[1][j, q] = jnp.where(q == mine, shares[j, q], cross[TALL][j, q])

    waiting = set(range(6))
    run({(i, c): colour(i, c) for i in range(6) for c in range(3)} | {(i, 3): finish(i) for i in range(6)}, REDUCE_ORDER)
    copies.sent()


def run(streams, order):
    for i, c in zip(order[::2], order[1::2], strict=True):
        next(streams[int(i), int(c)], None)
    for stream in streams.values():
        assert next(stream, 0) == 0, "not done"


def full_shape(kind):
    return dims(kind, ("x", "y", "z")) + (ROWS[kind], HALF[kind])


def reduce_scatter(grads):
    scratch = [
        pltpu.VMEM((4, *full_shape(WIDE)), BF16),
        pltpu.VMEM((2, *full_shape(TALL)), BF16),
        pltpu.VMEM((4, *full_shape(WIDE)), BF16),
        pltpu.VMEM((2, *full_shape(TALL)), BF16),
        pltpu.VMEM((4, 2, 4, 1280), F32),
        pltpu.VMEM((2, 40, 256), F32),
        pltpu.VMEM((4, 4, 1280), F32),
        pltpu.VMEM((2, 4, 10, 256), F32),
        pltpu.VMEM((2, 4, 10, 256), F32),
        pltpu.SemaphoreType.DMA((6,)),
        pltpu.SemaphoreType.DMA((256,)),
        pltpu.SemaphoreType.DMA((256,)),
    ]
    for kind, many in ((WIDE, 4), (TALL, 2)):
        scratch += [pltpu.VMEM((many, *shape), BF16) for shape in reduce_buffers(kind).values()]
    return pl.pallas_call(
        reduce_kernel,
        out_shape=(jax.ShapeDtypeStruct((4, 2, 4, 1280), F32), jax.ShapeDtypeStruct((2, 4, 10, 256), F32)),
        in_specs=[pl.BlockSpec(memory_space=pl.ANY)] * 6,
        out_specs=(pl.BlockSpec(memory_space=pltpu.VMEM), pl.BlockSpec(memory_space=pltpu.VMEM)),
        scratch_shapes=scratch,
        compiler_params=pltpu.CompilerParams(collective_id=0, has_side_effects=True, vmem_limit_bytes=VMEM_LIMIT),
        name="reduce_scatter",
    )(*grads)


def gather_colour(me, copies, key, kind, colour, ref):
    base = me.core * HALF[kind]
    fixed = dict(me.at)

    def part(at):
        return view(ref, kind, ("x", "y", "z"), at, colour, base)

    phases = COLOURS[colour][::-1]
    for phase, (d, how) in enumerate(phases):
        n, lastly = SIZES[d], phase == len(phases) - 1
        rest = {e: v for e, v in fixed.items() if e != d}
        here = part(fixed)

        def across(name, at):
            if lastly:
                copies.start((key, colour, "across", name), part(at), part(at), me.device(core=1 - me.core))

        if how == RING:
            long, short = lengths(n)
            ways = ((me.sign, long, "l"), (-me.sign, short, "s"))
            for s in range(long):
                for sign, length, name in ways:
                    if s >= length:
                        continue
                    at = {**rest, d: me.off(d, -sign * s)}
                    if s:
                        copies.arrived((key, colour, phase, name, s - 1))
                    copies.start((key, colour, phase, name, s), part(at), part(at), me.device(**{d: me.off(d, sign)}))
                    if s:
                        across((name, s - 1), at)
                if s == 0:
                    across("own", fixed)
                yield
            for sign, length, name in ways:
                if length:
                    copies.arrived((key, colour, phase, name, length - 1))
                    across((name, length - 1), {**rest, d: me.off(d, -sign * length)})
        else:
            copies.start_all(
                (key, colour, phase), n - 1, lambda i, d=d, here=here: (here, here, me.device(**{d: me.off(d, i + 1)}))
            )
            yield
            copies.arrived((key, colour, phase))
        fixed = rest
    yield
    names = ["own"]
    d, how = phases[-1]
    long, short = lengths(SIZES[d])
    names += [("l", s) for s in range(long)] + [("s", s) for s in range(short)]
    for name in names:
        copies.arrived((key, colour, "across", name))


def gather_kernel(*refs):
    wide, tall, outs, rest = refs[0], refs[1], refs[2:8], refs[8:]
    cross = {WIDE: rest[0], TALL: rest[1]}
    forty, send, recv = rest[2:5]
    me = Me()
    me.barrier()
    copies = Copies(send, recv)
    mine = 2 * lax.rem(me.at["z"], 2) + me.core

    for i, (kind, j) in enumerate(ORDER):
        if kind == WIDE:
            copies.start((i, "rows"), wide.at[j, 1 - me.core], cross[WIDE].at[j], me.device(core=1 - me.core))
        else:
            for o, (z, core) in enumerate(((me.at["z"], 1 - me.core), (me.pair(), me.core), (me.pair(), 1 - me.core))):
                q = 2 * lax.rem(z, 2) + core
                copies.start((i, "rows", o), tall.at[j, q], cross[TALL].at[j, mine], me.device(core=core, z=z))

    def begin(i):
        kind, j = ORDER[i]
        here = view(outs[i], kind, ("x", "y", "z"), me.at, None, me.core * HALF[kind])
        if kind == WIDE:
            copies.arrived((i, "rows"))
            own, theirs = wide[j, me.core], cross[WIDE][j]
            first = me.core == 0
            rows = [jnp.where(first, own, theirs), jnp.where(first, theirs, own)]
            here[...] = jnp.concatenate(rows, axis=0).astype(BF16)
        else:
            for o in range(3):
                copies.arrived((i, "rows", o))
            for q in range(4):
                forty[10 * q : 10 * q + 10, :] = jnp.where(q == mine, tall[j, q], cross[TALL][j, q])
            here[...] = forty[...].astype(BF16)

    def colour(i, c):
        if i in waiting:
            waiting.discard(i)
            begin(i)
        yield from gather_colour(me, copies, i, ORDER[i][0], c, outs[i])

    waiting = set(range(6))
    run({(i, c): colour(i, c) for i in range(6) for c in range(3)}, GATHER_ORDER)
    copies.sent()


def all_gather(wide, tall):
    scratch = [
        pltpu.VMEM((4, 4, 1280), F32),
        pltpu.VMEM((2, 4, 10, 256), F32),
        pltpu.VMEM((40, 256), F32),
        pltpu.SemaphoreType.DMA((384,)),
        pltpu.SemaphoreType.DMA((384,)),
    ]
    return pl.pallas_call(
        gather_kernel,
        out_shape=tuple(pltpu.VMEM((*dims(kind, ("x", "y", "z")), ROWS[kind], 2 * HALF[kind]), BF16) for kind, _ in ORDER),
        in_specs=[pl.BlockSpec(memory_space=pltpu.VMEM)] * 2,
        out_specs=(pl.BlockSpec(memory_space=pltpu.VMEM),) * 6,
        scratch_shapes=scratch,
        compiler_params=pltpu.CompilerParams(collective_id=1, has_side_effects=True, vmem_limit_bytes=4 * 1024 * 1024),
        name="all_gather",
    )(wide, tall)


def spill_kernel(*refs):
    ins, outs, sem = refs[:6], refs[6:9], refs[9]
    copies = []
    for i, (kind, j) in enumerate(ORDER):
        which, layer = (2, j) if kind == TALL else (j // 2, j % 2)
        copies.append(pltpu.make_async_copy(ins[i], outs[which].at[layer], sem.at[i]))
        copies[-1].start()
    for copy in copies:
        copy.wait()


def spill(new):
    wide, tall = ((2, *dims(kind, ("x", "y", "z")), ROWS[kind], 2 * HALF[kind]) for kind in (WIDE, TALL))
    return pl.pallas_call(
        spill_kernel,
        out_shape=tuple(jax.ShapeDtypeStruct(shape, BF16) for shape in (wide, wide, tall)),
        in_specs=[pl.BlockSpec(memory_space=pltpu.VMEM)] * 6,
        out_specs=(pl.BlockSpec(memory_space=pl.ANY),) * 3,
        scratch_shapes=[pltpu.SemaphoreType.DMA((6,))],
        compiler_params=pltpu.CompilerParams(vmem_limit_bytes=1024 * 1024),
        name="spill",
    )(*new)


def matmul(a, w):
    return jnp.dot(a, w, preferred_element_type=F32).astype(BF16)


def normed(h):
    wide = h.astype(F32)
    scale = lax.rsqrt(jnp.mean(wide**2, -1, keepdims=True) + 1e-6)
    return (wide * scale).astype(BF16)


def layer(h, w):
    a = normed(h)
    gate = jnp.dot(a, w["w_gate"], preferred_element_type=F32)
    up = jnp.dot(a, w["w_up"], preferred_element_type=F32)
    return h + matmul((jax.nn.silu(gate) * up).astype(BF16), w["w_down"])


def adamw(w, m, v, g):
    m = 0.9 * m + 0.1 * g
    v = 0.95 * v + 0.05 * g * g
    step = m * lax.rsqrt(v + 1e-8) + 0.1 * w
    return (w - 0.02 * step).astype(BF16), m, v


def stack(weights, h):
    for w in weights:
        h = layer(h, w)
    return h


def split(g, kind):
    return g.reshape(*dims(kind, ("x", "y", "z")), ROWS[kind], 2 * HALF[kind])


def reduced(grads):
    ordered = []
    for kind, j in ORDER:
        name = "w_down" if kind == TALL else NAMES[j // 2]
        ordered.append(split(grads[j % 2][name], kind))
    wide, tall = reduce_scatter(ordered)
    wide = wide.transpose(0, 2, 1, 3).reshape(2, 2, 4, 2560)
    tall = tall.reshape(2, 2, 2, 10, 256).transpose(0, 3, 2, 1, 4).reshape(2, 10, 1024)
    return wide[0], wide[1], tall


def gathered(gate, up, down):
    wide = jnp.stack([gate, up]).reshape(4, 4, 2, 1280).transpose(0, 2, 1, 3).astype(F32)
    tall = down.reshape(2, 10, 2, 2, 256).transpose(0, 3, 2, 1, 4).reshape(2, 4, 10, 256).astype(F32)
    new = spill(all_gather(wide, tall))
    return tuple(w.reshape(2, -1, w.shape[-1]) for w in new)


def solution(mesh):
    def step(x, dy, *arrays):
        weights, m, v = (arrays[i : i + 3] for i in (0, 3, 6))
        layers = [{name: w[l] for name, w in zip(NAMES, weights, strict=True)} for l in range(2)]
        _, back = jax.vjp(lambda w: stack(w, x[0]), layers)
        gradients = reduced(back(dy[0])[0])
        index = lax.axis_index("dp")
        news = []
        for w, mm, vv, g in zip(weights, m, v, gradients, strict=True):
            rows = mm.shape[1]
            mine = lax.dynamic_slice_in_dim(w, index * rows, rows, 1)
            news.append(adamw(mine.astype(F32), mm, vv, g))
        new = gathered(*(n[0] for n in news))
        return (*new, *(n[1] for n in news), *(n[2] for n in news))

    batch, whole, rows = P(("rep", "dp")), P(), P(None, "dp")
    return jax.shard_map(
        step,
        mesh=mesh,
        in_specs=(batch, batch, *(whole,) * 3, *(rows,) * 6),
        out_specs=(*(P("rep"),) * 3, *(P("rep", "dp"),) * 6),
        check_vma=False,
    )
```

```python
import functools

import jax
import jax.numpy as jnp
from jax import lax
from jax.experimental import pallas as pl
from jax.experimental.pallas import tpu as pltpu
from jax.sharding import PartitionSpec as P

NAMES = ("w_gate", "w_up", "w_down")
MESH = pl.DeviceIdType.MESH
F32, BF16 = jnp.float32, jnp.bfloat16
SIZES = {"x": 4, "y": 4, "z": 8}
VMEM_LIMIT = 64 * 1024 * 1024 - 64 * 1024

TICKS = {
    "first": ["0h"],
    "wide1": ["1h", "1s", "2h020100", "12110210222120"],
    "back": ["", "01001202", "111022", "", "122120010002", "111022", "1202210020", "0111102202001221200111021022202112000103221112101303"],
    "units": ["1321202223", "", "23", "", "", "", "", "", "", ""],
    "last": ["3h"],
    "wide0": ["4h", "4s", "5h323130", "42413240525150"],
    "tail": ["3130423241405242515032313052414042513230504031415251304231324140505251324230503133524142404351334352505353"],
}
GATHER_ORDER = "020100121110222120023231301242412240013202525150004211125210220121002032104211003120300110215241110240203051501200310122321011214240413050520220511201110122001132213140500010414210522102302112203151222032414042525002021231302212323140514230223252414050425241515051"


RING, DIRECT = "ring", "direct"
COLOURS = (
    (("x", RING), ("y", RING), ("z", DIRECT)),
    (("y", RING), ("x", RING), ("z", DIRECT)),
    (("z", RING), ("x", DIRECT), ("y", DIRECT)),
)
WIDE, TALL = "wide", "tall"
PART = {WIDE: ((0, 384), (384, 384), (768, 512)), TALL: ((0, 16), (16, 16), (32, 8))}
HALF = {WIDE: 1280, TALL: 512}
ROWS = {WIDE: 8, TALL: 40}
ORDER = ((TALL, 1), (WIDE, 1), (WIDE, 3), (TALL, 0), (WIDE, 0), (WIDE, 2))


class Me:
    def __init__(self):
        index = lax.axis_index("dp")
        Me.zero = index * 0
        self.core = lax.rem(index, 2)
        chip = index // 2
        self.at = {
            "z": lax.rem(chip, SIZES["z"]),
            "y": lax.rem(chip // SIZES["z"], SIZES["y"]),
            "x": chip // (SIZES["z"] * SIZES["y"]),
        }
        self.sign = 1 - 2 * self.core

    def off(self, d, by):
        return lax.rem(self.at[d] + by + SIZES[d], SIZES[d])

    def device(self, core=None, **at):
        at = {**self.at, **at}
        core = self.core if core is None else core
        return (0, ((at["x"] * SIZES["y"] + at["y"]) * SIZES["z"] + at["z"]) * 2 + core)

    def barrier(self):
        sem = pltpu.get_barrier_semaphore()

        def signal(peer):
            pl.semaphore_signal(sem, inc=1, device_id=peer, device_id_type=MESH)

        for d, n in SIZES.items():
            each(n - 1, lambda i, d=d: signal(self.device(**{d: self.off(d, i + 1)})))
        signal(self.device(core=1 - self.core))
        signal(self.device(core=1 - self.core, z=self.pair()))
        pl.semaphore_wait(sem, sum(SIZES.values()) - 1)

    def pair(self):
        return self.at["z"] + 1 - 2 * lax.rem(self.at["z"], 2)


def dims(kind, free):
    return tuple(SIZES[d] // (2 if kind == TALL and d == "z" else 1) for d in free)


def view(ref, kind, free, fixed, colour=None, base=0, own=False):
    index = [(fixed[d] // 2 if kind == TALL and d == "z" else fixed[d]) if d in fixed else slice(None) for d in free]
    if own and not (kind == TALL and "z" in free and "z" in fixed):
        return ref.at[(*index, slice(None), slice(None))]
    if kind == WIDE:
        first, size = (0, HALF[WIDE]) if colour is None else PART[WIDE][colour]
        rows, columns = slice(None), pl.ds(_at(base, first), size)
    else:
        rows = slice(None) if own or colour is None else pl.ds(*PART[TALL][colour])
        if "z" in free and "z" in fixed:
            columns = pl.ds(pl.multiple_of(base + lax.rem(fixed["z"], 2) * 256, 256), 256)
        else:
            columns = pl.ds(_at(base, 0), HALF[TALL])
    return ref.at[(*index, rows, columns)]


def _at(base, first):
    return first if isinstance(base, int) and base == 0 else pl.multiple_of(base + first, 128)


def block(kind, colour, free):
    first, size = PART[kind][colour]
    tail = (8, size) if kind == WIDE else (size, HALF[TALL] if "z" in free else HALF[TALL] // 2)
    return dims(kind, free) + tail


def lengths(n):
    return n // 2, (n - 1) // 2


def reduce_buffers(kind):
    shapes = {}
    for c, phases in enumerate(COLOURS):
        free = ["x", "y", "z"]
        for p, (d, how) in enumerate(phases):
            free.remove(d)
            shape = block(kind, c, tuple(free))
            count = SIZES[d] - 1
            shapes[c, p] = (count, *shape)
    return shapes


class Copies:
    def __init__(self, send, recv):
        self.send, self.recv, self.all, self.used, self.left = send, recv, {}, 0, set()

    def start(self, key, make):
        self.start_all(key, 1, lambda i: make())

    def start_all(self, key, count, make):
        first = self.used
        self.used += count

        def copy(i):
            src, dst, to = make(i)
            return pltpu.make_async_remote_copy(
                src_ref=src, dst_ref=dst, send_sem=self.send.at[first + i], recv_sem=self.recv.at[first + i], device_id=to, device_id_type=MESH
            )

        self.all[key] = count, copy
        each(count, lambda i: copy(i).start())

    def arrived(self, key):
        count, copy = self.all[key]
        each(count, lambda i: copy(i).wait_recv())

    def sent(self, mine=lambda key: True):
        for key, (count, copy) in self.all.items():
            if key not in self.left and mine(key):
                self.left.add(key)
                each(count, lambda i, copy=copy: copy(i).wait_send())


def each(count, do):
    if count == 1:
        do(0)
    else:

        loop(count)(do)


def loop(count):
    def run(body):
        def step(carry, _):
            body(carry[0])
            return (carry[0] + 1, None), None

        lax.scan(step, (Me.zero, None), None, length=count)

    return run


def total(parts):
    return functools.reduce(jnp.add, [p[...].astype(F32) for p in parts])


def reduce_colour(me, copies, key, kind, colour, grads, received, last):
    free, fixed = ("x", "y", "z"), {}
    parts = [lambda at, r=r: view(r(), kind, ("x", "y", "z"), at, colour) for r in grads]
    out = parts[0]

    def add(at, more):
        rest = [d for d in free if d not in at]
        if len(rest) >= 2:
            first = rest[0]

            @loop(SIZES[first])
            def _(i):
                now = {**at, first: i}
                out(now)[...] = total([p(now) for p in parts + more]).astype(BF16)
        else:
            out(at)[...] = total([p(at) for p in parts + more]).astype(BF16)

    for phase, (d, how) in enumerate(COLOURS[colour]):
        n, buffer = SIZES[d], functools.partial(received, colour, phase)
        left = tuple(e for e in ("x", "y", "z") if e not in fixed and e != d)

        def slot(i, buffer=buffer, left=left):
            return lambda at: view(buffer().at[i], kind, left, {e: v for e, v in at.items() if e in left}, colour, own=True)

        if how == RING:
            long, short = lengths(n)
            ways = ((1, long, 0, "l"), (-1, short, long, "s"))
            for s in range(long):
                for sign, length, base, name in ways:
                    if s >= length:
                        continue

                    def make(d=d, fixed=fixed, buffer=buffer, sign=sign, by=length - s, place=base + s):
                        at = {**fixed, d: me.off(d, me.sign * (sign * by))}
                        return out(at), buffer().at[place], me.device(**{d: me.off(d, me.sign * sign)})

                    if s:
                        copies.arrived((key, colour, phase, name, s - 1))
                    add({**fixed, d: me.off(d, me.sign * (sign * (length - s)))}, [slot(base + s - 1)] if s else [])
                    copies.start((key, colour, phase, name, s), make)
                yield
            for sign, length, base, name in ways:
                if length:
                    copies.arrived((key, colour, phase, name, length - 1))
            parts = parts + [slot(base + length - 1) for sign, length, base, name in ways if length]
        else:

            def make(i, d=d, fixed=fixed, buffer=buffer, add=add, out=out):
                to = me.off(d, i + 1)
                return out({**fixed, d: to}), buffer().at[i], me.device(**{d: to})

            each(n - 1, lambda i: add({**fixed, d: me.off(d, i + 1)}, []))
            copies.start_all((key, colour, phase), n - 1, make)
            yield
            copies.arrived((key, colour, phase))
            parts = parts + [slot(i) for i in range(n - 1)]
        fixed = {**fixed, d: me.at[d]}
    last(colour, total([p(fixed) for p in parts]).astype(BF16).astype(F32))


class Reduce:
    def __init__(self, me, own, theirs, halves, buffers, sums, cross, shares, outs, send, recv, free):
        self.me, self.own, self.theirs, self.halves, self.buffers = me, own, theirs, halves, buffers
        self.sums, self.cross, self.shares, self.outs, self.free = sums, cross, shares, outs, free
        self.copies = Copies(send, recv)
        self.waiting = set(range(6))
        self.streams = {(i, c): self.colour(i, c) for i in range(6) for c in range(3)} | {(i, 3): self.finish(i) for i in range(6)}

    def slot(self, i):
        kind, j = ORDER[i]
        return 0 if kind == TALL else j // 2

    def half(self, i):
        kind = ORDER[i][0]
        if i >= 3:
            pl.semaphore_wait(self.free.at[i - 3], sum(SIZES.values()) - len(SIZES) + 1)
        self.copies.start(
            (i, "half"), lambda: (self.halves[kind](), self.theirs[kind].at[self.slot(i)], self.me.device(core=1 - self.me.core))
        )

    def half_sent(self, i):
        self.copies.sent(lambda key: key == (i, "half"))

    def colour(self, i, c):
        kind, j = ORDER[i]
        slot = self.slot(i)
        if i in self.waiting:
            self.waiting.discard(i)
            self.copies.arrived((i, "half"))

        def last(colour, value):
            first, size = PART[kind][colour]
            if kind == WIDE:
                self.sums[WIDE][j, 0, :, first : first + size] = value[:4]
                self.sums[WIDE][j, 1, :, first : first + size] = value[4:]
            else:
                self.sums[TALL][j, first : first + size, :] = value

        grads = (lambda: self.own[kind].at[slot]), (lambda: self.theirs[kind].at[slot])
        yield from reduce_colour(self.me, self.copies, i, kind, c, grads, lambda c, p: self.buffers[kind, (c, p)].at[slot], last)

    def finish(self, i):
        (kind, j), me, copies = ORDER[i], self.me, self.copies
        sums, cross, shares, outs = self.sums, self.cross, self.shares, self.outs
        mine = 2 * lax.rem(me.at["z"], 2) + me.core
        if kind == WIDE:
            copies.start((i, "rows"), lambda: (sums[WIDE].at[j, 1 - me.core], cross[WIDE].at[j], me.device(core=1 - me.core)))
        else:
            for q in range(4):
                shares[j, q] = sums[TALL][j, 10 * q : 10 * q + 10, :]
            for o in range(3):

                def make(o=o):
                    z, core = ((me.at["z"], 1 - me.core), (me.pair(), me.core), (me.pair(), 1 - me.core))[o]
                    mine = 2 * lax.rem(me.at["z"], 2) + me.core
                    return shares.at[j, 2 * lax.rem(z, 2) + core], cross[TALL].at[j, mine], me.device(core=core, z=z)

                copies.start((i, "rows", o), make)
        if i < 3:
            for d, n in SIZES.items():
                each(n - 1, lambda o, d=d: self.done(i, me.device(**{d: me.off(d, o + 1)})))
            self.done(i, me.device(core=1 - me.core))
        yield
        mine = 2 * lax.rem(me.at["z"], 2) + me.core
        if kind == WIDE:
            copies.arrived((i, "rows"))
            outs[0][j, me.core] = sums[WIDE][j, me.core]
            outs[0][j, 1 - me.core] = cross[WIDE][j]
        else:
            for o in range(3):
                copies.arrived((i, "rows", o))
            for q in range(4):
                outs[1][j, q] = jnp.where(q == mine, shares[j, q], cross[TALL][j, q])
        copies.sent(lambda key: key[0] == i)

    def done(self, i, device):
        pl.semaphore_signal(self.free.at[i], inc=1, device_id=device, device_id_type=MESH)

    def run(self, order):
        for i, c in zip(order[::2], order[1::2], strict=True):
            if c == "h":
                self.half(int(i))
            elif c == "s":
                self.half_sent(int(i))
            else:
                next(self.streams[int(i), int(c)], None)


def dot(a, b, ca=1, cb=0):
    return lax.dot_general(a, b, (((ca,), (cb,)), ((), ())), preferred_element_type=F32)


def rem(a, b):
    return a % b if isinstance(a, int) else lax.rem(a, b)


def at_tile(i, size):
    return pl.ds(pl.multiple_of(i * size, size), size)


def put_rows(ref, i, value):
    y, z, rows = ref.shape[1:4]
    for s in range(0, 256, 8):
        row = i * 256 + s
        group = lax.div(row, rows)
        ref[lax.div(group, y * z), rem(lax.div(group, z), y), rem(group, z), pl.ds(pl.multiple_of(rem(row, rows), 8), 8), :] = value[s : s + 8]


def put_all(ref, value):
    ref[...] = value.reshape(ref.shape)


def backward_kernel(*refs):
    a1_in, dy_in, h1_in, a0_in, gate_in, up_in, w_gate, w_up, w_down = refs[:9]
    outs = refs[9:11]
    rest = list(refs[11:])
    take = lambda n: [rest.pop(0) for _ in range(n)]
    act, dy, turned, back, both, gates, ups, hidden = take(8)
    tile_g, tile_u, tile_d, rows_w = take(4)
    wide_own, wide_theirs, tall_own, tall_half, tall_theirs = take(5)
    wide_sums, tall_sums, wide_cross, tall_cross, shares = take(5)
    load, sem_g, sem_u, sem_d, sem_w, sem_f, send, recv, free = take(9)
    buffers = {}
    for kind in (WIDE, TALL):
        for k in reduce_buffers(kind):
            buffers[kind, k] = rest.pop(0)
    me = Me()

    def fetch(src, dst, sem):
        copy = pltpu.make_async_copy(src, dst, sem)
        copy.start()
        return copy

    class Stream:
        def __init__(self, tile, buffer, sem):
            self.tile, self.buffer, self.sem = tile, buffer, sem

        def copy(self, i):
            slot = rem(i, 2)
            return pltpu.make_async_copy(self.tile(i), self.buffer.at[slot], self.sem.at[slot])

    def stream(*streams, n):
        for s in streams:
            s.copy(0).start()

        def ahead(i):
            @pl.when(i + 1 < n)
            def _():
                for s in streams:
                    s.copy(i + 1).start()

            for s in streams:
                s.copy(i).wait()

        return ahead

    loads = [fetch(a1_in, act, load.at[0]), fetch(dy_in, dy, load.at[1])]
    first = stream(
        Stream(lambda i: w_gate.at[1, :, at_tile(i, 256)], tile_g, sem_g),
        Stream(lambda i: w_up.at[1, :, at_tile(i, 256)], tile_u, sem_u),
        Stream(lambda i: w_down.at[1, at_tile(i, 256), :], tile_d, sem_d),
        n=10,
    )
    me.barrier()
    own = {WIDE: wide_own, TALL: tall_own}
    theirs = {WIDE: wide_theirs, TALL: tall_theirs}
    halves = {WIDE: lambda: wide_own.at[2], TALL: lambda: tall_half}
    sums = {WIDE: wide_sums, TALL: tall_sums}
    cross = {WIDE: wide_cross, TALL: tall_cross}
    reduce = Reduce(me, own, theirs, halves, buffers, sums, cross, shares, outs, send, recv, free)

    def ticks(phase, i):
        orders = TICKS[phase]
        if any(orders):
            lax.switch(i, [functools.partial(reduce.run, order) for order in orders])

    def turn(src):
        @pl.loop(0, 8)
        def _(i):
            turned[:, at_tile(i, 128)] = src[at_tile(i, 128), :].T

    def unit(i, gate, up, dout):
        g, u, d = gate[...], up[...], hidden[...].astype(BF16).astype(F32)
        s = jax.nn.sigmoid(g)
        silu = g * s
        value = (silu * u).astype(BF16).T
        both[1, :, at_tile(i, 256)] = (d * silu).astype(BF16)
        both[0, :, at_tile(i, 256)] = (d * u * (s * (1 + g * (1 - s)))).astype(BF16)
        for ref, core in ((tall_own.at[0], me.core), (tall_half, 1 - me.core)):
            put_rows(ref, i, dot(value, dout[:, at_tile(core, 512)]).astype(BF16))

    def wide_grads(phase, layer):
        @pl.loop(0, 4)
        def _(k):
            which, mine = lax.div(k, 2), lax.rem(k, 2)
            core = mine * me.core + (1 - mine) * (1 - me.core)
            value = dot(turned[...], both[which, :, at_tile(core, 1280)]).astype(BF16)
            put_all(wide_own.at[lax.rem(2 - mine * (2 - which), 3)], value)
            ticks(phase, k)

    for copy in loads:
        copy.wait()
    turn(act)

    @pl.loop(0, 10)
    def _(i):
        first(i)
        unit(rem(i + 9, 10), gates.at[0], ups.at[0], dy)
        slot = lax.rem(i, 2)
        gates[0] = dot(act[...], tile_g[slot])
        ups[0] = dot(act[...], tile_u[slot])
        hidden[...] = dot(dy[...], tile_d[slot], 1, 1)

    unit(Me.zero + 9, gates.at[0], ups.at[0], dy)
    reduce.run(TICKS["first"][0])
    wide_grads("wide1", 1)

    load_h = fetch(h1_in, turned, load.at[0])

    def weight_rows(k, w):
        slot = rem(k, 2)
        rows = at_tile(k // 2 if isinstance(k, int) else lax.div(k, 2), 256)
        return pltpu.make_async_copy(w.at[1, rows, :], rows_w.at[slot], sem_w.at[slot])

    weight_rows(0, w_gate).start()

    @pl.loop(0, 8)
    def _(k):
        n, which = lax.div(k, 2), lax.rem(k, 2)

        @pl.when(which == 0)
        def _():
            weight_rows(k + 1, w_up).start()

        @pl.when((which == 1) & (k < 7))
        def _():
            weight_rows(k + 1, w_gate).start()

        weight_rows(k, w_gate).wait()
        part = dot(both[which], rows_w[which], 1, 1).astype(BF16).astype(F32)
        before = back[:, at_tile(n, 256)].astype(F32)
        back[:, at_tile(n, 256)] = (jnp.where(which == 0, 0.0, before) + part).astype(BF16)
        ticks("back", k)

    load_h.wait()

    @pl.loop(0, 8)
    def _(i):
        rows = at_tile(i, 128)
        h, d = turned[rows, :].astype(F32), back[rows, :].astype(F32)
        scale = lax.rsqrt(jnp.mean(h * h, -1, keepdims=True) + 1e-6)
        along = jnp.sum(d * h, -1, keepdims=True)
        d = (d * scale - h * (scale * scale * scale * along * (1 / 1024))).astype(BF16)
        act[rows, :] = (dy[rows, :].astype(F32) + d.astype(F32)).astype(BF16)

    load_a = fetch(a0_in, back, load.at[1])

    def gate_up(i):
        slot = rem(i, 2)
        return (
            pltpu.make_async_copy(gate_in.at[:, at_tile(i, 256)], gates.at[slot], sem_f.at[0, slot]),
            pltpu.make_async_copy(up_in.at[:, at_tile(i, 256)], ups.at[slot], sem_f.at[1, slot]),
        )

    second = stream(Stream(lambda i: w_down.at[0, at_tile(i, 256), :], tile_d, sem_d), n=10)
    load_a.wait()
    turn(back)

    @pl.loop(0, 10)
    def _(i):
        second(i)

        @pl.when(i > 0)
        def _():
            for copy in gate_up(i - 1):
                copy.wait()

        for copy in gate_up(i):
            copy.start()
        j = rem(i + 9, 10)
        unit(j, gates.at[lax.rem(j, 2)], ups.at[lax.rem(j, 2)], act)
        hidden[...] = dot(act[...], tile_d[lax.rem(i, 2)], 1, 1)
        ticks("units", i)

    for copy in gate_up(9):
        copy.wait()
    unit(Me.zero + 9, gates.at[1], ups.at[1], act)
    reduce.run(TICKS["last"][0])
    wide_grads("wide0", 0)
    reduce.run(TICKS["tail"][0])
    for stream_ in reduce.streams.values():
        assert next(stream_, 0) == 0, "not done"
    reduce.copies.sent()


def run(streams, order):
    for i, c in zip(order[::2], order[1::2], strict=True):
        next(streams[int(i), int(c)], None)
    for stream in streams.values():
        assert next(stream, 0) == 0, "not done"


def full_shape(kind):
    return dims(kind, ("x", "y", "z")) + (ROWS[kind], HALF[kind])


def backward(a1, dy, h1, a0, gate, up, w_gate, w_up, w_down):
    square = pltpu.VMEM((1024, 1024), BF16)
    scratch = [square] * 4 + [pltpu.VMEM((2, 1024, 2560), BF16)]
    scratch += [pltpu.VMEM((2, 1024, 256), F32)] * 2 + [pltpu.VMEM((1024, 256), F32)]
    scratch += [pltpu.VMEM((2, 1024, 256), BF16)] * 2 + [pltpu.VMEM((2, 256, 1024), BF16), pltpu.VMEM((2, 256, 2560), BF16)]
    scratch += [
        pltpu.VMEM((3, *full_shape(WIDE)), BF16),
        pltpu.VMEM((2, *full_shape(WIDE)), BF16),
        pltpu.VMEM((1, *full_shape(TALL)), BF16),
        pltpu.VMEM(full_shape(TALL), BF16),
        pltpu.VMEM((1, *full_shape(TALL)), BF16),
        pltpu.VMEM((4, 2, 4, 1280), F32),
        pltpu.VMEM((2, 40, 256), F32),
        pltpu.VMEM((4, 4, 1280), F32),
        pltpu.VMEM((2, 4, 10, 256), F32),
        pltpu.VMEM((2, 4, 10, 256), F32),
        *[pltpu.SemaphoreType.DMA((2,))] * 5,
        pltpu.SemaphoreType.DMA((2, 2)),
        pltpu.SemaphoreType.DMA((256,)),
        pltpu.SemaphoreType.DMA((256,)),
        pltpu.SemaphoreType.REGULAR((3,)),
    ]
    for kind, many in ((WIDE, 2), (TALL, 1)):
        scratch += [pltpu.VMEM((many, *shape), BF16) for shape in reduce_buffers(kind).values()]
    return pl.pallas_call(
        backward_kernel,
        out_shape=(jax.ShapeDtypeStruct((4, 2, 4, 1280), F32), jax.ShapeDtypeStruct((2, 4, 10, 256), F32)),
        in_specs=[pl.BlockSpec(memory_space=pl.ANY)] * 9,
        out_specs=(pl.BlockSpec(memory_space=pltpu.VMEM), pl.BlockSpec(memory_space=pltpu.VMEM)),
        scratch_shapes=scratch,
        compiler_params=pltpu.CompilerParams(collective_id=0, has_side_effects=True, vmem_limit_bytes=VMEM_LIMIT),
        name="backward",
    )(a1, dy, h1, a0, gate, up, w_gate, w_up, w_down)


def gather_colour(me, copies, key, kind, colour, ref):
    base = me.core * HALF[kind]
    fixed = dict(me.at)

    def part(at):
        return view(ref, kind, ("x", "y", "z"), at, colour, base)

    phases = COLOURS[colour][::-1]
    for phase, (d, how) in enumerate(phases):
        n, lastly = SIZES[d], phase == len(phases) - 1
        rest = {e: v for e, v in fixed.items() if e != d}
        here = part(fixed)

        def across(name, at):
            if lastly:
                copies.start((key, colour, "across", name), lambda: (part(at), part(at), me.device(core=1 - me.core)))

        if how == RING:
            long, short = lengths(n)
            ways = ((me.sign, long, "l"), (-me.sign, short, "s"))
            for s in range(long):
                for sign, length, name in ways:
                    if s >= length:
                        continue
                    at = {**rest, d: me.off(d, -sign * s)}
                    if s:
                        copies.arrived((key, colour, phase, name, s - 1))
                    copies.start(
                        (key, colour, phase, name, s),
                        lambda at=at, d=d, sign=sign: (part(at), part(at), me.device(**{d: me.off(d, sign)})),
                    )
                    if s:
                        across((name, s - 1), at)
                if s == 0:
                    across("own", fixed)
                yield
            for sign, length, name in ways:
                if length:
                    copies.arrived((key, colour, phase, name, length - 1))
                    across((name, length - 1), {**rest, d: me.off(d, -sign * length)})
        else:
            copies.start_all(
                (key, colour, phase), n - 1, lambda i, d=d, here=here: (here, here, me.device(**{d: me.off(d, i + 1)}))
            )
            yield
            copies.arrived((key, colour, phase))
        fixed = rest
    yield
    names = ["own"]
    d, how = phases[-1]
    long, short = lengths(SIZES[d])
    names += [("l", s) for s in range(long)] + [("s", s) for s in range(short)]
    for name in names:
        copies.arrived((key, colour, "across", name))


def gather_kernel(*refs):
    wide, tall, outs, rest = refs[0], refs[1], refs[2:8], refs[8:]
    cross = {WIDE: rest[0], TALL: rest[1]}
    forty, send, recv = rest[2:5]
    me = Me()
    me.barrier()
    copies = Copies(send, recv)
    mine = 2 * lax.rem(me.at["z"], 2) + me.core

    for i, (kind, j) in enumerate(ORDER):
        if kind == WIDE:
            copies.start((i, "rows"), lambda j=j: (wide.at[j, 1 - me.core], cross[WIDE].at[j], me.device(core=1 - me.core)))
        else:
            for o, (z, core) in enumerate(((me.at["z"], 1 - me.core), (me.pair(), me.core), (me.pair(), 1 - me.core))):
                q = 2 * lax.rem(z, 2) + core
                copies.start(
                    (i, "rows", o),
                    lambda j=j, q=q, z=z, core=core: (tall.at[j, q], cross[TALL].at[j, mine], me.device(core=core, z=z)),
                )

    def begin(i):
        kind, j = ORDER[i]
        here = view(outs[i], kind, ("x", "y", "z"), me.at, None, me.core * HALF[kind])
        if kind == WIDE:
            copies.arrived((i, "rows"))
            own, theirs = wide[j, me.core], cross[WIDE][j]
            first = me.core == 0
            rows = [jnp.where(first, own, theirs), jnp.where(first, theirs, own)]
            here[...] = jnp.concatenate(rows, axis=0).astype(BF16)
        else:
            for o in range(3):
                copies.arrived((i, "rows", o))
            for q in range(4):
                forty[10 * q : 10 * q + 10, :] = jnp.where(q == mine, tall[j, q], cross[TALL][j, q])
            here[...] = forty[...].astype(BF16)

    def colour(i, c):
        if i in waiting:
            waiting.discard(i)
            begin(i)
        yield from gather_colour(me, copies, i, ORDER[i][0], c, outs[i])

    waiting = set(range(6))
    run({(i, c): colour(i, c) for i in range(6) for c in range(3)}, GATHER_ORDER)
    copies.sent()


def all_gather(wide, tall):
    scratch = [
        pltpu.VMEM((4, 4, 1280), F32),
        pltpu.VMEM((2, 4, 10, 256), F32),
        pltpu.VMEM((40, 256), F32),
        pltpu.SemaphoreType.DMA((384,)),
        pltpu.SemaphoreType.DMA((384,)),
    ]
    return pl.pallas_call(
        gather_kernel,
        out_shape=tuple(pltpu.VMEM((*dims(kind, ("x", "y", "z")), ROWS[kind], 2 * HALF[kind]), BF16) for kind, _ in ORDER),
        in_specs=[pl.BlockSpec(memory_space=pltpu.VMEM)] * 2,
        out_specs=(pl.BlockSpec(memory_space=pltpu.VMEM),) * 6,
        scratch_shapes=scratch,
        compiler_params=pltpu.CompilerParams(collective_id=1, has_side_effects=True, vmem_limit_bytes=4 * 1024 * 1024),
        name="all_gather",
    )(wide, tall)


def spill_kernel(*refs):
    ins, outs, sem = refs[:6], refs[6:9], refs[9]
    copies = []
    for i, (kind, j) in enumerate(ORDER):
        which, layer = (2, j) if kind == TALL else (j // 2, j % 2)
        copies.append(pltpu.make_async_copy(ins[i], outs[which].at[layer], sem.at[i]))
        copies[-1].start()
    for copy in copies:
        copy.wait()


def spill(new):
    wide, tall = ((2, *dims(kind, ("x", "y", "z")), ROWS[kind], 2 * HALF[kind]) for kind in (WIDE, TALL))
    return pl.pallas_call(
        spill_kernel,
        out_shape=tuple(jax.ShapeDtypeStruct(shape, BF16) for shape in (wide, wide, tall)),
        in_specs=[pl.BlockSpec(memory_space=pltpu.VMEM)] * 6,
        out_specs=(pl.BlockSpec(memory_space=pl.ANY),) * 3,
        scratch_shapes=[pltpu.SemaphoreType.DMA((6,))],
        compiler_params=pltpu.CompilerParams(vmem_limit_bytes=1024 * 1024),
        name="spill",
    )(*new)


def normed(h):
    wide = h.astype(F32)
    scale = lax.rsqrt(jnp.mean(wide**2, -1, keepdims=True) + 1e-6)
    return (wide * scale).astype(BF16)


def adamw(w, m, v, g):
    m = 0.9 * m + 0.1 * g
    v = 0.95 * v + 0.05 * g * g
    step = m * lax.rsqrt(v + 1e-8) + 0.1 * w
    return (w - 0.02 * step).astype(BF16), m, v


def rows_of(wide, tall):
    wide = wide.transpose(0, 2, 1, 3).reshape(2, 2, 4, 2560)
    tall = tall.reshape(2, 2, 2, 10, 256).transpose(0, 3, 2, 1, 4).reshape(2, 10, 1024)
    return wide[0], wide[1], tall


def gathered(gate, up, down):
    wide = jnp.stack([gate, up]).reshape(4, 4, 2, 1280).transpose(0, 2, 1, 3).astype(F32)
    tall = down.reshape(2, 10, 2, 2, 256).transpose(0, 3, 2, 1, 4).reshape(2, 4, 10, 256).astype(F32)
    new = spill(all_gather(wide, tall))
    return tuple(w.reshape(2, -1, w.shape[-1]) for w in new)


def solution(mesh):
    def step(x, dy, *arrays):
        weights, m, v = (arrays[i : i + 3] for i in (0, 3, 6))
        w_gate, w_up, w_down = weights
        h0 = x[0]
        a0 = normed(h0)
        gate = jnp.dot(a0, w_gate[0], preferred_element_type=F32)
        up = jnp.dot(a0, w_up[0], preferred_element_type=F32)
        hidden = (jax.nn.silu(gate) * up).astype(BF16)
        h1 = h0 + jnp.dot(hidden, w_down[0], preferred_element_type=F32).astype(BF16)
        gradients = rows_of(*backward(normed(h1), dy[0], h1, a0, gate, up, w_gate, w_up, w_down))
        index = lax.axis_index("dp")
        news = []
        for w, mm, vv, g in zip(weights, m, v, gradients, strict=True):
            rows = mm.shape[1]
            mine = lax.dynamic_slice_in_dim(w, index * rows, rows, 1)
            news.append(adamw(mine.astype(F32), mm, vv, g))
        new = gathered(*(n[0] for n in news))
        return (*new, *(n[1] for n in news), *(n[2] for n in news))

    batch, whole, rows = P(("rep", "dp")), P(), P(None, "dp")
    return jax.shard_map(
        step,
        mesh=mesh,
        in_specs=(batch, batch, *(whole,) * 3, *(rows,) * 6),
        out_specs=(*(P("rep"),) * 3, *(P("rep", "dp"),) * 6),
        check_vma=False,
    )
```

```python
import functools

import jax
import jax.numpy as jnp
from jax import lax
from jax.experimental import pallas as pl
from jax.experimental.pallas import tpu as pltpu
from jax.sharding import PartitionSpec as P

NAMES = ("w_gate", "w_up", "w_down")
MESH = pl.DeviceIdType.MESH
F32, BF16 = jnp.float32, jnp.bfloat16
SIZES = {"x": 4, "y": 4, "z": 8}
VMEM_LIMIT = 64 * 1024 * 1024 - 64 * 1024

TICKS = {
    "first": ["0h"],
    "wide1": ["1h", "1s020100", "2h", "02121110"],
    "back": ["010022212002", "", "121110", "22", "02", "0100122120", "11220210", "010012212010110201001211100222212012012120000311221210131303"],
    "units": ["222120", "", "2223", "23", "", "", "", "", "", ""],
    "last": ["3h"],
    "wide0": ["4h", "4s323130", "5h", "32424140"],
    "tail": ["3130525150324241405232313042515052414032303151424050413032523151404241503251305250423133404252414333514350525353"],
}
GATHER_ORDER = "020100121110222120323102304212414022525101325002420052121110220100212032104200311152200130102141402051025000123101113022403250102142410152200201511112300040315000222110324110421111205251200231123022213240214241505202510212302212313230402242314132405042524151505251"


RING, DIRECT = "ring", "direct"
COLOURS = (
    (("x", RING), ("y", RING), ("z", DIRECT)),
    (("y", RING), ("x", RING), ("z", DIRECT)),
    (("z", RING), ("x", DIRECT), ("y", DIRECT)),
)
WIDE, TALL = "wide", "tall"
PART = {WIDE: ((0, 384), (384, 384), (768, 512)), TALL: ((0, 16), (16, 16), (32, 8))}
HALF = {WIDE: 1280, TALL: 512}
ROWS = {WIDE: 8, TALL: 40}
ORDER = ((TALL, 1), (WIDE, 1), (WIDE, 3), (TALL, 0), (WIDE, 0), (WIDE, 2))


class Me:
    def __init__(self):
        index = lax.axis_index("dp")
        Me.zero = index * 0
        self.core = lax.rem(index, 2)
        chip = index // 2
        self.at = {
            "z": lax.rem(chip, SIZES["z"]),
            "y": lax.rem(chip // SIZES["z"], SIZES["y"]),
            "x": chip // (SIZES["z"] * SIZES["y"]),
        }
        self.sign = 1 - 2 * self.core

    def off(self, d, by):
        return lax.rem(self.at[d] + by + SIZES[d], SIZES[d])

    def device(self, core=None, **at):
        at = {**self.at, **at}
        core = self.core if core is None else core
        return (0, ((at["x"] * SIZES["y"] + at["y"]) * SIZES["z"] + at["z"]) * 2 + core)

    def barrier(self):
        sem = pltpu.get_barrier_semaphore()

        def signal(peer):
            pl.semaphore_signal(sem, inc=1, device_id=peer, device_id_type=MESH)

        for d, n in SIZES.items():
            each(n - 1, lambda i, d=d: signal(self.device(**{d: self.off(d, i + 1)})))
        signal(self.device(core=1 - self.core))
        signal(self.device(core=1 - self.core, z=self.pair()))
        pl.semaphore_wait(sem, sum(SIZES.values()) - 1)

    def pair(self):
        return self.at["z"] + 1 - 2 * lax.rem(self.at["z"], 2)


def dims(kind, free):
    return tuple(SIZES[d] // (2 if kind == TALL and d == "z" else 1) for d in free)


def view(ref, kind, free, fixed, colour=None, base=0, own=False):
    index = [(fixed[d] // 2 if kind == TALL and d == "z" else fixed[d]) if d in fixed else slice(None) for d in free]
    if own and not (kind == TALL and "z" in free and "z" in fixed):
        return ref.at[(*index, slice(None), slice(None))]
    if kind == WIDE:
        first, size = (0, HALF[WIDE]) if colour is None else PART[WIDE][colour]
        rows, columns = slice(None), pl.ds(_at(base, first), size)
    else:
        rows = slice(None) if own or colour is None else pl.ds(*PART[TALL][colour])
        if "z" in free and "z" in fixed:
            columns = pl.ds(pl.multiple_of(base + lax.rem(fixed["z"], 2) * 256, 256), 256)
        else:
            columns = pl.ds(_at(base, 0), HALF[TALL])
    return ref.at[(*index, rows, columns)]


def _at(base, first):
    return first if isinstance(base, int) and base == 0 else pl.multiple_of(base + first, 128)


def block(kind, colour, free):
    first, size = PART[kind][colour]
    tail = (8, size) if kind == WIDE else (size, HALF[TALL] if "z" in free else HALF[TALL] // 2)
    return dims(kind, free) + tail


def lengths(n):
    return n // 2, (n - 1) // 2


def reduce_buffers(kind):
    shapes = {}
    for c, phases in enumerate(COLOURS):
        free = ["x", "y", "z"]
        for p, (d, how) in enumerate(phases):
            free.remove(d)
            shape = block(kind, c, tuple(free))
            count = SIZES[d] - 1
            shapes[c, p] = (count, *shape)
    return shapes


class Copies:
    def __init__(self, send, recv):
        self.send, self.recv, self.all, self.used, self.left = send, recv, {}, 0, set()

    def start(self, key, make):
        self.start_all(key, 1, lambda i: make())

    def start_all(self, key, count, make):
        first = self.used
        self.used += count

        def copy(i):
            src, dst, to = make(i)
            return pltpu.make_async_remote_copy(
                src_ref=src, dst_ref=dst, send_sem=self.send.at[first + i], recv_sem=self.recv.at[first + i], device_id=to, device_id_type=MESH
            )

        self.all[key] = count, copy
        each(count, lambda i: copy(i).start())

    def arrived(self, key):
        count, copy = self.all[key]
        each(count, lambda i: copy(i).wait_recv())

    def sent(self, mine=lambda key: True):
        for key, (count, copy) in self.all.items():
            if key not in self.left and mine(key):
                self.left.add(key)
                each(count, lambda i, copy=copy: copy(i).wait_send())


def each(count, do):
    if count == 1:
        do(0)
    else:

        loop(count)(do)


def loop(count):
    def run(body):
        def step(carry, _):
            body(carry[0])
            return (carry[0] + 1, None), None

        lax.scan(step, (Me.zero, None), None, length=count)

    return run


def total(parts):
    return functools.reduce(jnp.add, [p[...].astype(F32) for p in parts])


def reduce_colour(me, copies, key, kind, colour, grads, received, last):
    free, fixed = ("x", "y", "z"), {}
    parts = [lambda at, r=r: view(r(), kind, ("x", "y", "z"), at, colour) for r in grads]
    out = parts[0]

    def add(at, more):
        rest = [d for d in free if d not in at]
        if len(rest) >= 2:
            first = rest[0]

            @loop(SIZES[first])
            def _(i):
                now = {**at, first: i}
                out(now)[...] = total([p(now) for p in parts + more]).astype(BF16)
        else:
            out(at)[...] = total([p(at) for p in parts + more]).astype(BF16)

    for phase, (d, how) in enumerate(COLOURS[colour]):
        n, buffer = SIZES[d], functools.partial(received, colour, phase)
        left = tuple(e for e in ("x", "y", "z") if e not in fixed and e != d)

        def slot(i, buffer=buffer, left=left):
            return lambda at: view(buffer().at[i], kind, left, {e: v for e, v in at.items() if e in left}, colour, own=True)

        if how == RING:
            long, short = lengths(n)
            ways = ((1, long, 0, "l"), (-1, short, long, "s"))
            for s in range(long):
                for sign, length, base, name in ways:
                    if s >= length:
                        continue

                    def make(d=d, fixed=fixed, buffer=buffer, sign=sign, by=length - s, place=base + s):
                        at = {**fixed, d: me.off(d, me.sign * (sign * by))}
                        return out(at), buffer().at[place], me.device(**{d: me.off(d, me.sign * sign)})

                    if s:
                        copies.arrived((key, colour, phase, name, s - 1))
                    add({**fixed, d: me.off(d, me.sign * (sign * (length - s)))}, [slot(base + s - 1)] if s else [])
                    copies.start((key, colour, phase, name, s), make)
                yield
            for sign, length, base, name in ways:
                if length:
                    copies.arrived((key, colour, phase, name, length - 1))
            parts = parts + [slot(base + length - 1) for sign, length, base, name in ways if length]
        else:

            def make(i, d=d, fixed=fixed, buffer=buffer, add=add, out=out):
                to = me.off(d, i + 1)
                return out({**fixed, d: to}), buffer().at[i], me.device(**{d: to})

            each(n - 1, lambda i: add({**fixed, d: me.off(d, i + 1)}, []))
            copies.start_all((key, colour, phase), n - 1, make)
            yield
            copies.arrived((key, colour, phase))
            parts = parts + [slot(i) for i in range(n - 1)]
        fixed = {**fixed, d: me.at[d]}
    last(colour, total([p(fixed) for p in parts]).astype(BF16).astype(F32))


class Reduce:
    def __init__(self, me, own, theirs, halves, buffers, sums, cross, shares, outs, send, recv, free):
        self.me, self.own, self.theirs, self.halves, self.buffers = me, own, theirs, halves, buffers
        self.sums, self.cross, self.shares, self.outs, self.free = sums, cross, shares, outs, free
        self.copies = Copies(send, recv)
        self.waiting = set(range(6))
        self.streams = {(i, c): self.colour(i, c) for i in range(6) for c in range(3)} | {(i, 3): self.finish(i) for i in range(6)}

    def slot(self, i):
        kind, j = ORDER[i]
        return 0 if kind == TALL else j // 2

    def half(self, i):
        kind = ORDER[i][0]
        if i >= 3:
            pl.semaphore_wait(self.free.at[i - 3], sum(SIZES.values()) - len(SIZES) + 1)
        self.copies.start(
            (i, "half"), lambda: (self.halves[kind](), self.theirs[kind].at[self.slot(i)], self.me.device(core=1 - self.me.core))
        )

    def half_sent(self, i):
        self.copies.sent(lambda key: key == (i, "half"))

    def colour(self, i, c):
        kind, j = ORDER[i]
        slot = self.slot(i)
        if i in self.waiting:
            self.waiting.discard(i)
            self.copies.arrived((i, "half"))

        def last(colour, value):
            first, size = PART[kind][colour]
            if kind == WIDE:
                self.sums[WIDE][j, 0, :, first : first + size] = value[:4]
                self.sums[WIDE][j, 1, :, first : first + size] = value[4:]
            else:
                self.sums[TALL][j, first : first + size, :] = value

        grads = (lambda: self.own[kind].at[slot]), (lambda: self.theirs[kind].at[slot])
        yield from reduce_colour(self.me, self.copies, i, kind, c, grads, lambda c, p: self.buffers[kind, (c, p)].at[slot], last)

    def finish(self, i):
        (kind, j), me, copies = ORDER[i], self.me, self.copies
        sums, cross, shares, outs = self.sums, self.cross, self.shares, self.outs
        mine = 2 * lax.rem(me.at["z"], 2) + me.core
        if kind == WIDE:
            copies.start((i, "rows"), lambda: (sums[WIDE].at[j, 1 - me.core], cross[WIDE].at[j], me.device(core=1 - me.core)))
        else:
            for q in range(4):
                shares[j, q] = sums[TALL][j, 10 * q : 10 * q + 10, :]
            for o in range(3):

                def make(o=o):
                    z, core = ((me.at["z"], 1 - me.core), (me.pair(), me.core), (me.pair(), 1 - me.core))[o]
                    mine = 2 * lax.rem(me.at["z"], 2) + me.core
                    return shares.at[j, 2 * lax.rem(z, 2) + core], cross[TALL].at[j, mine], me.device(core=core, z=z)

                copies.start((i, "rows", o), make)
        if i < 3:
            for d, n in SIZES.items():
                each(n - 1, lambda o, d=d: self.done(i, me.device(**{d: me.off(d, o + 1)})))
            self.done(i, me.device(core=1 - me.core))
        yield
        mine = 2 * lax.rem(me.at["z"], 2) + me.core
        if kind == WIDE:
            copies.arrived((i, "rows"))
            outs[0][j, me.core] = sums[WIDE][j, me.core]
            outs[0][j, 1 - me.core] = cross[WIDE][j]
        else:
            for o in range(3):
                copies.arrived((i, "rows", o))
            for q in range(4):
                outs[1][j, q] = jnp.where(q == mine, shares[j, q], cross[TALL][j, q])
        copies.sent(lambda key: key[0] == i)

    def done(self, i, device):
        pl.semaphore_signal(self.free.at[i], inc=1, device_id=device, device_id_type=MESH)

    def run(self, order):
        for i, c in zip(order[::2], order[1::2], strict=True):
            if c == "h":
                self.half(int(i))
            elif c == "s":
                self.half_sent(int(i))
            else:
                next(self.streams[int(i), int(c)], None)


def dot(a, b, ca=1, cb=0):
    return lax.dot_general(a, b, (((ca,), (cb,)), ((), ())), preferred_element_type=F32)


def rem(a, b):
    return a % b if isinstance(a, int) else lax.rem(a, b)


def at_tile(i, size):
    return pl.ds(pl.multiple_of(i * size, size), size)


def put_rows(ref, i, value):
    y, z, rows = ref.shape[1:4]
    for s in range(0, 256, 8):
        row = i * 256 + s
        group = lax.div(row, rows)
        ref[lax.div(group, y * z), rem(lax.div(group, z), y), rem(group, z), pl.ds(pl.multiple_of(rem(row, rows), 8), 8), :] = value[s : s + 8]


def put_all(ref, value):
    ref[...] = value.reshape(ref.shape)


def step_kernel(*refs):
    x_in, dy_in, w_gate, w_up, w_down = refs[:5]
    outs, (gate_kept, up_kept, a0_kept, h1_kept) = refs[5:7], refs[7:11]
    rest = list(refs[11:])
    take = lambda n: [rest.pop(0) for _ in range(n)]
    act, dy, turned, back, both, gates, ups = take(7)
    tile_g, tile_u, tile_d, rows_w, columns_w = take(5)
    wide_own, wide_theirs, tall_own, tall_half, tall_theirs = take(5)
    wide_sums, tall_sums, wide_cross, tall_cross, shares = take(5)
    load, sem_g, sem_u, sem_d, sem_w, sem_c, sem_f, send, recv, free = take(10)
    buffers = {}
    for kind in (WIDE, TALL):
        for k in reduce_buffers(kind):
            buffers[kind, k] = rest.pop(0)
    me = Me()

    def fetch(src, dst, sem):
        copy = pltpu.make_async_copy(src, dst, sem)
        copy.start()
        return copy

    class Stream:
        def __init__(self, tile, buffer, sem):
            self.tile, self.buffer, self.sem = tile, buffer, sem

        def copy(self, i):
            slot = rem(i, 2)
            return pltpu.make_async_copy(self.tile(i), self.buffer.at[slot], self.sem.at[slot])

    def stream(*streams, n):
        for s in streams:
            s.copy(0).start()

        def ahead(i):
            @pl.when(i + 1 < n)
            def _():
                for s in streams:
                    s.copy(i + 1).start()

            for s in streams:
                s.copy(i).wait()

        return ahead

    def columns(w, layer, buffer, sem):
        return Stream(lambda i: w.at[layer, :, at_tile(i, 256)], buffer, sem)

    loads = [fetch(x_in, back, load.at[0]), fetch(dy_in, dy, load.at[1])]
    zeroth = stream(columns(w_gate, 0, tile_g, sem_g), columns(w_up, 0, tile_u, sem_u), n=10)
    down = stream(columns(w_down, 0, columns_w, sem_c), n=4)
    me.barrier()
    own = {WIDE: wide_own, TALL: tall_own}
    theirs = {WIDE: wide_theirs, TALL: tall_theirs}
    halves = {WIDE: lambda: wide_own.at[2], TALL: lambda: tall_half}
    sums = {WIDE: wide_sums, TALL: tall_sums}
    cross = {WIDE: wide_cross, TALL: tall_cross}
    reduce = Reduce(me, own, theirs, halves, buffers, sums, cross, shares, outs, send, recv, free)

    def ticks(phase, i):
        orders = TICKS[phase]
        if any(orders):
            lax.switch(i, [functools.partial(reduce.run, order) for order in orders])

    def norm():
        @pl.loop(0, 8)
        def _(i):
            rows = at_tile(i, 128)
            h = back[rows, :].astype(F32)
            act[rows, :] = (h * lax.rsqrt(jnp.mean(h * h, -1, keepdims=True) + 1e-6)).astype(BF16)

    def turn(src):
        @pl.loop(0, 8)
        def _(i):
            turned[:, at_tile(i, 128)] = src[at_tile(i, 128), :].T

    def unit(i, g, u, d, dout):
        d = d.astype(BF16).astype(F32)
        s = jax.nn.sigmoid(g)
        silu = g * s
        value = (silu * u).astype(BF16).T
        both[1, :, at_tile(i, 256)] = (d * silu).astype(BF16)
        both[0, :, at_tile(i, 256)] = (d * u * (s * (1 + g * (1 - s)))).astype(BF16)
        for ref, core in ((tall_own.at[0], me.core), (tall_half, 1 - me.core)):
            put_rows(ref, i, dot(value, dout[:, at_tile(core, 512)]).astype(BF16))

    def wide_grads(phase):
        @pl.loop(0, 4)
        def _(k):
            which, mine = lax.div(k, 2), lax.rem(k, 2)
            core = mine * me.core + (1 - mine) * (1 - me.core)
            value = dot(turned[...], both[which, :, at_tile(core, 1280)]).astype(BF16)
            put_all(wide_own.at[lax.rem(2 - mine * (2 - which), 3)], value)
            ticks(phase, k)

    def kept(i, out):
        slot = rem(i, 2)
        pairs = (gates.at[slot], gate_kept.at[:, at_tile(i, 256)]), (ups.at[slot], up_kept.at[:, at_tile(i, 256)])
        return [pltpu.make_async_copy(*(p if out else p[::-1]), sem_f.at[n, slot]) for n, p in enumerate(pairs)]

    for copy in loads:
        copy.wait()
    norm()
    keep = fetch(act, a0_kept, load.at[0])

    @pl.loop(0, 10)
    def _(i):
        zeroth(i)

        @pl.when(i >= 2)
        def _():
            for copy in kept(i - 2, True):
                copy.wait()

        slot = rem(i, 2)
        g, u = dot(act[...], tile_g[slot]), dot(act[...], tile_u[slot])
        gates[slot] = g
        ups[slot] = u
        both[0, :, at_tile(i, 256)] = (g * jax.nn.sigmoid(g) * u).astype(BF16)
        for copy in kept(i, True):
            copy.start()

    first = stream(
        columns(w_gate, 1, tile_g, sem_g),
        columns(w_up, 1, tile_u, sem_u),
        Stream(lambda i: w_down.at[1, at_tile(i, 256), :], tile_d, sem_d),
        n=10,
    )

    @pl.loop(0, 4)
    def _(i):
        down(i)
        part = dot(both[0], columns_w[rem(i, 2)]).astype(BF16).astype(F32)
        back[:, at_tile(i, 256)] = (back[:, at_tile(i, 256)].astype(F32) + part).astype(BF16)

    keep.wait()
    keep = fetch(back, h1_kept, load.at[0])
    norm()
    turn(act)

    @pl.loop(0, 10)
    def _(i):
        first(i)
        slot = rem(i, 2)
        unit(i, dot(act[...], tile_g[slot]), dot(act[...], tile_u[slot]), dot(dy[...], tile_d[slot], 1, 1), dy)

    reduce.run(TICKS["first"][0])
    wide_grads("wide1")

    keep.wait()
    for i in (8, 9):
        for copy in kept(i, True):
            copy.wait()
    load_h = fetch(h1_kept, turned, load.at[0])

    def weight_rows(k, w):
        slot = rem(k, 2)
        rows = at_tile(k // 2 if isinstance(k, int) else lax.div(k, 2), 256)
        return pltpu.make_async_copy(w.at[1, rows, :], rows_w.at[slot], sem_w.at[slot])

    weight_rows(0, w_gate).start()

    @pl.loop(0, 8)
    def _(k):
        n, which = lax.div(k, 2), lax.rem(k, 2)

        @pl.when(which == 0)
        def _():
            weight_rows(k + 1, w_up).start()

        @pl.when((which == 1) & (k < 7))
        def _():
            weight_rows(k + 1, w_gate).start()

        weight_rows(k, w_gate).wait()
        part = dot(both[which], rows_w[which], 1, 1).astype(BF16).astype(F32)
        before = back[:, at_tile(n, 256)].astype(F32)
        back[:, at_tile(n, 256)] = (jnp.where(which == 0, 0.0, before) + part).astype(BF16)
        ticks("back", k)

    load_h.wait()

    @pl.loop(0, 8)
    def _(i):
        rows = at_tile(i, 128)
        h, d = turned[rows, :].astype(F32), back[rows, :].astype(F32)
        scale = lax.rsqrt(jnp.mean(h * h, -1, keepdims=True) + 1e-6)
        along = jnp.sum(d * h, -1, keepdims=True)
        d = (d * scale - h * (scale * scale * scale * along * (1 / 1024))).astype(BF16)
        act[rows, :] = (dy[rows, :].astype(F32) + d.astype(F32)).astype(BF16)

    load_a = fetch(a0_kept, back, load.at[1])
    second = stream(Stream(lambda i: w_down.at[0, at_tile(i, 256), :], tile_d, sem_d), n=10)
    for copy in kept(0, False):
        copy.start()
    load_a.wait()
    turn(back)

    @pl.loop(0, 10)
    def _(i):
        @pl.when(i < 9)
        def _():
            for copy in kept(i + 1, False):
                copy.start()

        second(i)
        for copy in kept(i, False):
            copy.wait()
        slot = rem(i, 2)
        unit(i, gates[slot], ups[slot], dot(act[...], tile_d[slot], 1, 1), act)
        ticks("units", i)

    reduce.run(TICKS["last"][0])
    wide_grads("wide0")
    reduce.run(TICKS["tail"][0])
    for stream_ in reduce.streams.values():
        assert next(stream_, 0) == 0, "not done"
    reduce.copies.sent()


def run(streams, order):
    for i, c in zip(order[::2], order[1::2], strict=True):
        next(streams[int(i), int(c)], None)
    for stream in streams.values():
        assert next(stream, 0) == 0, "not done"


def full_shape(kind):
    return dims(kind, ("x", "y", "z")) + (ROWS[kind], HALF[kind])


def summed(x, dy, w_gate, w_up, w_down):
    square = pltpu.VMEM((1024, 1024), BF16)
    scratch = [square] * 4 + [pltpu.VMEM((2, 1024, 2560), BF16)]
    scratch += [pltpu.VMEM((2, 1024, 256), F32)] * 2
    scratch += [pltpu.VMEM((2, 1024, 256), BF16)] * 2 + [pltpu.VMEM((2, 256, 1024), BF16), pltpu.VMEM((2, 256, 2560), BF16)]
    scratch += [
        pltpu.VMEM((2, 2560, 256), BF16),
        pltpu.VMEM((3, *full_shape(WIDE)), BF16),
        pltpu.VMEM((2, *full_shape(WIDE)), BF16),
        pltpu.VMEM((1, *full_shape(TALL)), BF16),
        pltpu.VMEM(full_shape(TALL), BF16),
        pltpu.VMEM((1, *full_shape(TALL)), BF16),
        pltpu.VMEM((4, 2, 4, 1280), F32),
        pltpu.VMEM((2, 40, 256), F32),
        pltpu.VMEM((4, 4, 1280), F32),
        pltpu.VMEM((2, 4, 10, 256), F32),
        pltpu.VMEM((2, 4, 10, 256), F32),
        *[pltpu.SemaphoreType.DMA((2,))] * 6,
        pltpu.SemaphoreType.DMA((2, 2)),
        pltpu.SemaphoreType.DMA((256,)),
        pltpu.SemaphoreType.DMA((256,)),
        pltpu.SemaphoreType.REGULAR((3,)),
    ]
    for kind, many in ((WIDE, 2), (TALL, 1)):
        scratch += [pltpu.VMEM((many, *shape), BF16) for shape in reduce_buffers(kind).values()]
    kept = [jax.ShapeDtypeStruct((1024, 2560), F32)] * 2 + [jax.ShapeDtypeStruct((1024, 1024), BF16)] * 2
    return pl.pallas_call(
        step_kernel,
        out_shape=(jax.ShapeDtypeStruct((4, 2, 4, 1280), F32), jax.ShapeDtypeStruct((2, 4, 10, 256), F32), *kept),
        in_specs=[pl.BlockSpec(memory_space=pl.ANY)] * 5,
        out_specs=(*[pl.BlockSpec(memory_space=pltpu.VMEM)] * 2, *[pl.BlockSpec(memory_space=pl.ANY)] * 4),
        scratch_shapes=scratch,
        compiler_params=pltpu.CompilerParams(collective_id=0, has_side_effects=True, vmem_limit_bytes=VMEM_LIMIT),
        name="step",
    )(x, dy, w_gate, w_up, w_down)[:2]


def gather_colour(me, copies, key, kind, colour, ref):
    base = me.core * HALF[kind]
    fixed = dict(me.at)

    def part(at):
        return view(ref, kind, ("x", "y", "z"), at, colour, base)

    phases = COLOURS[colour][::-1]
    for phase, (d, how) in enumerate(phases):
        n, lastly = SIZES[d], phase == len(phases) - 1
        rest = {e: v for e, v in fixed.items() if e != d}
        here = part(fixed)

        def across(name, at):
            if lastly:
                copies.start((key, colour, "across", name), lambda: (part(at), part(at), me.device(core=1 - me.core)))

        if how == RING:
            long, short = lengths(n)
            ways = ((me.sign, long, "l"), (-me.sign, short, "s"))
            for s in range(long):
                for sign, length, name in ways:
                    if s >= length:
                        continue
                    at = {**rest, d: me.off(d, -sign * s)}
                    if s:
                        copies.arrived((key, colour, phase, name, s - 1))
                    copies.start(
                        (key, colour, phase, name, s),
                        lambda at=at, d=d, sign=sign: (part(at), part(at), me.device(**{d: me.off(d, sign)})),
                    )
                    if s:
                        across((name, s - 1), at)
                if s == 0:
                    across("own", fixed)
                yield
            for sign, length, name in ways:
                if length:
                    copies.arrived((key, colour, phase, name, length - 1))
                    across((name, length - 1), {**rest, d: me.off(d, -sign * length)})
        else:
            copies.start_all(
                (key, colour, phase), n - 1, lambda i, d=d, here=here: (here, here, me.device(**{d: me.off(d, i + 1)}))
            )
            yield
            copies.arrived((key, colour, phase))
        fixed = rest
    yield
    names = ["own"]
    d, how = phases[-1]
    long, short = lengths(SIZES[d])
    names += [("l", s) for s in range(long)] + [("s", s) for s in range(short)]
    for name in names:
        copies.arrived((key, colour, "across", name))


def gather_kernel(*refs):
    wide, tall, outs, rest = refs[0], refs[1], refs[2:8], refs[8:]
    cross = {WIDE: rest[0], TALL: rest[1]}
    forty, send, recv = rest[2:5]
    me = Me()
    me.barrier()
    copies = Copies(send, recv)
    mine = 2 * lax.rem(me.at["z"], 2) + me.core

    for i, (kind, j) in enumerate(ORDER):
        if kind == WIDE:
            copies.start((i, "rows"), lambda j=j: (wide.at[j, 1 - me.core], cross[WIDE].at[j], me.device(core=1 - me.core)))
        else:
            for o, (z, core) in enumerate(((me.at["z"], 1 - me.core), (me.pair(), me.core), (me.pair(), 1 - me.core))):
                q = 2 * lax.rem(z, 2) + core
                copies.start(
                    (i, "rows", o),
                    lambda j=j, q=q, z=z, core=core: (tall.at[j, q], cross[TALL].at[j, mine], me.device(core=core, z=z)),
                )

    def begin(i):
        kind, j = ORDER[i]
        here = view(outs[i], kind, ("x", "y", "z"), me.at, None, me.core * HALF[kind])
        if kind == WIDE:
            copies.arrived((i, "rows"))
            own, theirs = wide[j, me.core], cross[WIDE][j]
            first = me.core == 0
            rows = [jnp.where(first, own, theirs), jnp.where(first, theirs, own)]
            here[...] = jnp.concatenate(rows, axis=0).astype(BF16)
        else:
            for o in range(3):
                copies.arrived((i, "rows", o))
            for q in range(4):
                forty[10 * q : 10 * q + 10, :] = jnp.where(q == mine, tall[j, q], cross[TALL][j, q])
            here[...] = forty[...].astype(BF16)

    def colour(i, c):
        if i in waiting:
            waiting.discard(i)
            begin(i)
        yield from gather_colour(me, copies, i, ORDER[i][0], c, outs[i])

    waiting = set(range(6))
    run({(i, c): colour(i, c) for i in range(6) for c in range(3)}, GATHER_ORDER)
    copies.sent()


def all_gather(wide, tall):
    scratch = [
        pltpu.VMEM((4, 4, 1280), F32),
        pltpu.VMEM((2, 4, 10, 256), F32),
        pltpu.VMEM((40, 256), F32),
        pltpu.SemaphoreType.DMA((384,)),
        pltpu.SemaphoreType.DMA((384,)),
    ]
    return pl.pallas_call(
        gather_kernel,
        out_shape=tuple(pltpu.VMEM((*dims(kind, ("x", "y", "z")), ROWS[kind], 2 * HALF[kind]), BF16) for kind, _ in ORDER),
        in_specs=[pl.BlockSpec(memory_space=pltpu.VMEM)] * 2,
        out_specs=(pl.BlockSpec(memory_space=pltpu.VMEM),) * 6,
        scratch_shapes=scratch,
        compiler_params=pltpu.CompilerParams(collective_id=1, has_side_effects=True, vmem_limit_bytes=4 * 1024 * 1024),
        name="all_gather",
    )(wide, tall)


def spill_kernel(*refs):
    ins, outs, sem = refs[:6], refs[6:9], refs[9]
    copies = []
    for i, (kind, j) in enumerate(ORDER):
        which, layer = (2, j) if kind == TALL else (j // 2, j % 2)
        copies.append(pltpu.make_async_copy(ins[i], outs[which].at[layer], sem.at[i]))
        copies[-1].start()
    for copy in copies:
        copy.wait()


def spill(new):
    wide, tall = ((2, *dims(kind, ("x", "y", "z")), ROWS[kind], 2 * HALF[kind]) for kind in (WIDE, TALL))
    return pl.pallas_call(
        spill_kernel,
        out_shape=tuple(jax.ShapeDtypeStruct(shape, BF16) for shape in (wide, wide, tall)),
        in_specs=[pl.BlockSpec(memory_space=pltpu.VMEM)] * 6,
        out_specs=(pl.BlockSpec(memory_space=pl.ANY),) * 3,
        scratch_shapes=[pltpu.SemaphoreType.DMA((6,))],
        compiler_params=pltpu.CompilerParams(vmem_limit_bytes=1024 * 1024),
        name="spill",
    )(*new)


def adamw(w, m, v, g):
    m = 0.9 * m + 0.1 * g
    v = 0.95 * v + 0.05 * g * g
    step = m * lax.rsqrt(v + 1e-8) + 0.1 * w
    return (w - 0.02 * step).astype(BF16), m, v


def rows_of(wide, tall):
    wide = wide.transpose(0, 2, 1, 3).reshape(2, 2, 4, 2560)
    tall = tall.reshape(2, 2, 2, 10, 256).transpose(0, 3, 2, 1, 4).reshape(2, 10, 1024)
    return wide[0], wide[1], tall


def gathered(gate, up, down):
    wide = jnp.stack([gate, up]).reshape(4, 4, 2, 1280).transpose(0, 2, 1, 3).astype(F32)
    tall = down.reshape(2, 10, 2, 2, 256).transpose(0, 3, 2, 1, 4).reshape(2, 4, 10, 256).astype(F32)
    new = spill(all_gather(wide, tall))
    return tuple(w.reshape(2, -1, w.shape[-1]) for w in new)


def solution(mesh):
    def step(x, dy, *arrays):
        weights, m, v = (arrays[i : i + 3] for i in (0, 3, 6))
        gradients = rows_of(*summed(x[0], dy[0], *weights))
        index = lax.axis_index("dp")
        news = []
        for w, mm, vv, g in zip(weights, m, v, gradients, strict=True):
            rows = mm.shape[1]
            mine = lax.dynamic_slice_in_dim(w, index * rows, rows, 1)
            news.append(adamw(mine.astype(F32), mm, vv, g))
        new = gathered(*(n[0] for n in news))
        return (*new, *(n[1] for n in news), *(n[2] for n in news))

    batch, whole, rows = P(("rep", "dp")), P(), P(None, "dp")
    return jax.shard_map(
        step,
        mesh=mesh,
        in_specs=(batch, batch, *(whole,) * 3, *(rows,) * 6),
        out_specs=(*(P("rep"),) * 3, *(P("rep", "dp"),) * 6),
        check_vma=False,
    )
```

```python
import functools

import jax
import jax.numpy as jnp
from jax import lax
from jax.experimental import pallas as pl
from jax.experimental.pallas import tpu as pltpu
from jax.sharding import PartitionSpec as P

NAMES = ("w_gate", "w_up", "w_down")
MESH = pl.DeviceIdType.MESH
F32, BF16 = jnp.float32, jnp.bfloat16
SIZES = {"x": 4, "y": 4, "z": 8}
VMEM_LIMIT = 64 * 1024 * 1024 - 64 * 1024

TICKS = {
    "first": ["0h"],
    "wide1": ["1h", "1s020100", "2h121110", "0200"],
    "back": ["0112222120", "", "02111000", "12", "0122", "022120", "121100", "01102221020s"],
    "units": ["010012021110222120", "", "0211121021222001", "0003", "122022", "03111013", "132221", "2023", "23", ""],
    "last": ["3h"],
    "wide0": ["4h", "4s323130", "5h424140", "3230"],
    "tail": ["42523151504041324230523150325142413040315251323042405041523151403050324142515250324231335240414333514350525353"],
}
GATHER_ORDER = "020100121110222120323130424140525150021222324252010011021000122122203210420031520130112120411040300051203150014002301121124150223210014240005251000211122120225031323001414201115211100210214012512122203132422052500241301202302251124022324240313252425031524150415151"


RING, DIRECT = "ring", "direct"
COLOURS = (
    (("x", RING), ("y", RING), ("z", DIRECT)),
    (("y", RING), ("x", RING), ("z", DIRECT)),
    (("z", RING), ("x", DIRECT), ("y", DIRECT)),
)
WIDE, TALL = "wide", "tall"
PART = {WIDE: ((0, 512), (512, 384), (896, 384)), TALL: ((0, 8), (8, 16), (24, 16))}
HALF = {WIDE: 1280, TALL: 512}
ROWS = {WIDE: 8, TALL: 40}
ORDER = ((TALL, 1), (WIDE, 1), (WIDE, 3), (TALL, 0), (WIDE, 0), (WIDE, 2))


class Me:
    def __init__(self):
        index = lax.axis_index("dp")
        Me.zero = index * 0
        self.core = lax.rem(index, 2)
        chip = index // 2
        self.at = {
            "z": lax.rem(chip, SIZES["z"]),
            "y": lax.rem(chip // SIZES["z"], SIZES["y"]),
            "x": chip // (SIZES["z"] * SIZES["y"]),
        }
        self.sign = 1 - 2 * self.core

    def off(self, d, by):
        return lax.rem(self.at[d] + by + SIZES[d], SIZES[d])

    def device(self, core=None, **at):
        at = {**self.at, **at}
        core = self.core if core is None else core
        return (0, ((at["x"] * SIZES["y"] + at["y"]) * SIZES["z"] + at["z"]) * 2 + core)

    def barrier(self):
        sem = pltpu.get_barrier_semaphore()

        def signal(peer):
            pl.semaphore_signal(sem, inc=1, device_id=peer, device_id_type=MESH)

        for d, n in SIZES.items():
            each(n - 1, lambda i, d=d: signal(self.device(**{d: self.off(d, i + 1)})))
        signal(self.device(core=1 - self.core))
        signal(self.device(core=1 - self.core, z=self.pair()))
        pl.semaphore_wait(sem, sum(SIZES.values()) - 1)

    def pair(self):
        return self.at["z"] + 1 - 2 * lax.rem(self.at["z"], 2)


def dims(kind, free):
    return tuple(SIZES[d] // (2 if kind == TALL and d == "z" else 1) for d in free)


def view(ref, kind, free, fixed, colour=None, base=0, own=False):
    index = [(fixed[d] // 2 if kind == TALL and d == "z" else fixed[d]) if d in fixed else slice(None) for d in free]
    if own and not (kind == TALL and "z" in free and "z" in fixed):
        return ref.at[(*index, slice(None), slice(None))]
    if kind == WIDE:
        first, size = (0, HALF[WIDE]) if colour is None else PART[WIDE][colour]
        rows, columns = slice(None), pl.ds(_at(base, first), size)
    else:
        rows = slice(None) if own or colour is None else pl.ds(*PART[TALL][colour])
        if "z" in free and "z" in fixed:
            columns = pl.ds(pl.multiple_of(base + lax.rem(fixed["z"], 2) * 256, 256), 256)
        else:
            columns = pl.ds(_at(base, 0), HALF[TALL])
    return ref.at[(*index, rows, columns)]


def _at(base, first):
    return first if isinstance(base, int) and base == 0 else pl.multiple_of(base + first, 128)


def block(kind, colour, free):
    first, size = PART[kind][colour]
    tail = (8, size) if kind == WIDE else (size, HALF[TALL] if "z" in free else HALF[TALL] // 2)
    return dims(kind, free) + tail


def lengths(n):
    return n // 2, (n - 1) // 2


def reduce_buffers(kind):
    shapes = {}
    for c, phases in enumerate(COLOURS):
        free = ["x", "y", "z"]
        for p, (d, how) in enumerate(phases):
            free.remove(d)
            shape = block(kind, c, tuple(free))
            count = SIZES[d] - 1
            shapes[c, p] = (count, *shape)
    return shapes


class Copies:
    def __init__(self, send, recv):
        self.send, self.recv, self.all, self.used, self.left = send, recv, {}, 0, set()

    def start(self, key, make):
        self.start_all(key, 1, lambda i: make())

    def start_all(self, key, count, make):
        first = self.used
        self.used += count

        def copy(i):
            src, dst, to = make(i)
            return pltpu.make_async_remote_copy(
                src_ref=src, dst_ref=dst, send_sem=self.send.at[first + i], recv_sem=self.recv.at[first + i], device_id=to, device_id_type=MESH
            )

        self.all[key] = count, copy
        each(count, lambda i: copy(i).start())

    def arrived(self, key):
        count, copy = self.all[key]
        each(count, lambda i: copy(i).wait_recv())

    def sent(self, mine=lambda key: True):
        for key, (count, copy) in self.all.items():
            if key not in self.left and mine(key):
                self.left.add(key)
                each(count, lambda i, copy=copy: copy(i).wait_send())


def each(count, do):
    if count == 1:
        do(0)
    else:

        loop(count)(do)


def loop(count):
    def run(body):
        def step(carry, _):
            body(carry[0])
            return (carry[0] + 1, None), None

        lax.scan(step, (Me.zero, None), None, length=count)

    return run


def total(parts):
    return functools.reduce(jnp.add, [p[...].astype(F32) for p in parts])


def reduce_colour(me, copies, key, kind, colour, grads, received, last, keep=None):
    free, fixed = ("x", "y", "z"), {}
    parts = [lambda at, r=r: view(r(), kind, ("x", "y", "z"), at, colour) for r in grads]
    out = parts[0]

    def add(at, more):
        rest = [d for d in free if d not in at]
        if len(rest) >= 2:
            first = rest[0]

            @loop(SIZES[first])
            def _(i):
                now = {**at, first: i}
                out(now)[...] = total([p(now) for p in parts + more]).astype(BF16)
        else:
            out(at)[...] = total([p(at) for p in parts + more]).astype(BF16)

    for phase, (d, how) in enumerate(COLOURS[colour]):
        n, buffer = SIZES[d], functools.partial(received, colour, phase)
        left = tuple(e for e in ("x", "y", "z") if e not in fixed and e != d)

        def slot(i, buffer=buffer, left=left):
            return lambda at: view(buffer().at[i], kind, left, {e: v for e, v in at.items() if e in left}, colour, own=True)

        if how == RING:
            long, short = lengths(n)
            ways = ((1, long, 0, "l"), (-1, short, long, "s"))
            for s in range(long):
                for sign, length, base, name in ways:
                    if s >= length:
                        continue

                    def make(d=d, fixed=fixed, buffer=buffer, sign=sign, by=length - s, place=base + s):
                        at = {**fixed, d: me.off(d, me.sign * (sign * by))}
                        return out(at), buffer().at[place], me.device(**{d: me.off(d, me.sign * sign)})

                    if s:
                        copies.arrived((key, colour, phase, name, s - 1))
                    add({**fixed, d: me.off(d, me.sign * (sign * (length - s)))}, [slot(base + s - 1)] if s else [])
                    copies.start((key, colour, phase, name, s), make)
                yield
            for sign, length, base, name in ways:
                if length:
                    copies.arrived((key, colour, phase, name, length - 1))
            parts = parts + [slot(base + length - 1) for sign, length, base, name in ways if length]
        else:

            def make(i, d=d, fixed=fixed, buffer=buffer, add=add, out=out):
                to = me.off(d, i + 1)
                return out({**fixed, d: to}), buffer().at[i], me.device(**{d: to})

            each(n - 1, lambda i: add({**fixed, d: me.off(d, i + 1)}, []))
            copies.start_all((key, colour, phase), n - 1, make)
            yield
            copies.arrived((key, colour, phase))
            parts = parts + [slot(i) for i in range(n - 1)]
        fixed = {**fixed, d: me.at[d]}
        if keep is not None and phase == 0:
            copies.sent(lambda k: k[:3] == (key, colour, 0))
            stays = (lambda at, left=left: view(keep, kind, left, {e: v for e, v in at.items() if e in left}, colour, own=True))
            stays(fixed)[...] = out(fixed)[...]
            out = stays
            parts[0] = stays
    last(colour, total([p(fixed) for p in parts]).astype(BF16).astype(F32))


class Reduce:
    def __init__(self, me, own, theirs, halves, buffers, sums, cross, shares, outs, send, recv, free, kept):
        self.me, self.own, self.theirs, self.halves, self.buffers = me, own, theirs, halves, buffers
        self.sums, self.cross, self.shares, self.outs, self.free, self.kept = sums, cross, shares, outs, free, kept
        self.copies = Copies(send, recv)
        self.waiting = set(range(6))
        self.streams = {(i, c): self.colour(i, c) for i in range(6) for c in range(3)} | {(i, 3): self.finish(i) for i in range(6)}

    def slot(self, i):
        kind, j = ORDER[i]
        return 0 if kind == TALL else j // 2

    def half(self, i):
        kind = ORDER[i][0]
        if i >= 3:
            pl.semaphore_wait(self.free.at[i - 3], sum(SIZES.values()) - len(SIZES) + 1)
        self.copies.start(
            (i, "half"), lambda: (self.halves[kind](), self.theirs[kind].at[self.slot(i)], self.me.device(core=1 - self.me.core))
        )

    def half_sent(self, i):
        self.copies.sent(lambda key: key == (i, "half"))

    def colour(self, i, c):
        kind, j = ORDER[i]
        slot = self.slot(i)
        if i in self.waiting:
            self.waiting.discard(i)
            self.copies.arrived((i, "half"))

        def last(colour, value):
            first, size = PART[kind][colour]
            if kind == WIDE:
                self.sums[WIDE][j, 0, :, first : first + size] = value[:4]
                self.sums[WIDE][j, 1, :, first : first + size] = value[4:]
            else:
                self.sums[TALL][j, first : first + size, :] = value

        grads = (lambda: self.own[kind].at[slot]), (lambda: self.theirs[kind].at[slot])
        keep = self.kept[c] if i == 0 else None
        yield from reduce_colour(self.me, self.copies, i, kind, c, grads, lambda c, p: self.buffers[kind, (c, p)].at[slot], last, keep)

    def finish(self, i):
        (kind, j), me, copies = ORDER[i], self.me, self.copies
        sums, cross, shares, outs = self.sums, self.cross, self.shares, self.outs
        mine = 2 * lax.rem(me.at["z"], 2) + me.core
        if kind == WIDE:
            copies.start((i, "rows"), lambda: (sums[WIDE].at[j, 1 - me.core], cross[WIDE].at[j], me.device(core=1 - me.core)))
        else:
            for q in range(4):
                shares[j, q] = sums[TALL][j, 10 * q : 10 * q + 10, :]
            for o in range(3):

                def make(o=o):
                    z, core = ((me.at["z"], 1 - me.core), (me.pair(), me.core), (me.pair(), 1 - me.core))[o]
                    mine = 2 * lax.rem(me.at["z"], 2) + me.core
                    return shares.at[j, 2 * lax.rem(z, 2) + core], cross[TALL].at[j, mine], me.device(core=core, z=z)

                copies.start((i, "rows", o), make)
        if i < 3:
            for d, n in SIZES.items():
                each(n - 1, lambda o, d=d: self.done(i, me.device(**{d: me.off(d, o + 1)})))
            self.done(i, me.device(core=1 - me.core))
        yield
        mine = 2 * lax.rem(me.at["z"], 2) + me.core
        if kind == WIDE:
            copies.arrived((i, "rows"))
            outs[0][j, me.core] = sums[WIDE][j, me.core]
            outs[0][j, 1 - me.core] = cross[WIDE][j]
        else:
            for o in range(3):
                copies.arrived((i, "rows", o))
            for q in range(4):
                outs[1][j, q] = jnp.where(q == mine, shares[j, q], cross[TALL][j, q])
        copies.sent(lambda key: key[0] == i)

    def done(self, i, device):
        pl.semaphore_signal(self.free.at[i], inc=1, device_id=device, device_id_type=MESH)

    def run(self, order):
        for i, c in zip(order[::2], order[1::2], strict=True):
            if c == "h":
                self.half(int(i))
            elif c == "s":
                self.half_sent(int(i))
            else:
                next(self.streams[int(i), int(c)], None)


def dot(a, b, ca=1, cb=0):
    return lax.dot_general(a, b, (((ca,), (cb,)), ((), ())), preferred_element_type=F32)


def rem(a, b):
    return a % b if isinstance(a, int) else lax.rem(a, b)


def at_tile(i, size):
    return pl.ds(pl.multiple_of(i * size, size), size)


def put_rows(ref, i, value):
    y, z, rows = ref.shape[1:4]
    for s in range(0, 256, 8):
        row = i * 256 + s
        group = lax.div(row, rows)
        ref[lax.div(group, y * z), rem(lax.div(group, z), y), rem(group, z), pl.ds(pl.multiple_of(rem(row, rows), 8), 8), :] = value[s : s + 8]


def put_all(ref, value):
    ref[...] = value.reshape(ref.shape)


def step_kernel(*refs):
    x_in, dy_in, w_gate, w_up, w_down = refs[:5]
    outs, (gate_kept, up_kept, a0_kept, h1_kept) = refs[5:7], refs[7:11]
    rest = list(refs[11:])
    take = lambda n: [rest.pop(0) for _ in range(n)]
    act, dy, turned, back, both, gates, ups = take(7)
    tile_g, tile_u, tile_d, rows_w, columns_w = take(5)
    wide_own, wide_theirs, tall_own, tall_half, tall_theirs = take(5)
    wide_sums, tall_sums, wide_cross, tall_cross, shares = take(5)
    load, sem_g, sem_u, sem_d, sem_w, sem_c, sem_f, send, recv, free = take(10)
    buffers = {}
    for kind in (WIDE, TALL):
        for k in reduce_buffers(kind):
            buffers[kind, k] = rest.pop(0)
    tall_kept = take(3)
    me = Me()

    def fetch(src, dst, sem):
        copy = pltpu.make_async_copy(src, dst, sem)
        copy.start()
        return copy

    class Stream:
        def __init__(self, tile, buffer, sem):
            self.tile, self.buffer, self.sem = tile, buffer, sem

        def copy(self, i):
            slot = rem(i, 2)
            return pltpu.make_async_copy(self.tile(i), self.buffer.at[slot], self.sem.at[slot])

    def stream(*streams, n):
        for s in streams:
            s.copy(0).start()

        def ahead(i):
            @pl.when(i + 1 < n)
            def _():
                for s in streams:
                    s.copy(i + 1).start()

            for s in streams:
                s.copy(i).wait()

        return ahead

    def columns(w, layer, buffer, sem):
        return Stream(lambda i: w.at[layer, :, at_tile(i, 256)], buffer, sem)

    loads = [fetch(x_in, back, load.at[0]), fetch(dy_in, dy, load.at[1])]
    zeroth = stream(columns(w_gate, 0, tile_g, sem_g), columns(w_up, 0, tile_u, sem_u), n=10)

    def half_columns(i, half):
        src = w_down.at[0, pl.ds(half * 1280, 1280), at_tile(i, 256)]
        return pltpu.make_async_copy(src, columns_w.at[half], sem_c.at[half])

    for half in (0, 1):
        half_columns(0, half).start()
    me.barrier()
    own = {WIDE: wide_own, TALL: tall_own}
    theirs = {WIDE: wide_theirs, TALL: tall_theirs}
    halves = {WIDE: lambda: wide_own.at[2], TALL: lambda: tall_half}
    sums = {WIDE: wide_sums, TALL: tall_sums}
    cross = {WIDE: wide_cross, TALL: tall_cross}
    reduce = Reduce(me, own, theirs, halves, buffers, sums, cross, shares, outs, send, recv, free, tall_kept)

    def ticks(phase, i):
        orders = TICKS[phase]
        if any(orders):
            lax.switch(i, [functools.partial(reduce.run, order) for order in orders])

    def norm():
        @pl.loop(0, 8)
        def _(i):
            rows = at_tile(i, 128)
            h = back[rows, :].astype(F32)
            act[rows, :] = (h * lax.rsqrt(jnp.mean(h * h, -1, keepdims=True) + 1e-6)).astype(BF16)

    def turn(src):
        @pl.loop(0, 8)
        def _(i):
            turned[:, at_tile(i, 128)] = src[at_tile(i, 128), :].T

    def unit(i, g, u, d, dout):
        d = d.astype(BF16).astype(F32)
        s = jax.nn.sigmoid(g)
        silu = g * s
        value = (silu * u).astype(BF16).T
        both[1, :, at_tile(i, 256)] = (d * silu).astype(BF16)
        both[0, :, at_tile(i, 256)] = (d * u * (s * (1 + g * (1 - s)))).astype(BF16)
        for ref, core in ((tall_own.at[0], me.core), (tall_half, 1 - me.core)):
            put_rows(ref, i, dot(value, dout[:, at_tile(core, 512)]).astype(BF16))

    def wide_grads(phase):
        @pl.loop(0, 4)
        def _(k):
            which, mine = lax.div(k, 2), lax.rem(k, 2)
            core = mine * me.core + (1 - mine) * (1 - me.core)
            value = dot(turned[...], both[which, :, at_tile(core, 1280)]).astype(BF16)
            put_all(wide_own.at[lax.rem(2 - mine * (2 - which), 3)], value)
            ticks(phase, k)

    def kept(i, out):
        slot = rem(i, 2)
        pairs = (gates.at[slot], gate_kept.at[:, at_tile(i, 256)]), (ups.at[slot], up_kept.at[:, at_tile(i, 256)])
        return [pltpu.make_async_copy(*(p if out else p[::-1]), sem_f.at[n, slot]) for n, p in enumerate(pairs)]

    for copy in loads:
        copy.wait()
    norm()
    keep = fetch(act, a0_kept, load.at[0])

    @pl.loop(0, 10)
    def _(i):
        zeroth(i)

        @pl.when(i >= 2)
        def _():
            for copy in kept(i - 2, True):
                copy.wait()

        slot = rem(i, 2)
        g, u = dot(act[...], tile_g[slot]), dot(act[...], tile_u[slot])
        gates[slot] = g
        ups[slot] = u
        both[0, :, at_tile(i, 256)] = (g * jax.nn.sigmoid(g) * u).astype(BF16)
        for copy in kept(i, True):
            copy.start()

    first = stream(
        columns(w_gate, 1, tile_g, sem_g),
        columns(w_up, 1, tile_u, sem_u),
        Stream(lambda i: w_down.at[1, at_tile(i, 256), :], tile_d, sem_d),
        n=10,
    )

    @pl.loop(0, 4)
    def _(i):
        part = 0.0
        for half in (0, 1):
            half_columns(i, half).wait()
            part += dot(both[0, :, half * 1280 : half * 1280 + 1280], columns_w[half])

            @pl.when(i < 3)
            def _():
                half_columns(i + 1, half).start()

        part = part.astype(BF16).astype(F32)
        back[:, at_tile(i, 256)] = (back[:, at_tile(i, 256)].astype(F32) + part).astype(BF16)

    keep.wait()
    keep = fetch(back, h1_kept, load.at[0])
    norm()
    turn(act)

    @pl.loop(0, 10)
    def _(i):
        first(i)
        slot = rem(i, 2)
        unit(i, dot(act[...], tile_g[slot]), dot(act[...], tile_u[slot]), dot(dy[...], tile_d[slot], 1, 1), dy)

    reduce.run(TICKS["first"][0])
    wide_grads("wide1")

    keep.wait()
    for i in (8, 9):
        for copy in kept(i, True):
            copy.wait()
    load_h = fetch(h1_kept, turned, load.at[0])

    def weight_rows(k, w):
        slot = rem(k, 2)
        rows = at_tile(k // 2 if isinstance(k, int) else lax.div(k, 2), 256)
        return pltpu.make_async_copy(w.at[1, rows, :], rows_w.at[slot], sem_w.at[slot])

    weight_rows(0, w_gate).start()

    @pl.loop(0, 8)
    def _(k):
        n, which = lax.div(k, 2), lax.rem(k, 2)

        @pl.when(which == 0)
        def _():
            weight_rows(k + 1, w_up).start()

        @pl.when((which == 1) & (k < 7))
        def _():
            weight_rows(k + 1, w_gate).start()

        weight_rows(k, w_gate).wait()
        part = dot(both[which], rows_w[which], 1, 1).astype(BF16).astype(F32)
        before = back[:, at_tile(n, 256)].astype(F32)
        back[:, at_tile(n, 256)] = (jnp.where(which == 0, 0.0, before) + part).astype(BF16)
        ticks("back", k)

    load_h.wait()

    @pl.loop(0, 8)
    def _(i):
        rows = at_tile(i, 128)
        h, d = turned[rows, :].astype(F32), back[rows, :].astype(F32)
        scale = lax.rsqrt(jnp.mean(h * h, -1, keepdims=True) + 1e-6)
        along = jnp.sum(d * h, -1, keepdims=True)
        d = (d * scale - h * (scale * scale * scale * along * (1 / 1024))).astype(BF16)
        act[rows, :] = (dy[rows, :].astype(F32) + d.astype(F32)).astype(BF16)

    load_a = fetch(a0_kept, back, load.at[1])
    second = stream(Stream(lambda i: w_down.at[0, at_tile(i, 256), :], tile_d, sem_d), n=10)
    for copy in kept(0, False):
        copy.start()
    load_a.wait()
    turn(back)

    @pl.loop(0, 10)
    def _(i):
        @pl.when(i < 9)
        def _():
            for copy in kept(i + 1, False):
                copy.start()

        second(i)
        for copy in kept(i, False):
            copy.wait()
        slot = rem(i, 2)
        unit(i, gates[slot], ups[slot], dot(act[...], tile_d[slot], 1, 1), act)
        ticks("units", i)

    reduce.run(TICKS["last"][0])
    wide_grads("wide0")
    reduce.run(TICKS["tail"][0])
    for stream_ in reduce.streams.values():
        assert next(stream_, 0) == 0, "not done"
    reduce.copies.sent()


def run(streams, order):
    for i, c in zip(order[::2], order[1::2], strict=True):
        next(streams[int(i), int(c)], None)
    for stream in streams.values():
        assert next(stream, 0) == 0, "not done"


def full_shape(kind):
    return dims(kind, ("x", "y", "z")) + (ROWS[kind], HALF[kind])


def summed(x, dy, w_gate, w_up, w_down):
    square = pltpu.VMEM((1024, 1024), BF16)
    scratch = [square] * 4 + [pltpu.VMEM((2, 1024, 2560), BF16)]
    scratch += [pltpu.VMEM((2, 1024, 256), F32)] * 2
    scratch += [pltpu.VMEM((2, 1024, 256), BF16)] * 2 + [pltpu.VMEM((2, 256, 1024), BF16), pltpu.VMEM((2, 256, 2560), BF16)]
    scratch += [
        pltpu.VMEM((2, 1280, 256), BF16),
        pltpu.VMEM((3, *full_shape(WIDE)), BF16),
        pltpu.VMEM((2, *full_shape(WIDE)), BF16),
        pltpu.VMEM((1, *full_shape(TALL)), BF16),
        pltpu.VMEM(full_shape(TALL), BF16),
        pltpu.VMEM((1, *full_shape(TALL)), BF16),
        pltpu.VMEM((4, 2, 4, 1280), F32),
        pltpu.VMEM((2, 40, 256), F32),
        pltpu.VMEM((4, 4, 1280), F32),
        pltpu.VMEM((2, 4, 10, 256), F32),
        pltpu.VMEM((2, 4, 10, 256), F32),
        *[pltpu.SemaphoreType.DMA((2,))] * 6,
        pltpu.SemaphoreType.DMA((2, 2)),
        pltpu.SemaphoreType.DMA((256,)),
        pltpu.SemaphoreType.DMA((256,)),
        pltpu.SemaphoreType.REGULAR((3,)),
    ]
    for kind, many in ((WIDE, 2), (TALL, 1)):
        scratch += [pltpu.VMEM((many, *shape), BF16) for shape in reduce_buffers(kind).values()]
    scratch += [pltpu.VMEM(block(TALL, c, [d for d in "xyz" if d != COLOURS[c][0][0]]), BF16) for c in range(3)]
    kept = [jax.ShapeDtypeStruct((1024, 2560), F32)] * 2 + [jax.ShapeDtypeStruct((1024, 1024), BF16)] * 2
    return pl.pallas_call(
        step_kernel,
        out_shape=(jax.ShapeDtypeStruct((4, 2, 4, 1280), F32), jax.ShapeDtypeStruct((2, 4, 10, 256), F32), *kept),
        in_specs=[pl.BlockSpec(memory_space=pl.ANY)] * 5,
        out_specs=(*[pl.BlockSpec(memory_space=pltpu.VMEM)] * 2, *[pl.BlockSpec(memory_space=pl.ANY)] * 4),
        scratch_shapes=scratch,
        compiler_params=pltpu.CompilerParams(collective_id=0, has_side_effects=True, vmem_limit_bytes=VMEM_LIMIT),
        name="step",
    )(x, dy, w_gate, w_up, w_down)[:2]


def gather_colour(me, copies, key, kind, colour, ref):
    base = me.core * HALF[kind]
    fixed = dict(me.at)

    def part(at):
        return view(ref, kind, ("x", "y", "z"), at, colour, base)

    phases = COLOURS[colour][::-1]
    for phase, (d, how) in enumerate(phases):
        n, lastly = SIZES[d], phase == len(phases) - 1
        rest = {e: v for e, v in fixed.items() if e != d}
        here = part(fixed)

        def across(name, at):
            if lastly:
                copies.start((key, colour, "across", name), lambda: (part(at), part(at), me.device(core=1 - me.core)))

        if how == RING:
            long, short = lengths(n)
            ways = ((me.sign, long, "l"), (-me.sign, short, "s"))
            for s in range(long):
                for sign, length, name in ways:
                    if s >= length:
                        continue
                    at = {**rest, d: me.off(d, -sign * s)}
                    if s:
                        copies.arrived((key, colour, phase, name, s - 1))
                    copies.start(
                        (key, colour, phase, name, s),
                        lambda at=at, d=d, sign=sign: (part(at), part(at), me.device(**{d: me.off(d, sign)})),
                    )
                    if s:
                        across((name, s - 1), at)
                if s == 0:
                    across("own", fixed)
                yield
            for sign, length, name in ways:
                if length:
                    copies.arrived((key, colour, phase, name, length - 1))
                    across((name, length - 1), {**rest, d: me.off(d, -sign * length)})
        else:
            copies.start_all(
                (key, colour, phase), n - 1, lambda i, d=d, here=here: (here, here, me.device(**{d: me.off(d, i + 1)}))
            )
            yield
            copies.arrived((key, colour, phase))
        fixed = rest
    yield
    names = ["own"]
    d, how = phases[-1]
    long, short = lengths(SIZES[d])
    names += [("l", s) for s in range(long)] + [("s", s) for s in range(short)]
    for name in names:
        copies.arrived((key, colour, "across", name))


def gather_kernel(*refs):
    wide_sums, tall_sums, m, v, weights = refs[0], refs[1], refs[2:5], refs[5:8], refs[8:11]
    outs, new_m, new_v, rest = refs[11:17], refs[17:20], refs[20:23], refs[23:]
    wide, tall = rest[:2]
    cross = {WIDE: rest[2], TALL: rest[3]}
    rows = {WIDE: rest[4], TALL: rest[5]}
    forty, load, send, recv = rest[6:10]
    me = Me()
    mine = 2 * lax.rem(me.at["z"], 2) + me.core

    def which(i):
        kind, j = ORDER[i]
        return (2, j) if kind == TALL else (j // 2, j % 2)

    loads = []
    for i, (kind, j) in enumerate(ORDER):
        n, layer = which(i)
        group = me.at["x"] * SIZES["y"] + me.at["y"]
        z = me.at["z"] if kind == WIDE else lax.div(me.at["z"], 2)
        first = (group * dims(kind, "z")[0] + z) * ROWS[kind]
        src = weights[n].at[layer, pl.ds(pl.multiple_of(first, 8), ROWS[kind]), :]
        loads.append(pltpu.make_async_copy(src, rows[kind].at[j], load.at[i]))
        loads[-1].start()
    me.barrier()
    copies = Copies(send, recv)

    for i, (kind, j) in enumerate(ORDER):
        n, layer = which(i)
        loads[i].wait()
        many, width = (2, HALF[WIDE]) if kind == WIDE else (4, HALF[TALL] // 2)
        for q in range(many):
            at = pl.ds((q if kind == WIDE else q % 2 * 2 + q // 2) * width, width)
            w = rows[kind][j, :, at].astype(F32)
            size = ROWS[kind] // many
            own = w[:size]
            for p in range(1, many):
                own = jnp.where((me.core if kind == WIDE else mine) == p, w[p * size : (p + 1) * size], own)
            sums, fresh = (wide_sums, wide) if kind == WIDE else (tall_sums, tall)
            value, new_m[n][layer, :, at], new_v[n][layer, :, at] = adamw(own, m[n][layer, :, at], v[n][layer, :, at], sums[j, q])
            fresh[j, q] = value.astype(F32)
        if kind == WIDE:
            copies.start((i, "rows"), lambda j=j: (wide.at[j, 1 - me.core], cross[WIDE].at[j], me.device(core=1 - me.core)))
        else:
            for o, (z, core) in enumerate(((me.at["z"], 1 - me.core), (me.pair(), me.core), (me.pair(), 1 - me.core))):
                q = 2 * lax.rem(z, 2) + core
                copies.start(
                    (i, "rows", o),
                    lambda j=j, q=q, z=z, core=core: (tall.at[j, q], cross[TALL].at[j, mine], me.device(core=core, z=z)),
                )

    def begin(i):
        kind, j = ORDER[i]
        here = view(outs[i], kind, ("x", "y", "z"), me.at, None, me.core * HALF[kind])
        if kind == WIDE:
            copies.arrived((i, "rows"))
            own, theirs = wide[j, me.core], cross[WIDE][j]
            first = me.core == 0
            rows = [jnp.where(first, own, theirs), jnp.where(first, theirs, own)]
            here[...] = jnp.concatenate(rows, axis=0).astype(BF16)
        else:
            for o in range(3):
                copies.arrived((i, "rows", o))
            for q in range(4):
                forty[10 * q : 10 * q + 10, :] = jnp.where(q == mine, tall[j, q], cross[TALL][j, q])
            here[...] = forty[...].astype(BF16)

    def colour(i, c):
        if i in waiting:
            waiting.discard(i)
            begin(i)
        yield from gather_colour(me, copies, i, ORDER[i][0], c, outs[i])

    waiting = set(range(6))
    run({(i, c): colour(i, c) for i in range(6) for c in range(3)}, GATHER_ORDER)
    copies.sent()


def all_gather(wide, tall, m, v, weights):
    moments = [pltpu.VMEM(t.shape, F32) for t in m]
    scratch = [
        pltpu.VMEM((4, 2, 4, 1280), F32),
        pltpu.VMEM((2, 4, 10, 256), F32),
        pltpu.VMEM((4, 4, 1280), F32),
        pltpu.VMEM((2, 4, 10, 256), F32),
        pltpu.VMEM((4, ROWS[WIDE], 2560), BF16),
        pltpu.VMEM((2, ROWS[TALL], 1024), BF16),
        pltpu.VMEM((40, 256), F32),
        pltpu.SemaphoreType.DMA((6,)),
        pltpu.SemaphoreType.DMA((384,)),
        pltpu.SemaphoreType.DMA((384,)),
    ]
    matrices = [pltpu.VMEM((*dims(kind, ("x", "y", "z")), ROWS[kind], 2 * HALF[kind]), BF16) for kind, _ in ORDER]
    return pl.pallas_call(
        gather_kernel,
        out_shape=(*matrices, *moments, *moments),
        in_specs=[pl.BlockSpec(memory_space=pltpu.VMEM)] * 8 + [pl.BlockSpec(memory_space=pl.ANY)] * 3,
        out_specs=(pl.BlockSpec(memory_space=pltpu.VMEM),) * 12,
        scratch_shapes=scratch,
        compiler_params=pltpu.CompilerParams(collective_id=1, has_side_effects=True, vmem_limit_bytes=4 * 1024 * 1024),
        name="all_gather",
    )(wide, tall, *m, *v, *weights)


def spill_kernel(*refs):
    ins, moments, outs, sem = refs[:6], refs[6:12], refs[12:21], refs[21]
    copies = []
    for i, (kind, j) in enumerate(ORDER):
        which, layer = (2, j) if kind == TALL else (j // 2, j % 2)
        copies.append(pltpu.make_async_copy(ins[i], outs[which].at[layer], sem.at[i]))
    for i in range(6):
        copies.append(pltpu.make_async_copy(moments[i], outs[3 + i], sem.at[6 + i]))
    for copy in copies:
        copy.start()
    for copy in copies:
        copy.wait()


def spill(new):
    wide, tall = ((2, *dims(kind, ("x", "y", "z")), ROWS[kind], 2 * HALF[kind]) for kind in (WIDE, TALL))
    return pl.pallas_call(
        spill_kernel,
        out_shape=(*(jax.ShapeDtypeStruct(shape, BF16) for shape in (wide, wide, tall)), *(jax.ShapeDtypeStruct(t.shape, F32) for t in new[6:])),
        in_specs=[pl.BlockSpec(memory_space=pltpu.VMEM)] * 12,
        out_specs=(pl.BlockSpec(memory_space=pl.ANY),) * 9,
        scratch_shapes=[pltpu.SemaphoreType.DMA((12,))],
        compiler_params=pltpu.CompilerParams(vmem_limit_bytes=1024 * 1024),
        name="spill",
    )(*new)


def adamw(w, m, v, g):
    m = 0.9 * m + 0.1 * g
    v = 0.95 * v + 0.05 * g * g
    step = m * lax.rsqrt(v + 1e-8) + 0.1 * w
    return (w - 0.02 * step).astype(BF16), m, v


def solution(mesh):
    def step(x, dy, *arrays):
        weights, m, v = (arrays[i : i + 3] for i in (0, 3, 6))
        new = spill(all_gather(*summed(x[0], dy[0], *weights), m, v, weights))
        return (*(w.reshape(2, -1, w.shape[-1]) for w in new[:3]), *new[3:])

    batch, whole, rows = P(("rep", "dp")), P(), P(None, "dp")
    return jax.shard_map(
        step,
        mesh=mesh,
        in_specs=(batch, batch, *(whole,) * 3, *(rows,) * 6),
        out_specs=(*(P("rep"),) * 3, *(P("rep", "dp"),) * 6),
        check_vma=False,
    )
```

```python
import functools

import jax
import jax.numpy as jnp
from jax import lax
from jax.experimental import pallas as pl
from jax.experimental.pallas import tpu as pltpu
from jax.sharding import PartitionSpec as P

NAMES = ("w_gate", "w_up", "w_down")
MESH = pl.DeviceIdType.MESH
F32, BF16 = jnp.float32, jnp.bfloat16
SIZES = {"x": 4, "y": 4, "z": 8}
VMEM_LIMIT = 64 * 1024 * 1024 - 64 * 1024

TICKS = {
    "first": ["0h"],
    "wide1": ["1h", "1s010200", "2h121011", "0200"],
    "back": ["0112212022", "", "10020011", "12", "0122", "02002120", "1211", "0110002221020s"],
    "units": ["011210020020112122", "", "10121121022022", "0103", "1220", "031022", "111321", "13202223", "23", ""],
    "last": ["3h"],
    "wide0": ["4h", "4s313230", "5h404241", "3230"],
    "tail": ["31524250514041323052423150513241523040314251303250404152314251504132405230514250313233524142404333435152505353"],
}
GATHER_ORDER = "023120220100113012321040412152514250022212325242312002012220001211322030520042103101403011410020102131014051023011504110221200313220522120514201024022301150411231323110520142000111210250510011412240123221305242300210510222501012412232124041322152504240215152504251"


RING, DIRECT = "ring", "direct"
COLOURS = (
    (("x", RING), ("y", RING), ("z", DIRECT)),
    (("y", RING), ("x", RING), ("z", DIRECT)),
    (("z", RING), ("x", DIRECT), ("y", DIRECT)),
)
GATE, UP, TALL = KINDS = "gate", "up", "tall"
PART = {
    GATE: ((0, 512), (512, 384), (896, 384)),
    UP: ((0, 512), (512, 384), (896, 384)),
    TALL: ((0, 8), (8, 16), (24, 16)),
}
GATHER_PART = {
    GATE: ((0, 512), (512, 384), (896, 384)),
    UP: ((0, 256), (256, 384), (640, 640)),
    TALL: ((0, 16), (16, 16), (32, 8)),
}
HALF = {GATE: 1280, UP: 1280, TALL: 512}
ROWS = {GATE: 8, UP: 8, TALL: 40}
ORDER = ((TALL, 1), (GATE, 1), (UP, 3), (TALL, 0), (GATE, 0), (UP, 2))


def by_kind(wide, tall):
    return {GATE: wide, UP: wide, TALL: tall}


class Me:
    def __init__(self):
        index = lax.axis_index("dp")
        Me.zero = index * 0
        self.core = lax.rem(index, 2)
        chip = index // 2
        self.at = {
            "z": lax.rem(chip, SIZES["z"]),
            "y": lax.rem(chip // SIZES["z"], SIZES["y"]),
            "x": chip // (SIZES["z"] * SIZES["y"]),
        }
        self.sign = 1 - 2 * self.core

    def off(self, d, by):
        return lax.rem(self.at[d] + by + SIZES[d], SIZES[d])

    def device(self, core=None, **at):
        at = {**self.at, **at}
        core = self.core if core is None else core
        return (0, ((at["x"] * SIZES["y"] + at["y"]) * SIZES["z"] + at["z"]) * 2 + core)

    def arrive(self):
        sem = pltpu.get_barrier_semaphore()

        def signal(peer):
            pl.semaphore_signal(sem, inc=1, device_id=peer, device_id_type=MESH)

        for d, n in SIZES.items():
            each(n - 1, lambda i, d=d: signal(self.device(**{d: self.off(d, i + 1)})))
        signal(self.device(core=1 - self.core))
        signal(self.device(core=1 - self.core, z=self.pair()))
        return sem

    def arrived(self, sem):
        pl.semaphore_wait(sem, sum(SIZES.values()) - 1)

    def pair(self):
        return self.at["z"] + 1 - 2 * lax.rem(self.at["z"], 2)


def dims(kind, free):
    return tuple(SIZES[d] // (2 if kind == TALL and d == "z" else 1) for d in free)


def view(ref, kind, free, fixed, colour=None, base=0, own=False, parts=PART):
    index = [(fixed[d] // 2 if kind == TALL and d == "z" else fixed[d]) if d in fixed else slice(None) for d in free]
    if own and not (kind == TALL and "z" in free and "z" in fixed):
        return ref.at[(*index, slice(None), slice(None))]
    if kind != TALL:
        first, size = (0, HALF[kind]) if colour is None else parts[kind][colour]
        rows, columns = slice(None), pl.ds(_at(base, first), size)
    else:
        rows = slice(None) if own or colour is None else pl.ds(*parts[TALL][colour])
        if "z" in free and "z" in fixed:
            columns = pl.ds(pl.multiple_of(base + lax.rem(fixed["z"], 2) * 256, 256), 256)
        else:
            columns = pl.ds(_at(base, 0), HALF[TALL])
    return ref.at[(*index, rows, columns)]


def _at(base, first):
    return first if isinstance(base, int) and base == 0 else pl.multiple_of(base + first, 128)


def block(kind, colour, free):
    first, size = PART[kind][colour]
    tail = (8, size) if kind != TALL else (size, HALF[TALL] if "z" in free else HALF[TALL] // 2)
    return dims(kind, free) + tail


def lengths(n):
    return n // 2, (n - 1) // 2


def reduce_buffers(kind):
    shapes = {}
    for c, phases in enumerate(COLOURS):
        free = ["x", "y", "z"]
        for p, (d, how) in enumerate(phases):
            free.remove(d)
            shape = block(kind, c, tuple(free))
            count = SIZES[d] - 1
            shapes[c, p] = (count, *shape)
    return shapes


class Copies:
    def __init__(self, send, recv):
        self.send, self.recv, self.all, self.used, self.left = send, recv, {}, 0, set()

    def start(self, key, make):
        self.start_all(key, 1, lambda i: make())

    def start_all(self, key, count, make):
        first = self.used
        self.used += count

        def copy(i):
            src, dst, to = make(i)
            return pltpu.make_async_remote_copy(
                src_ref=src, dst_ref=dst, send_sem=self.send.at[first + i], recv_sem=self.recv.at[first + i], device_id=to, device_id_type=MESH
            )

        self.all[key] = count, copy
        each(count, lambda i: copy(i).start())

    def arrived(self, key):
        count, copy = self.all[key]
        each(count, lambda i: copy(i).wait_recv())

    def sent(self, mine=lambda key: True):
        for key, (count, copy) in self.all.items():
            if key not in self.left and mine(key):
                self.left.add(key)
                each(count, lambda i, copy=copy: copy(i).wait_send())


def each(count, do):
    if count == 1:
        do(0)
    else:

        loop(count)(do)


def loop(count):
    def run(body):
        def step(carry, _):
            body(carry[0])
            return (carry[0] + 1, None), None

        lax.scan(step, (Me.zero, None), None, length=count)

    return run


def total(parts):
    return functools.reduce(jnp.add, [p[...].astype(F32) for p in parts])


def reduce_colour(me, copies, key, kind, colour, grads, received, last, keep=None):
    free, fixed = ("x", "y", "z"), {}
    parts = [lambda at, r=r: view(r(), kind, ("x", "y", "z"), at, colour) for r in grads]
    out = parts[0]

    def add(at, more):
        rest = [d for d in free if d not in at]
        if len(rest) >= 2:
            first = rest[0]

            @loop(SIZES[first])
            def _(i):
                now = {**at, first: i}
                out(now)[...] = total([p(now) for p in parts + more]).astype(BF16)
        else:
            out(at)[...] = total([p(at) for p in parts + more]).astype(BF16)

    for phase, (d, how) in enumerate(COLOURS[colour]):
        n, buffer = SIZES[d], functools.partial(received, colour, phase)
        left = tuple(e for e in ("x", "y", "z") if e not in fixed and e != d)

        def slot(i, buffer=buffer, left=left):
            return lambda at: view(buffer().at[i], kind, left, {e: v for e, v in at.items() if e in left}, colour, own=True)

        if how == RING:
            long, short = lengths(n)
            ways = ((1, long, 0, "l"), (-1, short, long, "s"))
            for s in range(long):
                for sign, length, base, name in ways:
                    if s >= length:
                        continue

                    def make(d=d, fixed=fixed, buffer=buffer, sign=sign, by=length - s, place=base + s):
                        at = {**fixed, d: me.off(d, me.sign * (sign * by))}
                        return out(at), buffer().at[place], me.device(**{d: me.off(d, me.sign * sign)})

                    if s:
                        copies.arrived((key, colour, phase, name, s - 1))
                    add({**fixed, d: me.off(d, me.sign * (sign * (length - s)))}, [slot(base + s - 1)] if s else [])
                    copies.start((key, colour, phase, name, s), make)
                yield
            for sign, length, base, name in ways:
                if length:
                    copies.arrived((key, colour, phase, name, length - 1))
            parts = parts + [slot(base + length - 1) for sign, length, base, name in ways if length]
        else:

            def make(i, d=d, fixed=fixed, buffer=buffer, add=add, out=out):
                to = me.off(d, i + 1)
                return out({**fixed, d: to}), buffer().at[i], me.device(**{d: to})

            each(n - 1, lambda i: add({**fixed, d: me.off(d, i + 1)}, []))
            copies.start_all((key, colour, phase), n - 1, make)
            yield
            copies.arrived((key, colour, phase))
            parts = parts + [slot(i) for i in range(n - 1)]
        fixed = {**fixed, d: me.at[d]}
        if keep is not None and phase == 0:
            copies.sent(lambda k: k[:3] == (key, colour, 0))
            stays = (lambda at, left=left: view(keep, kind, left, {e: v for e, v in at.items() if e in left}, colour, own=True))
            stays(fixed)[...] = out(fixed)[...]
            out = stays
            parts[0] = stays
    last(colour, total([p(fixed) for p in parts]).astype(BF16).astype(F32))


class Reduce:
    def __init__(self, me, own, theirs, halves, buffers, sums, cross, shares, outs, send, recv, free, kept):
        self.me, self.own, self.theirs, self.halves, self.buffers = me, own, theirs, halves, buffers
        self.sums, self.cross, self.shares, self.outs, self.free, self.kept = sums, cross, shares, outs, free, kept
        self.copies = Copies(send, recv)
        self.waiting = set(range(6))
        self.streams = {(i, c): self.colour(i, c) for i in range(6) for c in range(3)} | {(i, 3): self.finish(i) for i in range(6)}

    def slot(self, i):
        kind, j = ORDER[i]
        return 0 if kind == TALL else j // 2

    def half(self, i):
        kind = ORDER[i][0]
        if i >= 3:
            pl.semaphore_wait(self.free.at[i - 3], sum(SIZES.values()) - len(SIZES) + 1)
        self.copies.start(
            (i, "half"), lambda: (self.halves[kind](), self.theirs[kind].at[self.slot(i)], self.me.device(core=1 - self.me.core))
        )

    def half_sent(self, i):
        self.copies.sent(lambda key: key == (i, "half"))

    def colour(self, i, c):
        kind, j = ORDER[i]
        slot = self.slot(i)
        if i in self.waiting:
            self.waiting.discard(i)
            self.copies.arrived((i, "half"))

        def last(colour, value):
            first, size = PART[kind][colour]
            if kind != TALL:
                self.sums[kind][j, 0, :, first : first + size] = value[:4]
                self.sums[kind][j, 1, :, first : first + size] = value[4:]
            else:
                self.sums[TALL][j, first : first + size, :] = value

        grads = (lambda: self.own[kind].at[slot]), (lambda: self.theirs[kind].at[slot])
        keep = self.kept[c] if i == 0 else None
        yield from reduce_colour(self.me, self.copies, i, kind, c, grads, lambda c, p: self.buffers[kind, (c, p)].at[0], last, keep)

    def finish(self, i):
        (kind, j), me, copies = ORDER[i], self.me, self.copies
        sums, cross, shares, outs = self.sums, self.cross, self.shares, self.outs
        mine = 2 * lax.rem(me.at["z"], 2) + me.core
        if kind != TALL:
            copies.start((i, "rows"), lambda: (sums[kind].at[j, 1 - me.core], cross[kind].at[j], me.device(core=1 - me.core)))
        else:
            for q in range(4):
                shares[j, q] = sums[TALL][j, 10 * q : 10 * q + 10, :]
            for o in range(3):

                def make(o=o):
                    z, core = ((me.at["z"], 1 - me.core), (me.pair(), me.core), (me.pair(), 1 - me.core))[o]
                    mine = 2 * lax.rem(me.at["z"], 2) + me.core
                    return shares.at[j, 2 * lax.rem(z, 2) + core], cross[TALL].at[j, mine], me.device(core=core, z=z)

                copies.start((i, "rows", o), make)
        if i < 3:
            for d, n in SIZES.items():
                each(n - 1, lambda o, d=d: self.done(i, me.device(**{d: me.off(d, o + 1)})))
            self.done(i, me.device(core=1 - me.core))
        yield
        mine = 2 * lax.rem(me.at["z"], 2) + me.core
        if kind != TALL:
            copies.arrived((i, "rows"))
            outs[0][j, me.core] = sums[kind][j, me.core]
            outs[0][j, 1 - me.core] = cross[kind][j]
        else:
            for o in range(3):
                copies.arrived((i, "rows", o))
            for q in range(4):
                outs[1][j, q] = jnp.where(q == mine, shares[j, q], cross[TALL][j, q])
        copies.sent(lambda key: key[0] == i)

    def done(self, i, device):
        pl.semaphore_signal(self.free.at[i], inc=1, device_id=device, device_id_type=MESH)

    def run(self, order):
        for i, c in zip(order[::2], order[1::2], strict=True):
            if c == "h":
                self.half(int(i))
            elif c == "s":
                self.half_sent(int(i))
            else:
                next(self.streams[int(i), int(c)], None)


def dot(a, b, ca=1, cb=0):
    return lax.dot_general(a, b, (((ca,), (cb,)), ((), ())), preferred_element_type=F32)


def rem(a, b):
    return a % b if isinstance(a, int) else lax.rem(a, b)


def at_tile(i, size):
    return pl.ds(pl.multiple_of(i * size, size), size)


def put_rows(ref, i, value):
    y, z, rows = ref.shape[1:4]
    for s in range(0, 256, 8):
        row = i * 256 + s
        group = lax.div(row, rows)
        ref[lax.div(group, y * z), rem(lax.div(group, z), y), rem(group, z), pl.ds(pl.multiple_of(rem(row, rows), 8), 8), :] = value[s : s + 8]


def put_all(ref, value):
    ref[...] = value.reshape(ref.shape)


def step_kernel(*refs):
    x_in, dy_in, w_gate, w_up, w_down = refs[:5]
    outs, (gate_kept, up_kept, a0_kept, h1_kept) = refs[5:7], refs[7:11]
    rest = list(refs[11:])
    take = lambda n: [rest.pop(0) for _ in range(n)]
    act, dy, turned, back, both, gates, ups = take(7)
    tile_g, tile_u, tile_d, rows_w, columns_w = take(5)
    wide_own, wide_theirs, tall_own, tall_half, tall_theirs = take(5)
    wide_sums, tall_sums, wide_cross, tall_cross, shares = take(5)
    load, sem_g, sem_u, sem_d, sem_w, sem_c, sem_f, send, recv, free = take(10)
    buffers = {}
    for kind in KINDS:
        for k in reduce_buffers(kind):
            buffers[kind, k] = rest.pop(0)
    tall_kept = take(3)
    me = Me()

    def fetch(src, dst, sem):
        copy = pltpu.make_async_copy(src, dst, sem)
        copy.start()
        return copy

    class Stream:
        def __init__(self, tile, buffer, sem):
            self.tile, self.buffer, self.sem = tile, buffer, sem

        def copy(self, i):
            slot = rem(i, 2)
            return pltpu.make_async_copy(self.tile(i), self.buffer.at[slot], self.sem.at[slot])

    def stream(*streams, n):
        for s in streams:
            s.copy(0).start()

        def ahead(i):
            @pl.when(i + 1 < n)
            def _():
                for s in streams:
                    s.copy(i + 1).start()

            for s in streams:
                s.copy(i).wait()

        return ahead

    def columns(w, layer, buffer, sem):
        return Stream(lambda i: w.at[layer, :, at_tile(i, 256)], buffer, sem)

    loads = [fetch(x_in, back, load.at[0]), fetch(dy_in, dy, load.at[1])]
    zeroth = stream(columns(w_gate, 0, tile_g, sem_g), columns(w_up, 0, tile_u, sem_u), n=10)

    def half_columns(i, half):
        src = w_down.at[0, pl.ds(half * 1280, 1280), at_tile(i, 256)]
        return pltpu.make_async_copy(src, columns_w.at[half], sem_c.at[half])

    for half in (0, 1):
        half_columns(0, half).start()
    peers = me.arrive()
    own = by_kind(wide_own, tall_own)
    theirs = by_kind(wide_theirs, tall_theirs)
    halves = by_kind(lambda: wide_own.at[2], lambda: tall_half)
    sums, cross = by_kind(wide_sums, tall_sums), by_kind(wide_cross, tall_cross)
    reduce = Reduce(me, own, theirs, halves, buffers, sums, cross, shares, outs, send, recv, free, tall_kept)

    def ticks(phase, i):
        orders = TICKS[phase]
        if any(orders):
            lax.switch(i, [functools.partial(reduce.run, order) for order in orders])

    def norm():
        @pl.loop(0, 8)
        def _(i):
            rows = at_tile(i, 128)
            h = back[rows, :].astype(F32)
            act[rows, :] = (h * lax.rsqrt(jnp.mean(h * h, -1, keepdims=True) + 1e-6)).astype(BF16)

    def turn(src, i):
        i = rem(i, 8)
        turned[:, at_tile(i, 128)] = src[at_tile(i, 128), :].T

    def unit(i, g, u, d, dout):
        d = d.astype(BF16).astype(F32)
        s = jax.nn.sigmoid(g)
        silu = g * s
        value = (silu * u).astype(BF16).T
        both[1, :, at_tile(i, 256)] = (d * silu).astype(BF16)
        both[0, :, at_tile(i, 256)] = (d * u * (s * (1 + g * (1 - s)))).astype(BF16)
        for ref, core in ((tall_own.at[0], me.core), (tall_half, 1 - me.core)):
            put_rows(ref, i, dot(value, dout[:, at_tile(core, 512)]).astype(BF16))

    def wide_grads(phase):
        @pl.loop(0, 4)
        def _(k):
            which, mine = lax.div(k, 2), lax.rem(k, 2)
            core = mine * me.core + (1 - mine) * (1 - me.core)
            value = dot(turned[...], both[which, :, at_tile(core, 1280)]).astype(BF16)
            put_all(wide_own.at[lax.rem(2 - mine * (2 - which), 3)], value)
            ticks(phase, k)

    def kept(i, out):
        slot = rem(i, 2)
        pairs = (gates.at[slot], gate_kept.at[:, at_tile(i, 256)]), (ups.at[slot], up_kept.at[:, at_tile(i, 256)])
        return [pltpu.make_async_copy(*(p if out else p[::-1]), sem_f.at[n, slot]) for n, p in enumerate(pairs)]

    loads[0].wait()
    norm()
    keep = fetch(act, a0_kept, load.at[0])

    @pl.loop(0, 10)
    def _(i):
        zeroth(i)

        @pl.when(i >= 2)
        def _():
            for copy in kept(i - 2, True):
                copy.wait()

        slot = rem(i, 2)
        g, u = dot(act[...], tile_g[slot]), dot(act[...], tile_u[slot])
        gates[slot] = g
        ups[slot] = u
        both[0, :, at_tile(i, 256)] = (g * jax.nn.sigmoid(g) * u).astype(BF16)
        for copy in kept(i, True):
            copy.start()

    first = stream(
        columns(w_gate, 1, tile_g, sem_g),
        columns(w_up, 1, tile_u, sem_u),
        Stream(lambda i: w_down.at[1, at_tile(i, 256), :], tile_d, sem_d),
        n=10,
    )

    @pl.loop(0, 4)
    def _(i):
        part = 0.0
        for half in (0, 1):
            half_columns(i, half).wait()
            part += dot(both[0, :, half * 1280 : half * 1280 + 1280], columns_w[half])

            @pl.when(i < 3)
            def _():
                half_columns(i + 1, half).start()

        part = part.astype(BF16).astype(F32)
        back[:, at_tile(i, 256)] = (back[:, at_tile(i, 256)].astype(F32) + part).astype(BF16)

    keep.wait()
    keep = fetch(back, h1_kept, load.at[0])
    norm()

    loads[1].wait()

    @pl.loop(0, 10)
    def _(i):
        first(i)
        turn(act, i)
        slot = rem(i, 2)
        unit(i, dot(act[...], tile_g[slot]), dot(act[...], tile_u[slot]), dot(dy[...], tile_d[slot], 1, 1), dy)

    me.arrived(peers)
    reduce.run(TICKS["first"][0])
    wide_grads("wide1")

    keep.wait()
    for i in (8, 9):
        for copy in kept(i, True):
            copy.wait()
    load_h = fetch(h1_kept, turned, load.at[0])

    def weight_rows(k, w):
        slot = rem(k, 2)
        rows = at_tile(k // 2 if isinstance(k, int) else lax.div(k, 2), 256)
        return pltpu.make_async_copy(w.at[1, rows, :], rows_w.at[slot], sem_w.at[slot])

    weight_rows(0, w_gate).start()

    @pl.loop(0, 8)
    def _(k):
        n, which = lax.div(k, 2), lax.rem(k, 2)

        @pl.when(which == 0)
        def _():
            weight_rows(k + 1, w_up).start()

        @pl.when((which == 1) & (k < 7))
        def _():
            weight_rows(k + 1, w_gate).start()

        weight_rows(k, w_gate).wait()
        part = dot(both[which], rows_w[which], 1, 1).astype(BF16).astype(F32)
        before = back[:, at_tile(n, 256)].astype(F32)
        back[:, at_tile(n, 256)] = (jnp.where(which == 0, 0.0, before) + part).astype(BF16)
        ticks("back", k)

    load_h.wait()

    @pl.loop(0, 8)
    def _(i):
        rows = at_tile(i, 128)
        h, d = turned[rows, :].astype(F32), back[rows, :].astype(F32)
        scale = lax.rsqrt(jnp.mean(h * h, -1, keepdims=True) + 1e-6)
        along = jnp.sum(d * h, -1, keepdims=True)
        d = (d * scale - h * (scale * scale * scale * along * (1 / 1024))).astype(BF16)
        act[rows, :] = (dy[rows, :].astype(F32) + d.astype(F32)).astype(BF16)

    load_a = fetch(a0_kept, back, load.at[1])
    second = stream(Stream(lambda i: w_down.at[0, at_tile(i, 256), :], tile_d, sem_d), n=10)
    for copy in kept(0, False):
        copy.start()
    load_a.wait()

    @pl.loop(0, 10)
    def _(i):
        @pl.when(i < 9)
        def _():
            for copy in kept(i + 1, False):
                copy.start()

        second(i)
        turn(back, i)
        for copy in kept(i, False):
            copy.wait()
        slot = rem(i, 2)
        unit(i, gates[slot], ups[slot], dot(act[...], tile_d[slot], 1, 1), act)
        ticks("units", i)

    reduce.run(TICKS["last"][0])
    wide_grads("wide0")
    reduce.run(TICKS["tail"][0])
    for stream_ in reduce.streams.values():
        assert next(stream_, 0) == 0, "not done"
    reduce.copies.sent()


def run(streams, order):
    for i, c in zip(order[::2], order[1::2], strict=True):
        next(streams[int(i), int(c)], None)
    for stream in streams.values():
        assert next(stream, 0) == 0, "not done"


def full_shape(kind):
    return dims(kind, ("x", "y", "z")) + (ROWS[kind], HALF[kind])


def summed(x, dy, w_gate, w_up, w_down):
    square = pltpu.VMEM((1024, 1024), BF16)
    scratch = [square] * 4 + [pltpu.VMEM((2, 1024, 2560), BF16)]
    scratch += [pltpu.VMEM((2, 1024, 256), F32)] * 2
    scratch += [pltpu.VMEM((2, 1024, 256), BF16)] * 2 + [pltpu.VMEM((2, 256, 1024), BF16), pltpu.VMEM((2, 256, 2560), BF16)]
    scratch += [
        pltpu.VMEM((2, 1280, 256), BF16),
        pltpu.VMEM((3, *full_shape(GATE)), BF16),
        pltpu.VMEM((2, *full_shape(GATE)), BF16),
        pltpu.VMEM((1, *full_shape(TALL)), BF16),
        pltpu.VMEM(full_shape(TALL), BF16),
        pltpu.VMEM((1, *full_shape(TALL)), BF16),
        pltpu.VMEM((4, 2, 4, 1280), F32),
        pltpu.VMEM((2, 40, 256), F32),
        pltpu.VMEM((4, 4, 1280), F32),
        pltpu.VMEM((2, 4, 10, 256), F32),
        pltpu.VMEM((2, 4, 10, 256), F32),
        *[pltpu.SemaphoreType.DMA((2,))] * 6,
        pltpu.SemaphoreType.DMA((2, 2)),
        pltpu.SemaphoreType.DMA((256,)),
        pltpu.SemaphoreType.DMA((256,)),
        pltpu.SemaphoreType.REGULAR((3,)),
    ]
    for kind in KINDS:
        scratch += [pltpu.VMEM((1, *shape), BF16) for shape in reduce_buffers(kind).values()]
    scratch += [pltpu.VMEM(block(TALL, c, [d for d in "xyz" if d != COLOURS[c][0][0]]), BF16) for c in range(3)]
    kept = [jax.ShapeDtypeStruct((1024, 2560), F32)] * 2 + [jax.ShapeDtypeStruct((1024, 1024), BF16)] * 2
    return pl.pallas_call(
        step_kernel,
        out_shape=(jax.ShapeDtypeStruct((4, 2, 4, 1280), F32), jax.ShapeDtypeStruct((2, 4, 10, 256), F32), *kept),
        in_specs=[pl.BlockSpec(memory_space=pl.ANY)] * 5,
        out_specs=(*[pl.BlockSpec(memory_space=pltpu.VMEM)] * 2, *[pl.BlockSpec(memory_space=pl.ANY)] * 4),
        scratch_shapes=scratch,
        compiler_params=pltpu.CompilerParams(collective_id=0, has_side_effects=True, vmem_limit_bytes=VMEM_LIMIT),
        name="step",
    )(x, dy, w_gate, w_up, w_down)[:2]


def gather_colour(me, copies, key, kind, colour, ref):
    base = me.core * HALF[kind]
    fixed = dict(me.at)

    def part(at):
        return view(ref, kind, ("x", "y", "z"), at, colour, base, parts=GATHER_PART)

    phases = COLOURS[colour][::-1]
    for phase, (d, how) in enumerate(phases):
        n, lastly = SIZES[d], phase == len(phases) - 1
        rest = {e: v for e, v in fixed.items() if e != d}
        here = part(fixed)

        def across(name, at):
            if lastly:
                copies.start((key, colour, "across", name), lambda: (part(at), part(at), me.device(core=1 - me.core)))

        if how == RING:
            long, short = lengths(n)
            ways = ((me.sign, long, "l"), (-me.sign, short, "s"))
            for s in range(long):
                for sign, length, name in ways:
                    if s >= length:
                        continue
                    at = {**rest, d: me.off(d, -sign * s)}
                    if s:
                        copies.arrived((key, colour, phase, name, s - 1))
                    copies.start(
                        (key, colour, phase, name, s),
                        lambda at=at, d=d, sign=sign: (part(at), part(at), me.device(**{d: me.off(d, sign)})),
                    )
                    if s:
                        across((name, s - 1), at)
                if s == 0:
                    across("own", fixed)
                yield
            for sign, length, name in ways:
                if length:
                    copies.arrived((key, colour, phase, name, length - 1))
                    across((name, length - 1), {**rest, d: me.off(d, -sign * length)})
        else:
            copies.start_all(
                (key, colour, phase), n - 1, lambda i, d=d, here=here: (here, here, me.device(**{d: me.off(d, i + 1)}))
            )
            yield
            copies.arrived((key, colour, phase))
        fixed = rest
    yield
    names = ["own"]
    d, how = phases[-1]
    long, short = lengths(SIZES[d])
    names += [("l", s) for s in range(long)] + [("s", s) for s in range(short)]
    for name in names:
        copies.arrived((key, colour, "across", name))


def gather_kernel(*refs):
    given, weights = refs[:8], refs[8:11]
    outs, new_m, new_v, rest = refs[11:17], refs[17:20], refs[20:23], refs[23:]
    taken, rest = rest[:8], rest[8:]
    wide_sums, tall_sums, m, v = taken[0], taken[1], taken[2:5], taken[5:8]
    wide, tall = rest[:2]
    cross, rows = by_kind(*rest[2:4]), by_kind(*rest[4:6])
    forty, load, send, recv = rest[6:10]
    me = Me()
    mine = 2 * lax.rem(me.at["z"], 2) + me.core

    def which(i):
        kind, j = ORDER[i]
        return (2, j) if kind == TALL else (j // 2, j % 2)

    loads = []
    takes = [pltpu.make_async_copy(*pair, load.at[6 + n]) for n, pair in enumerate(zip(given, taken, strict=True))]
    for copy in takes:
        copy.start()
    for i, (kind, j) in enumerate(ORDER):
        n, layer = which(i)
        group = me.at["x"] * SIZES["y"] + me.at["y"]
        z = me.at["z"] if kind != TALL else lax.div(me.at["z"], 2)
        first = (group * dims(kind, "z")[0] + z) * ROWS[kind]
        src = weights[n].at[layer, pl.ds(pl.multiple_of(first, 8), ROWS[kind]), :]
        loads.append(pltpu.make_async_copy(src, rows[kind].at[j], load.at[i]))
        loads[-1].start()
    peers = me.arrive()
    copies = Copies(send, recv)
    for copy in takes:
        copy.wait()

    def update(i):
        kind, j = ORDER[i]
        n, layer = which(i)
        loads[i].wait()
        many, width = (2, HALF[kind]) if kind != TALL else (4, HALF[TALL] // 2)
        for q in range(many):
            at = pl.ds((q if kind != TALL else q % 2 * 2 + q // 2) * width, width)
            here = (layer, slice(None), at) if kind != TALL else (slice(None), layer, at)
            w = rows[kind][j, :, at].astype(F32)
            size = ROWS[kind] // many
            own = w[:size]
            for p in range(1, many):
                own = jnp.where((me.core if kind != TALL else mine) == p, w[p * size : (p + 1) * size], own)
            sums, fresh = (wide_sums, wide) if kind != TALL else (tall_sums, tall)
            value, new_m[n][here], new_v[n][here] = adamw(own, m[n][here], v[n][here], sums[j, q])
            fresh[j, q] = value.astype(F32)
        if not copies.used:
            me.arrived(peers)
        if kind != TALL:
            copies.start((i, "rows"), lambda: (wide.at[j, 1 - me.core], cross[kind].at[j], me.device(core=1 - me.core)))
        else:
            for o, (z, core) in enumerate(((me.at["z"], 1 - me.core), (me.pair(), me.core), (me.pair(), 1 - me.core))):
                q = 2 * lax.rem(z, 2) + core
                copies.start(
                    (i, "rows", o),
                    lambda q=q, z=z, core=core: (tall.at[j, q], cross[TALL].at[j, mine], me.device(core=core, z=z)),
                )

    def begin(i):
        kind, j = ORDER[i]
        here = view(outs[i], kind, ("x", "y", "z"), me.at, None, me.core * HALF[kind])
        if kind != TALL:
            copies.arrived((i, "rows"))
            own, theirs = wide[j, me.core], cross[kind][j]
            first = me.core == 0
            rows = [jnp.where(first, own, theirs), jnp.where(first, theirs, own)]
            here[...] = jnp.concatenate(rows, axis=0).astype(BF16)
        else:
            for o in range(3):
                copies.arrived((i, "rows", o))
            for q in range(4):
                forty[10 * q : 10 * q + 10, :] = jnp.where(q == mine, tall[j, q], cross[TALL][j, q])
            here[...] = forty[...].astype(BF16)

    def colour(i, c):
        if i in waiting:
            waiting.discard(i)
            for following in turns[turns.index(i) + 2 :][:1]:
                update(following)
            begin(i)
        yield from gather_colour(me, copies, i, ORDER[i][0], c, outs[i])

    waiting = set(range(6))
    turns = list(dict.fromkeys(int(i) for i in GATHER_ORDER[::2]))
    update(turns[0])
    update(turns[1])
    run({(i, c): colour(i, c) for i in range(6) for c in range(3)}, GATHER_ORDER)
    copies.sent()


def all_gather(wide, tall, m, v, weights):
    moments = [pltpu.VMEM(t.shape, F32) for t in m]
    scratch = [
        *(pltpu.VMEM(t.shape, F32) for t in (wide, tall, *m, *v)),
        pltpu.VMEM((4, 2, 4, 1280), F32),
        pltpu.VMEM((2, 4, 10, 256), F32),
        pltpu.VMEM((4, 4, 1280), F32),
        pltpu.VMEM((2, 4, 10, 256), F32),
        pltpu.VMEM((4, ROWS[GATE], 2560), BF16),
        pltpu.VMEM((2, ROWS[TALL], 1024), BF16),
        pltpu.VMEM((40, 256), F32),
        pltpu.SemaphoreType.DMA((14,)),
        pltpu.SemaphoreType.DMA((384,)),
        pltpu.SemaphoreType.DMA((384,)),
    ]
    matrices = [pltpu.VMEM((*dims(kind, ("x", "y", "z")), ROWS[kind], 2 * HALF[kind]), BF16) for kind, _ in ORDER]
    return pl.pallas_call(
        gather_kernel,
        out_shape=(*matrices, *moments, *moments),
        in_specs=[pl.BlockSpec(memory_space=pl.ANY)] * 11,
        out_specs=(pl.BlockSpec(memory_space=pltpu.VMEM),) * 12,
        scratch_shapes=scratch,
        compiler_params=pltpu.CompilerParams(collective_id=1, has_side_effects=True, vmem_limit_bytes=28 * 1024 * 1024),
        name="all_gather",
    )(wide, tall, *m, *v, *weights)


def spill_kernel(*refs):
    ins, moments, outs, sem = refs[:6], refs[6:12], refs[12:21], refs[21]
    copies = []
    for i, (kind, j) in enumerate(ORDER):
        which, layer = (2, j) if kind == TALL else (j // 2, j % 2)
        copies.append(pltpu.make_async_copy(ins[i], outs[which].at[layer], sem.at[i]))
    for i in range(6):
        copies.append(pltpu.make_async_copy(moments[i], outs[3 + i], sem.at[6 + i]))
    for copy in copies:
        copy.start()
    for copy in copies:
        copy.wait()


def spill(new):
    wide, tall = ((2, *dims(kind, ("x", "y", "z")), ROWS[kind], 2 * HALF[kind]) for kind in (GATE, TALL))
    return pl.pallas_call(
        spill_kernel,
        out_shape=(*(jax.ShapeDtypeStruct(shape, BF16) for shape in (wide, wide, tall)), *(jax.ShapeDtypeStruct(t.shape, F32) for t in new[6:])),
        in_specs=[pl.BlockSpec(memory_space=pltpu.VMEM)] * 12,
        out_specs=(pl.BlockSpec(memory_space=pl.ANY),) * 9,
        scratch_shapes=[pltpu.SemaphoreType.DMA((12,))],
        compiler_params=pltpu.CompilerParams(vmem_limit_bytes=1024 * 1024),
        name="spill",
    )(*new)


def adamw(w, m, v, g):
    m = 0.9 * m + 0.1 * g
    v = 0.95 * v + 0.05 * g * g
    step = m * lax.rsqrt(v + 1e-8) + 0.1 * w
    return (w - 0.02 * step).astype(BF16), m, v


def solution(mesh):
    def step(x, dy, *arrays):
        weights, m, v = (arrays[i : i + 3] for i in (0, 3, 6))
        m, v = ((*t[:2], t[2].transpose(1, 0, 2)) for t in (m, v))
        new = spill(all_gather(*summed(x[0], dy[0], *weights), m, v, weights))
        m, v = ((*t[:2], t[2].transpose(1, 0, 2)) for t in (new[3:6], new[6:9]))
        return (*(w.reshape(2, -1, w.shape[-1]) for w in new[:3]), *m, *v)

    batch, whole, rows = P(("rep", "dp")), P(), P(None, "dp")
    return jax.shard_map(
        step,
        mesh=mesh,
        in_specs=(batch, batch, *(whole,) * 3, *(rows,) * 6),
        out_specs=(*(P("rep"),) * 3, *(P("rep", "dp"),) * 6),
        check_vma=False,
    )
```

```python
import functools

import jax
import jax.numpy as jnp
from jax import lax
from jax.experimental import pallas as pl
from jax.experimental.pallas import tpu as pltpu
from jax.sharding import PartitionSpec as P

NAMES = ("w_gate", "w_up", "w_down")
MESH = pl.DeviceIdType.MESH
F32, BF16 = jnp.float32, jnp.bfloat16
SIZES = {"x": 4, "y": 4, "z": 8}
VMEM_LIMIT = 64 * 1024 * 1024 - 64 * 1024

TICKS = {
    "first": ["0h"],
    "wide1": ["1h", "1s010002", "2h111012", "0002"],
    "back": ["0121201222", "", "111002", "0012", "0122", "212002", "110012", "0110222100020s"],
    "units": ["11012120101222", "0002", "112120", "011012020322", "20", "1112", "0321221013", "13", "202223", "23"],
    "last": ["3h"],
    "wide0": ["4h", "4s313032", "5h404142", "3032"],
    "tail": ["31505152424041323052423150513241524030314251325040304152315142504132405230514250313233524142404333514352505353"],
}
GATHER_ORDER = "023120220100113012321040412152514250022212325242312002012220001211322030520042103101403011410020102131014051023011504110221200313220522120514201024022301150411231323110520142000111210250510011412240123221305242300210510222501012412232124041322152504240215152504251"


RING, DIRECT = "ring", "direct"
COLOURS = (
    (("x", RING), ("y", RING), ("z", DIRECT)),
    (("y", RING), ("x", RING), ("z", DIRECT)),
    (("z", RING), ("x", DIRECT), ("y", DIRECT)),
)
GATE, UP, TALL = KINDS = "gate", "up", "tall"
PART = {
    GATE: ((0, 512), (512, 384), (896, 384)),
    UP: ((0, 512), (512, 384), (896, 384)),
    TALL: ((0, 8), (8, 16), (24, 16)),
}
GATHER_PART = {
    GATE: ((0, 512), (512, 384), (896, 384)),
    UP: ((0, 256), (256, 384), (640, 640)),
    TALL: ((0, 16), (16, 16), (32, 8)),
}
HALF = {GATE: 1280, UP: 1280, TALL: 512}
ROWS = {GATE: 8, UP: 8, TALL: 40}
ORDER = ((TALL, 1), (GATE, 1), (UP, 3), (TALL, 0), (GATE, 0), (UP, 2))


def by_kind(wide, tall):
    return {GATE: wide, UP: wide, TALL: tall}


class Me:
    def __init__(self):
        index = lax.axis_index("dp")
        Me.zero = index * 0
        self.core = lax.rem(index, 2)
        chip = index // 2
        self.at = {
            "z": lax.rem(chip, SIZES["z"]),
            "y": lax.rem(chip // SIZES["z"], SIZES["y"]),
            "x": chip // (SIZES["z"] * SIZES["y"]),
        }
        self.sign = 1 - 2 * self.core

    def off(self, d, by):
        return lax.rem(self.at[d] + by + SIZES[d], SIZES[d])

    def device(self, core=None, **at):
        at = {**self.at, **at}
        core = self.core if core is None else core
        return (0, ((at["x"] * SIZES["y"] + at["y"]) * SIZES["z"] + at["z"]) * 2 + core)

    def arrive(self):
        sem = pltpu.get_barrier_semaphore()

        def signal(peer):
            pl.semaphore_signal(sem, inc=1, device_id=peer, device_id_type=MESH)

        for d, n in SIZES.items():
            each(n - 1, lambda i, d=d: signal(self.device(**{d: self.off(d, i + 1)})))
        signal(self.device(core=1 - self.core))
        signal(self.device(core=1 - self.core, z=self.pair()))
        return sem

    def arrived(self, sem):
        pl.semaphore_wait(sem, sum(SIZES.values()) - 1)

    def pair(self):
        return self.at["z"] + 1 - 2 * lax.rem(self.at["z"], 2)


def dims(kind, free):
    return tuple(SIZES[d] // (2 if kind == TALL and d == "z" else 1) for d in free)


def view(ref, kind, free, fixed, colour=None, base=0, own=False, parts=PART):
    index = [(fixed[d] // 2 if kind == TALL and d == "z" else fixed[d]) if d in fixed else slice(None) for d in free]
    if own and not (kind == TALL and "z" in free and "z" in fixed):
        return ref.at[(*index, slice(None), slice(None))]
    if kind != TALL:
        first, size = (0, HALF[kind]) if colour is None else parts[kind][colour]
        rows, columns = slice(None), pl.ds(_at(base, first), size)
    else:
        rows = slice(None) if own or colour is None else pl.ds(*parts[TALL][colour])
        if "z" in free and "z" in fixed:
            columns = pl.ds(pl.multiple_of(base + lax.rem(fixed["z"], 2) * 256, 256), 256)
        else:
            columns = pl.ds(_at(base, 0), HALF[TALL])
    return ref.at[(*index, rows, columns)]


def _at(base, first):
    return first if isinstance(base, int) and base == 0 else pl.multiple_of(base + first, 128)


def block(kind, colour, free):
    first, size = PART[kind][colour]
    tail = (8, size) if kind != TALL else (size, HALF[TALL] if "z" in free else HALF[TALL] // 2)
    return dims(kind, free) + tail


def lengths(n):
    return n // 2, (n - 1) // 2


def reduce_buffers(kind):
    shapes = {}
    for c, phases in enumerate(COLOURS):
        free = ["x", "y", "z"]
        for p, (d, how) in enumerate(phases):
            free.remove(d)
            shape = block(kind, c, tuple(free))
            count = SIZES[d] - 1
            shapes[c, p] = (count, *shape)
    return shapes


class Copies:
    def __init__(self, send, recv):
        self.send, self.recv, self.all, self.used, self.left = send, recv, {}, 0, set()

    def start(self, key, make):
        self.start_all(key, 1, lambda i: make())

    def start_all(self, key, count, make):
        first = self.used
        self.used += count

        def copy(i):
            src, dst, to = make(i)
            return pltpu.make_async_remote_copy(
                src_ref=src, dst_ref=dst, send_sem=self.send.at[first + i], recv_sem=self.recv.at[first + i], device_id=to, device_id_type=MESH
            )

        self.all[key] = count, copy
        each(count, lambda i: copy(i).start())

    def arrived(self, key):
        count, copy = self.all[key]
        each(count, lambda i: copy(i).wait_recv())

    def sent(self, mine=lambda key: True):
        for key, (count, copy) in self.all.items():
            if key not in self.left and mine(key):
                self.left.add(key)
                each(count, lambda i, copy=copy: copy(i).wait_send())


def each(count, do):
    if count == 1:
        do(0)
    else:

        loop(count)(do)


def loop(count):
    def run(body):
        def step(carry, _):
            body(carry[0])
            return (carry[0] + 1, None), None

        lax.scan(step, (Me.zero, None), None, length=count)

    return run


def total(parts):
    return functools.reduce(jnp.add, [p[...].astype(F32) for p in parts])


def reduce_colour(me, copies, key, kind, colour, grads, received, last, keep=None):
    free, fixed = ("x", "y", "z"), {}
    parts = [lambda at, r=r: view(r(), kind, ("x", "y", "z"), at, colour) for r in grads]
    out = parts[0]

    def add(at, more):
        rest = [d for d in free if d not in at]
        if len(rest) >= 2:
            first = rest[0]

            @loop(SIZES[first])
            def _(i):
                now = {**at, first: i}
                out(now)[...] = total([p(now) for p in parts + more]).astype(BF16)
        else:
            out(at)[...] = total([p(at) for p in parts + more]).astype(BF16)

    for phase, (d, how) in enumerate(COLOURS[colour]):
        n, buffer = SIZES[d], functools.partial(received, colour, phase)
        left = tuple(e for e in ("x", "y", "z") if e not in fixed and e != d)

        def slot(i, buffer=buffer, left=left):
            return lambda at: view(buffer().at[i], kind, left, {e: v for e, v in at.items() if e in left}, colour, own=True)

        if how == RING:
            long, short = lengths(n)
            ways = ((1, long, 0, "l"), (-1, short, long, "s"))
            for s in range(long):
                for sign, length, base, name in ways:
                    if s >= length:
                        continue

                    def make(d=d, fixed=fixed, buffer=buffer, sign=sign, by=length - s, place=base + s):
                        at = {**fixed, d: me.off(d, me.sign * (sign * by))}
                        return out(at), buffer().at[place], me.device(**{d: me.off(d, me.sign * sign)})

                    if s:
                        copies.arrived((key, colour, phase, name, s - 1))
                    add({**fixed, d: me.off(d, me.sign * (sign * (length - s)))}, [slot(base + s - 1)] if s else [])
                    copies.start((key, colour, phase, name, s), make)
                yield
            for sign, length, base, name in ways:
                if length:
                    copies.arrived((key, colour, phase, name, length - 1))
            parts = parts + [slot(base + length - 1) for sign, length, base, name in ways if length]
        else:

            def make(i, d=d, fixed=fixed, buffer=buffer, add=add, out=out):
                to = me.off(d, i + 1)
                return out({**fixed, d: to}), buffer().at[i], me.device(**{d: to})

            each(n - 1, lambda i: add({**fixed, d: me.off(d, i + 1)}, []))
            copies.start_all((key, colour, phase), n - 1, make)
            yield
            copies.arrived((key, colour, phase))
            parts = parts + [slot(i) for i in range(n - 1)]
        fixed = {**fixed, d: me.at[d]}
        if keep is not None and phase == 0:
            copies.sent(lambda k: k[:3] == (key, colour, 0))
            stays = (lambda at, left=left: view(keep, kind, left, {e: v for e, v in at.items() if e in left}, colour, own=True))
            stays(fixed)[...] = out(fixed)[...]
            out = stays
            parts[0] = stays
    last(colour, total([p(fixed) for p in parts]).astype(BF16).astype(F32))


class Reduce:
    def __init__(self, me, own, theirs, halves, buffers, sums, cross, shares, outs, send, recv, free, kept):
        self.me, self.own, self.theirs, self.halves, self.buffers = me, own, theirs, halves, buffers
        self.sums, self.cross, self.shares, self.outs, self.free, self.kept = sums, cross, shares, outs, free, kept
        self.copies = Copies(send, recv)
        self.waiting = set(range(6))
        self.streams = {(i, c): self.colour(i, c) for i in range(6) for c in range(3)} | {(i, 3): self.finish(i) for i in range(6)}

    def slot(self, i):
        kind, j = ORDER[i]
        return 0 if kind == TALL else j // 2

    def half(self, i):
        kind = ORDER[i][0]
        if i >= 3:
            pl.semaphore_wait(self.free.at[i - 3], sum(SIZES.values()) - len(SIZES) + 1)
        self.copies.start(
            (i, "half"), lambda: (self.halves[kind](), self.theirs[kind].at[self.slot(i)], self.me.device(core=1 - self.me.core))
        )

    def half_sent(self, i):
        self.copies.sent(lambda key: key == (i, "half"))

    def colour(self, i, c):
        kind, j = ORDER[i]
        slot = self.slot(i)
        if i in self.waiting:
            self.waiting.discard(i)
            self.copies.arrived((i, "half"))

        def last(colour, value):
            first, size = PART[kind][colour]
            if kind != TALL:
                self.sums[kind][j, 0, :, first : first + size] = value[:4]
                self.sums[kind][j, 1, :, first : first + size] = value[4:]
            else:
                self.sums[TALL][j, first : first + size, :] = value

        grads = (lambda: self.own[kind].at[slot]), (lambda: self.theirs[kind].at[slot])
        keep = self.kept[c] if i == 0 else None
        yield from reduce_colour(self.me, self.copies, i, kind, c, grads, lambda c, p: self.buffers[kind, (c, p)].at[0], last, keep)

    def finish(self, i):
        (kind, j), me, copies = ORDER[i], self.me, self.copies
        sums, cross, shares, outs = self.sums, self.cross, self.shares, self.outs
        mine = 2 * lax.rem(me.at["z"], 2) + me.core
        if kind != TALL:
            copies.start((i, "rows"), lambda: (sums[kind].at[j, 1 - me.core], cross[kind].at[j], me.device(core=1 - me.core)))
        else:
            for q in range(4):
                shares[j, q] = sums[TALL][j, 10 * q : 10 * q + 10, :]
            for o in range(3):

                def make(o=o):
                    z, core = ((me.at["z"], 1 - me.core), (me.pair(), me.core), (me.pair(), 1 - me.core))[o]
                    mine = 2 * lax.rem(me.at["z"], 2) + me.core
                    return shares.at[j, 2 * lax.rem(z, 2) + core], cross[TALL].at[j, mine], me.device(core=core, z=z)

                copies.start((i, "rows", o), make)
        if i < 3:
            for d, n in SIZES.items():
                each(n - 1, lambda o, d=d: self.done(i, me.device(**{d: me.off(d, o + 1)})))
            self.done(i, me.device(core=1 - me.core))
        yield
        mine = 2 * lax.rem(me.at["z"], 2) + me.core
        if kind != TALL:
            copies.arrived((i, "rows"))
            outs[0][j, me.core] = sums[kind][j, me.core]
            outs[0][j, 1 - me.core] = cross[kind][j]
        else:
            for o in range(3):
                copies.arrived((i, "rows", o))
            for q in range(4):
                outs[1][j, q] = jnp.where(q == mine, shares[j, q], cross[TALL][j, q])
        copies.sent(lambda key: key[0] == i)

    def done(self, i, device):
        pl.semaphore_signal(self.free.at[i], inc=1, device_id=device, device_id_type=MESH)

    def run(self, order):
        for i, c in zip(order[::2], order[1::2], strict=True):
            if c == "h":
                self.half(int(i))
            elif c == "s":
                self.half_sent(int(i))
            else:
                next(self.streams[int(i), int(c)], None)


def dot(a, b, ca=1, cb=0):
    return lax.dot_general(a, b, (((ca,), (cb,)), ((), ())), preferred_element_type=F32)


def rem(a, b):
    return a % b if isinstance(a, int) else lax.rem(a, b)


def at_tile(i, size):
    return pl.ds(pl.multiple_of(i * size, size), size)


def put_rows(ref, i, value):
    y, z, rows = ref.shape[1:4]
    for s in range(0, 256, 8):
        row = i * 256 + s
        group = lax.div(row, rows)
        ref[lax.div(group, y * z), rem(lax.div(group, z), y), rem(group, z), pl.ds(pl.multiple_of(rem(row, rows), 8), 8), :] = value[s : s + 8]


def put_all(ref, value):
    ref[...] = value.reshape(ref.shape)


def step_kernel(*refs):
    x_in, dy_in, w_gate, w_up, w_down = refs[:5]
    outs, (gate_kept, up_kept, hidden_kept, a0_kept, h1_kept) = refs[5:7], refs[7:12]
    rest = list(refs[12:])
    take = lambda n: [rest.pop(0) for _ in range(n)]
    act, dy, turned, back, both, gates, ups = take(7)
    tile_g, tile_u, tile_d, rows_w, columns_w = take(5)
    wide_own, wide_theirs, tall_own, tall_half, tall_theirs = take(5)
    wide_sums, tall_sums, wide_cross, tall_cross, shares = take(5)
    load, sem_g, sem_u, sem_d, sem_w, sem_c, sem_f, send, recv, free = take(10)
    buffers = {}
    for kind in KINDS:
        for k in reduce_buffers(kind):
            buffers[kind, k] = rest.pop(0)
    tall_kept = take(3)
    me = Me()

    def fetch(src, dst, sem):
        copy = pltpu.make_async_copy(src, dst, sem)
        copy.start()
        return copy

    class Stream:
        def __init__(self, tile, buffer, sem):
            self.tile, self.buffer, self.sem = tile, buffer, sem

        def copy(self, i):
            slot = rem(i, 2)
            return pltpu.make_async_copy(self.tile(i), self.buffer.at[slot], self.sem.at[slot])

    def stream(*streams, n):
        for s in streams:
            s.copy(0).start()

        def ahead(i):
            @pl.when(i + 1 < n)
            def _():
                for s in streams:
                    s.copy(i + 1).start()

            for s in streams:
                s.copy(i).wait()

        return ahead

    def columns(w, layer, buffer, sem):
        return Stream(lambda i: w.at[layer, :, at_tile(i, 256)], buffer, sem)

    loads = [fetch(x_in, back, load.at[0]), fetch(dy_in, dy, load.at[1])]
    zeroth = stream(columns(w_gate, 0, tile_g, sem_g), columns(w_up, 0, tile_u, sem_u), n=10)

    def half_columns(i, half):
        src = w_down.at[0, pl.ds(half * 1280, 1280), at_tile(i, 256)]
        return pltpu.make_async_copy(src, columns_w.at[half], sem_c.at[half])

    for half in (0, 1):
        half_columns(0, half).start()
    peers = me.arrive()
    own = by_kind(wide_own, tall_own)
    theirs = by_kind(wide_theirs, tall_theirs)
    halves = by_kind(lambda: wide_own.at[2], lambda: tall_half)
    sums, cross = by_kind(wide_sums, tall_sums), by_kind(wide_cross, tall_cross)
    reduce = Reduce(me, own, theirs, halves, buffers, sums, cross, shares, outs, send, recv, free, tall_kept)

    def ticks(phase, i):
        orders = TICKS[phase]
        if any(orders):
            lax.switch(i, [functools.partial(reduce.run, order) for order in orders])

    def norm():
        @pl.loop(0, 8)
        def _(i):
            rows = at_tile(i, 128)
            h = back[rows, :].astype(F32)
            act[rows, :] = (h * lax.rsqrt(jnp.mean(h * h, -1, keepdims=True) + 1e-6)).astype(BF16)

    def turn(src, i):
        i = rem(i, 8)
        turned[:, at_tile(i, 128)] = src[at_tile(i, 128), :].T

    def silu_of(g):
        s = jax.nn.sigmoid(g)
        return g * s, s * (1 + g * (1 - s))

    def unit(i, silu, slope, hidden, d, dout):
        d = d.astype(BF16).astype(F32)
        both[1, :, at_tile(i, 256)] = (d * silu).astype(BF16)
        both[0, :, at_tile(i, 256)] = (d * slope).astype(BF16)
        for ref, core in ((tall_own.at[0], me.core), (tall_half, 1 - me.core)):
            put_rows(ref, i, dot(hidden, dout[:, at_tile(core, 512)]).astype(BF16))

    def wide_grads(phase):
        @pl.loop(0, 4)
        def _(k):
            which, mine = lax.div(k, 2), lax.rem(k, 2)
            core = mine * me.core + (1 - mine) * (1 - me.core)
            value = dot(turned[...], both[which, :, at_tile(core, 1280)]).astype(BF16)
            put_all(wide_own.at[lax.rem(2 - mine * (2 - which), 3)], value)
            ticks(phase, k)

    def kept(i, out):
        slot = rem(i, 2)
        pairs = (gates.at[slot], gate_kept.at[:, at_tile(i, 256)]), (ups.at[slot], up_kept.at[:, at_tile(i, 256)])
        return [pltpu.make_async_copy(*(p if out else p[::-1]), sem_f.at[n, slot]) for n, p in enumerate(pairs)]

    loads[0].wait()
    norm()
    keep = fetch(act, a0_kept, load.at[0])

    @pl.loop(0, 10)
    def _(i):
        zeroth(i)

        @pl.when(i >= 2)
        def _():
            for copy in kept(i - 2, True):
                copy.wait()

        slot = rem(i, 2)
        g, u = dot(act[...], tile_g[slot]), dot(act[...], tile_u[slot])
        silu, slope = silu_of(g)
        gates[slot] = silu
        ups[slot] = u * slope
        both[0, :, at_tile(i, 256)] = (silu * u).astype(BF16)
        for copy in kept(i, True):
            copy.start()

    keep_hidden = fetch(both.at[0], hidden_kept, load.at[2])
    first = stream(
        columns(w_gate, 1, tile_g, sem_g),
        columns(w_up, 1, tile_u, sem_u),
        Stream(lambda i: w_down.at[1, at_tile(i, 256), :], tile_d, sem_d),
        n=10,
    )

    @pl.loop(0, 4)
    def _(i):
        part = 0.0
        for half in (0, 1):
            half_columns(i, half).wait()
            part += dot(both[0, :, half * 1280 : half * 1280 + 1280], columns_w[half])

            @pl.when(i < 3)
            def _():
                half_columns(i + 1, half).start()

        part = part.astype(BF16).astype(F32)
        back[:, at_tile(i, 256)] = (back[:, at_tile(i, 256)].astype(F32) + part).astype(BF16)

    keep.wait()
    keep = fetch(back, h1_kept, load.at[0])
    norm()

    loads[1].wait()
    keep_hidden.wait()

    @pl.loop(0, 10)
    def _(i):
        first(i)
        turn(act, i)
        slot = rem(i, 2)
        silu, slope = silu_of(dot(act[...], tile_g[slot]))
        u = dot(act[...], tile_u[slot])
        unit(i, silu, u * slope, (silu * u).astype(BF16).T, dot(dy[...], tile_d[slot], 1, 1), dy)

    me.arrived(peers)
    reduce.run(TICKS["first"][0])
    wide_grads("wide1")

    keep.wait()
    for i in (8, 9):
        for copy in kept(i, True):
            copy.wait()
    load_h = fetch(h1_kept, turned, load.at[0])

    def weight_rows(k, w):
        slot = rem(k, 2)
        rows = at_tile(k // 2 if isinstance(k, int) else lax.div(k, 2), 256)
        return pltpu.make_async_copy(w.at[1, rows, :], rows_w.at[slot], sem_w.at[slot])

    weight_rows(0, w_gate).start()

    @pl.loop(0, 8)
    def _(k):
        n, which = lax.div(k, 2), lax.rem(k, 2)

        @pl.when(which == 0)
        def _():
            weight_rows(k + 1, w_up).start()

        @pl.when((which == 1) & (k < 7))
        def _():
            weight_rows(k + 1, w_gate).start()

        weight_rows(k, w_gate).wait()
        part = dot(both[which], rows_w[which], 1, 1).astype(BF16).astype(F32)
        before = back[:, at_tile(n, 256)].astype(F32)
        back[:, at_tile(n, 256)] = (jnp.where(which == 0, 0.0, before) + part).astype(BF16)
        ticks("back", k)

    load_h.wait()

    @pl.loop(0, 8)
    def _(i):
        rows = at_tile(i, 128)
        h, d = turned[rows, :].astype(F32), back[rows, :].astype(F32)
        scale = lax.rsqrt(jnp.mean(h * h, -1, keepdims=True) + 1e-6)
        along = jnp.sum(d * h, -1, keepdims=True)
        d = (d * scale - h * (scale * scale * scale * along * (1 / 1024))).astype(BF16)
        act[rows, :] = (dy[rows, :].astype(F32) + d.astype(F32)).astype(BF16)

    load_a = fetch(a0_kept, back, load.at[1])
    second = stream(
        Stream(lambda i: w_down.at[0, at_tile(i, 256), :], tile_d, sem_d),
        Stream(lambda i: hidden_kept.at[:, at_tile(i, 256)], tile_g, sem_g),
        n=10,
    )
    for copy in kept(0, False):
        copy.start()
    load_a.wait()

    @pl.loop(0, 10)
    def _(i):
        @pl.when(i < 9)
        def _():
            for copy in kept(i + 1, False):
                copy.start()

        second(i)
        turn(back, i)
        for copy in kept(i, False):
            copy.wait()
        slot = rem(i, 2)
        unit(i, gates[slot], ups[slot], tile_g[slot].T, dot(act[...], tile_d[slot], 1, 1), act)
        ticks("units", i)

    reduce.run(TICKS["last"][0])
    wide_grads("wide0")
    reduce.run(TICKS["tail"][0])
    for stream_ in reduce.streams.values():
        assert next(stream_, 0) == 0, "not done"
    reduce.copies.sent()


def run(streams, order):
    for i, c in zip(order[::2], order[1::2], strict=True):
        next(streams[int(i), int(c)], None)
    for stream in streams.values():
        assert next(stream, 0) == 0, "not done"


def full_shape(kind):
    return dims(kind, ("x", "y", "z")) + (ROWS[kind], HALF[kind])


def summed(x, dy, w_gate, w_up, w_down):
    square = pltpu.VMEM((1024, 1024), BF16)
    scratch = [square] * 4 + [pltpu.VMEM((2, 1024, 2560), BF16)]
    scratch += [pltpu.VMEM((2, 1024, 256), F32)] * 2
    scratch += [pltpu.VMEM((2, 1024, 256), BF16)] * 2 + [pltpu.VMEM((2, 256, 1024), BF16), pltpu.VMEM((2, 256, 2560), BF16)]
    scratch += [
        pltpu.VMEM((2, 1280, 256), BF16),
        pltpu.VMEM((3, *full_shape(GATE)), BF16),
        pltpu.VMEM((2, *full_shape(GATE)), BF16),
        pltpu.VMEM((1, *full_shape(TALL)), BF16),
        pltpu.VMEM(full_shape(TALL), BF16),
        pltpu.VMEM((1, *full_shape(TALL)), BF16),
        pltpu.VMEM((4, 2, 4, 1280), F32),
        pltpu.VMEM((2, 40, 256), F32),
        pltpu.VMEM((4, 4, 1280), F32),
        pltpu.VMEM((2, 4, 10, 256), F32),
        pltpu.VMEM((2, 4, 10, 256), F32),
        pltpu.SemaphoreType.DMA((3,)),
        *[pltpu.SemaphoreType.DMA((2,))] * 5,
        pltpu.SemaphoreType.DMA((2, 2)),
        pltpu.SemaphoreType.DMA((256,)),
        pltpu.SemaphoreType.DMA((256,)),
        pltpu.SemaphoreType.REGULAR((3,)),
    ]
    for kind in KINDS:
        scratch += [pltpu.VMEM((1, *shape), BF16) for shape in reduce_buffers(kind).values()]
    scratch += [pltpu.VMEM(block(TALL, c, [d for d in "xyz" if d != COLOURS[c][0][0]]), BF16) for c in range(3)]
    kept = [jax.ShapeDtypeStruct((1024, 2560), t) for t in (F32, F32, BF16)] + [jax.ShapeDtypeStruct((1024, 1024), BF16)] * 2
    return pl.pallas_call(
        step_kernel,
        out_shape=(jax.ShapeDtypeStruct((4, 2, 4, 1280), F32), jax.ShapeDtypeStruct((2, 4, 10, 256), F32), *kept),
        in_specs=[pl.BlockSpec(memory_space=pl.ANY)] * 5,
        out_specs=(*[pl.BlockSpec(memory_space=pltpu.VMEM)] * 2, *[pl.BlockSpec(memory_space=pl.ANY)] * 5),
        scratch_shapes=scratch,
        compiler_params=pltpu.CompilerParams(
            collective_id=0, has_side_effects=True, vmem_limit_bytes=VMEM_LIMIT
        ),
        name="step",
    )(x, dy, w_gate, w_up, w_down)[:2]


def gather_colour(me, copies, key, kind, colour, ref):
    base = me.core * HALF[kind]
    fixed = dict(me.at)

    def part(at):
        return view(ref, kind, ("x", "y", "z"), at, colour, base, parts=GATHER_PART)

    phases = COLOURS[colour][::-1]
    for phase, (d, how) in enumerate(phases):
        n, lastly = SIZES[d], phase == len(phases) - 1
        rest = {e: v for e, v in fixed.items() if e != d}
        here = part(fixed)

        def across(name, at):
            if lastly:
                copies.start((key, colour, "across", name), lambda: (part(at), part(at), me.device(core=1 - me.core)))

        if how == RING:
            long, short = lengths(n)
            ways = ((me.sign, long, "l"), (-me.sign, short, "s"))
            for s in range(long):
                for sign, length, name in ways:
                    if s >= length:
                        continue
                    at = {**rest, d: me.off(d, -sign * s)}
                    if s:
                        copies.arrived((key, colour, phase, name, s - 1))
                    copies.start(
                        (key, colour, phase, name, s),
                        lambda at=at, d=d, sign=sign: (part(at), part(at), me.device(**{d: me.off(d, sign)})),
                    )
                    if s:
                        across((name, s - 1), at)
                if s == 0:
                    across("own", fixed)
                yield
            for sign, length, name in ways:
                if length:
                    copies.arrived((key, colour, phase, name, length - 1))
                    across((name, length - 1), {**rest, d: me.off(d, -sign * length)})
        else:
            copies.start_all(
                (key, colour, phase), n - 1, lambda i, d=d, here=here: (here, here, me.device(**{d: me.off(d, i + 1)}))
            )
            yield
            copies.arrived((key, colour, phase))
        fixed = rest
    yield
    names = ["own"]
    d, how = phases[-1]
    long, short = lengths(SIZES[d])
    names += [("l", s) for s in range(long)] + [("s", s) for s in range(short)]
    for name in names:
        copies.arrived((key, colour, "across", name))


def gather_kernel(*refs):
    given, weights = refs[:8], refs[8:11]
    outs, new_m, new_v, rest = refs[11:17], refs[17:20], refs[20:23], refs[23:]
    taken, rest = rest[:8], rest[8:]
    wide_sums, tall_sums, m, v = taken[0], taken[1], taken[2:5], taken[5:8]
    wide, tall = rest[:2]
    cross, rows = by_kind(*rest[2:4]), by_kind(*rest[4:6])
    forty, load, send, recv = rest[6:10]
    me = Me()
    mine = 2 * lax.rem(me.at["z"], 2) + me.core

    def which(i):
        kind, j = ORDER[i]
        return (2, j) if kind == TALL else (j // 2, j % 2)

    loads = []
    takes = [pltpu.make_async_copy(*pair, load.at[6 + n]) for n, pair in enumerate(zip(given, taken, strict=True))]
    for copy in takes:
        copy.start()
    for i, (kind, j) in enumerate(ORDER):
        n, layer = which(i)
        group = me.at["x"] * SIZES["y"] + me.at["y"]
        z = me.at["z"] if kind != TALL else lax.div(me.at["z"], 2)
        first = (group * dims(kind, "z")[0] + z) * ROWS[kind]
        src = weights[n].at[layer, pl.ds(pl.multiple_of(first, 8), ROWS[kind]), :]
        loads.append(pltpu.make_async_copy(src, rows[kind].at[j], load.at[i]))
        loads[-1].start()
    peers = me.arrive()
    copies = Copies(send, recv)
    for copy in takes:
        copy.wait()

    def update(i):
        kind, j = ORDER[i]
        n, layer = which(i)
        loads[i].wait()
        many, width = (2, HALF[kind]) if kind != TALL else (4, HALF[TALL] // 2)
        for q in range(many):
            at = pl.ds((q if kind != TALL else q % 2 * 2 + q // 2) * width, width)
            here = (layer, slice(None), at) if kind != TALL else (slice(None), layer, at)
            w = rows[kind][j, :, at].astype(F32)
            size = ROWS[kind] // many
            own = w[:size]
            for p in range(1, many):
                own = jnp.where((me.core if kind != TALL else mine) == p, w[p * size : (p + 1) * size], own)
            sums, fresh = (wide_sums, wide) if kind != TALL else (tall_sums, tall)
            value, new_m[n][here], new_v[n][here] = adamw(own, m[n][here], v[n][here], sums[j, q])
            fresh[j, q] = value.astype(F32)
        if not copies.used:
            me.arrived(peers)
        if kind != TALL:
            copies.start((i, "rows"), lambda: (wide.at[j, 1 - me.core], cross[kind].at[j], me.device(core=1 - me.core)))
        else:
            for o, (z, core) in enumerate(((me.at["z"], 1 - me.core), (me.pair(), me.core), (me.pair(), 1 - me.core))):
                q = 2 * lax.rem(z, 2) + core
                copies.start(
                    (i, "rows", o),
                    lambda q=q, z=z, core=core: (tall.at[j, q], cross[TALL].at[j, mine], me.device(core=core, z=z)),
                )

    def begin(i):
        kind, j = ORDER[i]
        here = view(outs[i], kind, ("x", "y", "z"), me.at, None, me.core * HALF[kind])
        if kind != TALL:
            copies.arrived((i, "rows"))
            own, theirs = wide[j, me.core], cross[kind][j]
            first = me.core == 0
            rows = [jnp.where(first, own, theirs), jnp.where(first, theirs, own)]
            here[...] = jnp.concatenate(rows, axis=0).astype(BF16)
        else:
            for o in range(3):
                copies.arrived((i, "rows", o))
            for q in range(4):
                forty[10 * q : 10 * q + 10, :] = jnp.where(q == mine, tall[j, q], cross[TALL][j, q])
            here[...] = forty[...].astype(BF16)

    def colour(i, c):
        if i in waiting:
            waiting.discard(i)
            for following in turns[turns.index(i) + 2 :][:1]:
                update(following)
            begin(i)
        yield from gather_colour(me, copies, i, ORDER[i][0], c, outs[i])

    waiting = set(range(6))
    turns = list(dict.fromkeys(int(i) for i in GATHER_ORDER[::2]))
    update(turns[0])
    update(turns[1])
    run({(i, c): colour(i, c) for i in range(6) for c in range(3)}, GATHER_ORDER)
    copies.sent()


def all_gather(wide, tall, m, v, weights):
    moments = [pltpu.VMEM(t.shape, F32) for t in m]
    scratch = [
        *(pltpu.VMEM(t.shape, F32) for t in (wide, tall, *m, *v)),
        pltpu.VMEM((4, 2, 4, 1280), F32),
        pltpu.VMEM((2, 4, 10, 256), F32),
        pltpu.VMEM((4, 4, 1280), F32),
        pltpu.VMEM((2, 4, 10, 256), F32),
        pltpu.VMEM((4, ROWS[GATE], 2560), BF16),
        pltpu.VMEM((2, ROWS[TALL], 1024), BF16),
        pltpu.VMEM((40, 256), F32),
        pltpu.SemaphoreType.DMA((14,)),
        pltpu.SemaphoreType.DMA((384,)),
        pltpu.SemaphoreType.DMA((384,)),
    ]
    matrices = [pltpu.VMEM((*dims(kind, ("x", "y", "z")), ROWS[kind], 2 * HALF[kind]), BF16) for kind, _ in ORDER]
    return pl.pallas_call(
        gather_kernel,
        out_shape=(*matrices, *moments, *moments),
        in_specs=[pl.BlockSpec(memory_space=pl.ANY)] * 11,
        out_specs=(pl.BlockSpec(memory_space=pltpu.VMEM),) * 12,
        scratch_shapes=scratch,
        compiler_params=pltpu.CompilerParams(collective_id=1, has_side_effects=True, vmem_limit_bytes=28 * 1024 * 1024),
        name="all_gather",
    )(wide, tall, *m, *v, *weights)


def spill_kernel(*refs):
    ins, moments, outs, sem = refs[:6], refs[6:12], refs[12:21], refs[21]
    copies = []
    for i, (kind, j) in enumerate(ORDER):
        which, layer = (2, j) if kind == TALL else (j // 2, j % 2)
        copies.append(pltpu.make_async_copy(ins[i], outs[which].at[layer], sem.at[i]))
    for i in range(6):
        copies.append(pltpu.make_async_copy(moments[i], outs[3 + i], sem.at[6 + i]))
    for copy in copies:
        copy.start()
    for copy in copies:
        copy.wait()


def spill(new):
    wide, tall = ((2, *dims(kind, ("x", "y", "z")), ROWS[kind], 2 * HALF[kind]) for kind in (GATE, TALL))
    return pl.pallas_call(
        spill_kernel,
        out_shape=(*(jax.ShapeDtypeStruct(shape, BF16) for shape in (wide, wide, tall)), *(jax.ShapeDtypeStruct(t.shape, F32) for t in new[6:])),
        in_specs=[pl.BlockSpec(memory_space=pltpu.VMEM)] * 12,
        out_specs=(pl.BlockSpec(memory_space=pl.ANY),) * 9,
        scratch_shapes=[pltpu.SemaphoreType.DMA((12,))],
        compiler_params=pltpu.CompilerParams(vmem_limit_bytes=1024 * 1024),
        name="spill",
    )(*new)


def adamw(w, m, v, g):
    m = 0.9 * m + 0.1 * g
    v = 0.95 * v + 0.05 * g * g
    step = m * lax.rsqrt(v + 1e-8) + 0.1 * w
    return (w - 0.02 * step).astype(BF16), m, v


def solution(mesh):
    def step(x, dy, *arrays):
        weights, m, v = (arrays[i : i + 3] for i in (0, 3, 6))
        m, v = ((*t[:2], t[2].transpose(1, 0, 2)) for t in (m, v))
        new = spill(all_gather(*summed(x[0], dy[0], *weights), m, v, weights))
        m, v = ((*t[:2], t[2].transpose(1, 0, 2)) for t in (new[3:6], new[6:9]))
        return (*(w.reshape(2, -1, w.shape[-1]) for w in new[:3]), *m, *v)

    batch, whole, rows = P(("rep", "dp")), P(), P(None, "dp")
    return jax.shard_map(
        step,
        mesh=mesh,
        in_specs=(batch, batch, *(whole,) * 3, *(rows,) * 6),
        out_specs=(*(P("rep"),) * 3, *(P("rep", "dp"),) * 6),
        check_vma=False,
    )
```

```python
import functools

import jax
import jax.numpy as jnp
from jax import lax
from jax.experimental import pallas as pl
from jax.experimental.pallas import tpu as pltpu
from jax.sharding import PartitionSpec as P

NAMES = ("w_gate", "w_up", "w_down")
MESH = pl.DeviceIdType.MESH
F32, BF16 = jnp.float32, jnp.bfloat16
SIZES = {"x": 4, "y": 4, "z": 8}
VMEM_LIMIT = 64 * 1024 * 1024 - 64 * 1024

TICKS = {
    "first": ["0h"],
    "wide1": ["1h", "1s010200", "2h121011", "0200"],
    "back": ["0112212022", "", "10020011", "12", "0122", "02002120", "1211", "0110002221020s"],
    "units": ["0112100020112122", "02", "", "12102011010203032122", "", "1220", "22", "1011131321", "", "20222323"],
    "last": ["3h"],
    "wide0": ["4h", "4s313230", "5h404241", "3230"],
    "tail": ["31524250514041323052423150513241523040314251303250404152314251504132405230514250313233335241424043435152505353"],
}
GATHER_ORDER = "023120220100113012321040412152514250022212325242312002012220001211322030520042103101403011410020102131014051023011504110221200313220522120514201024022301150411231323110520142000111210250510011412240123221305242300210510222501012412232124041322152504240215152504251"


RING, DIRECT = "ring", "direct"
COLOURS = (
    (("x", RING), ("y", RING), ("z", DIRECT)),
    (("y", RING), ("x", RING), ("z", DIRECT)),
    (("z", RING), ("x", DIRECT), ("y", DIRECT)),
)
GATE, UP, TALL = KINDS = "gate", "up", "tall"
PART = {
    GATE: ((0, 512), (512, 384), (896, 384)),
    UP: ((0, 512), (512, 384), (896, 384)),
    TALL: ((0, 8), (8, 16), (24, 16)),
}
GATHER_PART = {
    GATE: ((0, 512), (512, 384), (896, 384)),
    UP: ((0, 256), (256, 384), (640, 640)),
    TALL: ((0, 16), (16, 16), (32, 8)),
}
HALF = {GATE: 1280, UP: 1280, TALL: 512}
ROWS = {GATE: 8, UP: 8, TALL: 40}
ORDER = ((TALL, 1), (GATE, 1), (UP, 3), (TALL, 0), (GATE, 0), (UP, 2))


def by_kind(wide, tall):
    return {GATE: wide, UP: wide, TALL: tall}


class Me:
    def __init__(self):
        index = lax.axis_index("dp")
        Me.zero = index * 0
        self.core = lax.rem(index, 2)
        chip = index // 2
        self.at = {
            "z": lax.rem(chip, SIZES["z"]),
            "y": lax.rem(chip // SIZES["z"], SIZES["y"]),
            "x": chip // (SIZES["z"] * SIZES["y"]),
        }
        self.sign = 1 - 2 * self.core

    def off(self, d, by):
        return lax.rem(self.at[d] + by + SIZES[d], SIZES[d])

    def device(self, core=None, **at):
        at = {**self.at, **at}
        core = self.core if core is None else core
        return (0, ((at["x"] * SIZES["y"] + at["y"]) * SIZES["z"] + at["z"]) * 2 + core)

    def arrive(self):
        sem = pltpu.get_barrier_semaphore()

        def signal(peer):
            pl.semaphore_signal(sem, inc=1, device_id=peer, device_id_type=MESH)

        for d, n in SIZES.items():
            each(n - 1, lambda i, d=d: signal(self.device(**{d: self.off(d, i + 1)})))
        signal(self.device(core=1 - self.core))
        signal(self.device(core=1 - self.core, z=self.pair()))
        return sem

    def arrived(self, sem):
        pl.semaphore_wait(sem, sum(SIZES.values()) - 1)

    def quarter(self):
        return 2 * lax.rem(self.at["z"], 2) + self.core

    def others(self):
        return (self.at["z"], 1 - self.core), (self.pair(), self.core), (self.pair(), 1 - self.core)

    def pair(self):
        return self.at["z"] + 1 - 2 * lax.rem(self.at["z"], 2)


def quarter(z, core):
    return pl.ds(pl.multiple_of(core * 512 + lax.rem(z, 2) * 256, 256), 256)


def dims(kind, free):
    return tuple(SIZES[d] // (2 if kind == TALL and d == "z" else 1) for d in free)


def view(ref, kind, free, fixed, colour=None, base=0, own=False, parts=PART):
    index = [(fixed[d] // 2 if kind == TALL and d == "z" else fixed[d]) if d in fixed else slice(None) for d in free]
    if own and not (kind == TALL and "z" in free and "z" in fixed):
        return ref.at[(*index, slice(None), slice(None))]
    if kind != TALL:
        first, size = (0, HALF[kind]) if colour is None else parts[kind][colour]
        rows, columns = slice(None), pl.ds(_at(base, first), size)
    else:
        rows = slice(None) if own or colour is None else pl.ds(*parts[TALL][colour])
        if "z" in free and "z" in fixed:
            columns = pl.ds(pl.multiple_of(base + lax.rem(fixed["z"], 2) * 256, 256), 256)
        else:
            columns = pl.ds(_at(base, 0), HALF[TALL])
    return ref.at[(*index, rows, columns)]


def _at(base, first):
    return first if isinstance(base, int) and base == 0 else pl.multiple_of(base + first, 128)


def block(kind, colour, free):
    first, size = PART[kind][colour]
    tail = (8, size) if kind != TALL else (size, HALF[TALL] if "z" in free else HALF[TALL] // 2)
    return dims(kind, free) + tail


def lengths(n):
    return n // 2, (n - 1) // 2


def reduce_buffers(kind):
    shapes = {}
    for c, phases in enumerate(COLOURS):
        free = ["x", "y", "z"]
        for p, (d, how) in enumerate(phases):
            free.remove(d)
            shape = block(kind, c, tuple(free))
            count = SIZES[d] - 1
            shapes[c, p] = (count, *shape)
    return shapes


class Copies:
    def __init__(self, send, recv):
        self.send, self.recv, self.all, self.used, self.left = send, recv, {}, 0, set()

    def start(self, key, make):
        self.start_all(key, 1, lambda i: make())

    def start_all(self, key, count, make):
        first = self.used
        self.used += count
        assert self.used <= self.send.shape[0]

        def copy(i):
            src, dst, to = make(i)
            return pltpu.make_async_remote_copy(
                src_ref=src, dst_ref=dst, send_sem=self.send.at[first + i], recv_sem=self.recv.at[first + i], device_id=to, device_id_type=MESH
            )

        self.all[key] = count, copy
        each(count, lambda i: copy(i).start())

    def arrived(self, key):
        count, copy = self.all[key]
        each(count, lambda i: copy(i).wait_recv())

    def sent(self, mine=lambda key: True):
        for key, (count, copy) in self.all.items():
            if key not in self.left and mine(key):
                self.left.add(key)
                each(count, lambda i, copy=copy: copy(i).wait_send())


def each(count, do):
    if count == 1:
        do(0)
    else:

        loop(count)(do)


def loop(count):
    def run(body):
        def step(carry, _):
            body(carry[0])
            return (carry[0] + 1, None), None

        lax.scan(step, (Me.zero, None), None, length=count)

    return run


def total(parts):
    return functools.reduce(jnp.add, [p[...].astype(F32) for p in parts])


def reduce_colour(me, copies, key, kind, colour, grads, received, last, keep=None):
    free, fixed = ("x", "y", "z"), {}
    parts = [lambda at, r=r: view(r(), kind, ("x", "y", "z"), at, colour) for r in grads]
    out = parts[0]

    def add(at, more):
        rest = [d for d in free if d not in at]
        if len(rest) >= 2:
            first = rest[0]

            @loop(SIZES[first])
            def _(i):
                now = {**at, first: i}
                out(now)[...] = total([p(now) for p in parts + more]).astype(BF16)
        else:
            out(at)[...] = total([p(at) for p in parts + more]).astype(BF16)

    for phase, (d, how) in enumerate(COLOURS[colour]):
        n, buffer = SIZES[d], functools.partial(received, colour, phase)
        left = tuple(e for e in ("x", "y", "z") if e not in fixed and e != d)

        def slot(i, buffer=buffer, left=left):
            return lambda at: view(buffer().at[i], kind, left, {e: v for e, v in at.items() if e in left}, colour, own=True)

        if how == RING:
            long, short = lengths(n)
            ways = ((1, long, 0, "l"), (-1, short, long, "s"))
            for s in range(long):
                for sign, length, base, name in ways:
                    if s >= length:
                        continue

                    def make(d=d, fixed=fixed, buffer=buffer, sign=sign, by=length - s, place=base + s):
                        at = {**fixed, d: me.off(d, me.sign * (sign * by))}
                        return out(at), buffer().at[place], me.device(**{d: me.off(d, me.sign * sign)})

                    if s:
                        copies.arrived((key, colour, phase, name, s - 1))
                    add({**fixed, d: me.off(d, me.sign * (sign * (length - s)))}, [slot(base + s - 1)] if s else [])
                    copies.start((key, colour, phase, name, s), make)
                yield
            for sign, length, base, name in ways:
                if length:
                    copies.arrived((key, colour, phase, name, length - 1))
            parts = parts + [slot(base + length - 1) for sign, length, base, name in ways if length]
        else:

            def make(i, d=d, fixed=fixed, buffer=buffer, add=add, out=out):
                to = me.off(d, i + 1)
                return out({**fixed, d: to}), buffer().at[i], me.device(**{d: to})

            each(n - 1, lambda i: add({**fixed, d: me.off(d, i + 1)}, []))
            copies.start_all((key, colour, phase), n - 1, make)
            yield
            copies.arrived((key, colour, phase))
            parts = parts + [slot(i) for i in range(n - 1)]
        fixed = {**fixed, d: me.at[d]}
        if keep is not None and phase == 0:
            copies.sent(lambda k: k[:3] == (key, colour, 0))
            stays = (lambda at, left=left: view(keep, kind, left, {e: v for e, v in at.items() if e in left}, colour, own=True))
            stays(fixed)[...] = out(fixed)[...]
            out = stays
            parts[0] = stays
    last(colour, total([p(fixed) for p in parts]).astype(BF16).astype(F32))


class Reduce:
    def __init__(self, me, own, theirs, halves, buffers, sums, send, recv, free, kept):
        self.me, self.own, self.theirs, self.halves, self.buffers = me, own, theirs, halves, buffers
        self.sums, self.free, self.kept = sums, free, kept
        self.copies = Copies(send, recv)
        self.waiting = set(range(6))
        self.streams = {(i, c): self.colour(i, c) for i in range(6) for c in range(3)} | {(i, 3): self.finish(i) for i in range(6)}

    def slot(self, i):
        kind, j = ORDER[i]
        return 0 if kind == TALL else j // 2

    def half(self, i):
        kind = ORDER[i][0]
        if i >= 3:
            pl.semaphore_wait(self.free.at[i - 3], sum(SIZES.values()) - len(SIZES) + 1)
        self.copies.start(
            (i, "half"), lambda: (self.halves[kind](), self.theirs[kind].at[self.slot(i)], self.me.device(core=1 - self.me.core))
        )

    def half_sent(self, i):
        self.copies.sent(lambda key: key == (i, "half"))

    def colour(self, i, c):
        kind, j = ORDER[i]
        slot = self.slot(i)
        if i in self.waiting:
            self.waiting.discard(i)
            self.copies.arrived((i, "half"))

        def last(colour, value):
            first, size = PART[kind][colour]
            if kind != TALL:
                self.sums[kind][j, 0, :, first : first + size] = value[:4]
                self.sums[kind][j, 1, :, first : first + size] = value[4:]
            else:
                self.sums[TALL][j, first : first + size, :] = value

        grads = (lambda: self.own[kind].at[slot]), (lambda: self.theirs[kind].at[slot])
        keep = self.kept[c] if i == 0 else None
        yield from reduce_colour(self.me, self.copies, i, kind, c, grads, lambda c, p: self.buffers[kind, (c, p)].at[0], last, keep)

    def finish(self, i):
        if i < 3:
            for d, n in SIZES.items():
                each(n - 1, lambda o, d=d: self.done(i, self.me.device(**{d: self.me.off(d, o + 1)})))
            self.done(i, self.me.device(core=1 - self.me.core))
        self.copies.sent(lambda key: key[0] == i)
        yield

    def done(self, i, device):
        pl.semaphore_signal(self.free.at[i], inc=1, device_id=device, device_id_type=MESH)

    def run(self, order):
        for i, c in zip(order[::2], order[1::2], strict=True):
            if c == "h":
                self.half(int(i))
            elif c == "s":
                self.half_sent(int(i))
            else:
                next(self.streams[int(i), int(c)], None)


def dot(a, b, ca=1, cb=0):
    return lax.dot_general(a, b, (((ca,), (cb,)), ((), ())), preferred_element_type=F32)


def rem(a, b):
    return a % b if isinstance(a, int) else lax.rem(a, b)


def at_tile(i, size):
    return pl.ds(pl.multiple_of(i * size, size), size)


def put_rows(ref, i, value):
    y, z, rows = ref.shape[1:4]
    for s in range(0, 256, 8):
        row = i * 256 + s
        group = lax.div(row, rows)
        ref[lax.div(group, y * z), rem(lax.div(group, z), y), rem(group, z), pl.ds(pl.multiple_of(rem(row, rows), 8), 8), :] = value[s : s + 8]


def put_all(ref, value):
    ref[...] = value.reshape(ref.shape)


def step_kernel(*refs):
    x_in, dy_in, w_gate, w_up, w_down = refs[:5]
    moments, outs, (wide_moments, tall_moments), rest = (refs[5:8], refs[8:11]), refs[11:13], refs[13:15], list(refs[15:])
    gate_kept, up_kept, hidden_kept, a0_kept, h1_kept = rest[:5]
    rest = rest[5:]
    take = lambda n: [rest.pop(0) for _ in range(n)]
    act, dy, turned, back, both, gates, ups = take(7)
    tile_g, tile_u, tile_d, rows_w, columns_w = take(5)
    wide_own, wide_theirs, tall_own, tall_half, tall_theirs = take(5)
    load, sem_g, sem_u, sem_d, sem_w, sem_c, sem_f, send, recv, free = take(10)
    buffers = {}
    for kind in KINDS:
        for k in reduce_buffers(kind):
            buffers[kind, k] = rest.pop(0)
    tall_kept = take(3)
    me = Me()

    def fetch(src, dst, sem):
        copy = pltpu.make_async_copy(src, dst, sem)
        copy.start()
        return copy

    class Stream:
        def __init__(self, tile, buffer, sem):
            self.tile, self.buffer, self.sem = tile, buffer, sem

        def copy(self, i):
            slot = rem(i, 2)
            return pltpu.make_async_copy(self.tile(i), self.buffer.at[slot], self.sem.at[slot])

    def stream(*streams, n):
        for s in streams:
            s.copy(0).start()

        def ahead(i):
            @pl.when(i + 1 < n)
            def _():
                for s in streams:
                    s.copy(i + 1).start()

            for s in streams:
                s.copy(i).wait()

        return ahead

    def columns(w, layer, buffer, sem):
        return Stream(lambda i: w.at[layer, :, at_tile(i, 256)], buffer, sem)

    loads = [fetch(x_in, back, load.at[0]), fetch(dy_in, dy, load.at[1])]
    zeroth = stream(columns(w_gate, 0, tile_g, sem_g), columns(w_up, 0, tile_u, sem_u), n=10)

    def half_columns(i, half):
        src = w_down.at[0, pl.ds(half * 1280, 1280), at_tile(i, 256)]
        return pltpu.make_async_copy(src, columns_w.at[half], sem_c.at[half])

    for half in (0, 1):
        half_columns(0, half).start()
    peers = me.arrive()
    own = by_kind(wide_own, tall_own)
    theirs = by_kind(wide_theirs, tall_theirs)
    halves = by_kind(lambda: wide_own.at[2], lambda: tall_half)
    reduce = Reduce(me, own, theirs, halves, buffers, by_kind(*outs), send, recv, free, tall_kept)

    def ticks(phase, i):
        orders = TICKS[phase]
        if any(orders):
            lax.switch(i, [functools.partial(reduce.run, order) for order in orders])

    def norm():
        @pl.loop(0, 8)
        def _(i):
            rows = at_tile(i, 128)
            h = back[rows, :].astype(F32)
            act[rows, :] = (h * lax.rsqrt(jnp.mean(h * h, -1, keepdims=True) + 1e-6)).astype(BF16)

    def turn(src, i):
        i = rem(i, 8)
        turned[:, at_tile(i, 128)] = src[at_tile(i, 128), :].T

    def silu_of(g):
        s = jax.nn.sigmoid(g)
        return g * s, s * (1 + g * (1 - s))

    def unit(i, silu, slope, hidden, d, dout):
        d = d.astype(BF16).astype(F32)
        both[1, :, at_tile(i, 256)] = (d * silu).astype(BF16)
        both[0, :, at_tile(i, 256)] = (d * slope).astype(BF16)
        for ref, core in ((tall_own.at[0], me.core), (tall_half, 1 - me.core)):
            put_rows(ref, i, dot(hidden, dout[:, at_tile(core, 512)]).astype(BF16))

    def wide_grads(phase):
        @pl.loop(0, 4)
        def _(k):
            which, mine = lax.div(k, 2), lax.rem(k, 2)
            core = mine * me.core + (1 - mine) * (1 - me.core)
            value = dot(turned[...], both[which, :, at_tile(core, 1280)]).astype(BF16)
            put_all(wide_own.at[lax.rem(2 - mine * (2 - which), 3)], value)
            ticks(phase, k)

    def kept(i, out):
        slot = rem(i, 2)
        pairs = (gates.at[slot], gate_kept.at[:, at_tile(i, 256)]), (ups.at[slot], up_kept.at[:, at_tile(i, 256)])
        return [pltpu.make_async_copy(*(p if out else p[::-1]), sem_f.at[n, slot]) for n, p in enumerate(pairs)]

    loads[0].wait()
    norm()
    keep = fetch(act, a0_kept, load.at[0])

    @pl.loop(0, 10)
    def _(i):
        zeroth(i)

        @pl.when(i >= 2)
        def _():
            for copy in kept(i - 2, True):
                copy.wait()

        slot = rem(i, 2)
        g, u = dot(act[...], tile_g[slot]), dot(act[...], tile_u[slot])
        silu, slope = silu_of(g)
        gates[slot] = silu
        ups[slot] = u * slope
        both[0, :, at_tile(i, 256)] = (silu * u).astype(BF16)
        for copy in kept(i, True):
            copy.start()

    keep_hidden = fetch(both.at[0], hidden_kept, load.at[2])
    first = stream(
        columns(w_gate, 1, tile_g, sem_g),
        columns(w_up, 1, tile_u, sem_u),
        Stream(lambda i: w_down.at[1, at_tile(i, 256), :], tile_d, sem_d),
        n=10,
    )

    @pl.loop(0, 4)
    def _(i):
        part = 0.0
        for half in (0, 1):
            half_columns(i, half).wait()
            part += dot(both[0, :, half * 1280 : half * 1280 + 1280], columns_w[half])

            @pl.when(i < 3)
            def _():
                half_columns(i + 1, half).start()

        part = part.astype(BF16).astype(F32)
        back[:, at_tile(i, 256)] = (back[:, at_tile(i, 256)].astype(F32) + part).astype(BF16)

    keep.wait()
    keep = fetch(back, h1_kept, load.at[0])
    norm()

    loads[1].wait()
    keep_hidden.wait()

    @pl.loop(0, 10)
    def _(i):
        first(i)
        turn(act, i)
        slot = rem(i, 2)
        silu, slope = silu_of(dot(act[...], tile_g[slot]))
        u = dot(act[...], tile_u[slot])
        unit(i, silu, u * slope, (silu * u).astype(BF16).T, dot(dy[...], tile_d[slot], 1, 1), dy)

    me.arrived(peers)
    for n, three in enumerate(moments):
        for which in (0, 1):

            def make(n=n, which=which, three=three):
                theirs = pl.ds(pl.multiple_of((1 - me.core) * 1280, 1280), 1280)
                return three[which].at[:, :, theirs], wide_moments.at[n, pl.ds(2 * which, 2)], me.device(core=1 - me.core)

            reduce.copies.start(("moments", n, which), make)
        for o in range(3):

            def make(n=n, o=o, three=three):
                z, core = me.others()[o]
                return three[2].at[:, :, quarter(z, core)], tall_moments.at[n, me.quarter()], me.device(core=core, z=z)

            reduce.copies.start(("moments", n, 2 + o), make)
    reduce.run(TICKS["first"][0])
    wide_grads("wide1")

    keep.wait()
    for i in (8, 9):
        for copy in kept(i, True):
            copy.wait()
    load_h = fetch(h1_kept, turned, load.at[0])

    def weight_rows(k, w):
        slot = rem(k, 2)
        rows = at_tile(k // 2 if isinstance(k, int) else lax.div(k, 2), 256)
        return pltpu.make_async_copy(w.at[1, rows, :], rows_w.at[slot], sem_w.at[slot])

    weight_rows(0, w_gate).start()

    @pl.loop(0, 8)
    def _(k):
        n, which = lax.div(k, 2), lax.rem(k, 2)

        @pl.when(which == 0)
        def _():
            weight_rows(k + 1, w_up).start()

        @pl.when((which == 1) & (k < 7))
        def _():
            weight_rows(k + 1, w_gate).start()

        weight_rows(k, w_gate).wait()
        part = dot(both[which], rows_w[which], 1, 1).astype(BF16).astype(F32)
        before = back[:, at_tile(n, 256)].astype(F32)
        back[:, at_tile(n, 256)] = (jnp.where(which == 0, 0.0, before) + part).astype(BF16)
        ticks("back", k)

    load_h.wait()

    @pl.loop(0, 8)
    def _(i):
        rows = at_tile(i, 128)
        h, d = turned[rows, :].astype(F32), back[rows, :].astype(F32)
        scale = lax.rsqrt(jnp.mean(h * h, -1, keepdims=True) + 1e-6)
        along = jnp.sum(d * h, -1, keepdims=True)
        d = (d * scale - h * (scale * scale * scale * along * (1 / 1024))).astype(BF16)
        act[rows, :] = (dy[rows, :].astype(F32) + d.astype(F32)).astype(BF16)

    load_a = fetch(a0_kept, back, load.at[1])
    second = stream(
        Stream(lambda i: w_down.at[0, at_tile(i, 256), :], tile_d, sem_d),
        Stream(lambda i: hidden_kept.at[:, at_tile(i, 256)], tile_g, sem_g),
        n=10,
    )
    for copy in kept(0, False):
        copy.start()
    load_a.wait()

    @pl.loop(0, 10)
    def _(i):
        @pl.when(i < 9)
        def _():
            for copy in kept(i + 1, False):
                copy.start()

        second(i)
        turn(back, i)
        for copy in kept(i, False):
            copy.wait()
        slot = rem(i, 2)
        unit(i, gates[slot], ups[slot], tile_g[slot].T, dot(act[...], tile_d[slot], 1, 1), act)
        ticks("units", i)

    reduce.run(TICKS["last"][0])
    wide_grads("wide0")
    reduce.run(TICKS["tail"][0])
    for stream_ in reduce.streams.values():
        assert next(stream_, 0) == 0, "not done"
    for n in range(2):
        for o in range(5):
            reduce.copies.arrived(("moments", n, o))
    reduce.copies.sent()


def run(streams, order):
    for i, c in zip(order[::2], order[1::2], strict=True):
        next(streams[int(i), int(c)], None)
    for stream in streams.values():
        assert next(stream, 0) == 0, "not done"


def full_shape(kind):
    return dims(kind, ("x", "y", "z")) + (ROWS[kind], HALF[kind])


def summed(x, dy, w_gate, w_up, w_down, m, v):
    square = pltpu.VMEM((1024, 1024), BF16)
    scratch = [square] * 4 + [pltpu.VMEM((2, 1024, 2560), BF16)]
    scratch += [pltpu.VMEM((2, 1024, 256), F32)] * 2
    scratch += [pltpu.VMEM((2, 1024, 256), BF16)] * 2 + [pltpu.VMEM((2, 256, 1024), BF16), pltpu.VMEM((2, 256, 2560), BF16)]
    scratch += [
        pltpu.VMEM((2, 1280, 256), BF16),
        pltpu.VMEM((3, *full_shape(GATE)), BF16),
        pltpu.VMEM((2, *full_shape(GATE)), BF16),
        pltpu.VMEM((1, *full_shape(TALL)), BF16),
        pltpu.VMEM(full_shape(TALL), BF16),
        pltpu.VMEM((1, *full_shape(TALL)), BF16),
        pltpu.SemaphoreType.DMA((3,)),
        *[pltpu.SemaphoreType.DMA((2,))] * 5,
        pltpu.SemaphoreType.DMA((2, 2)),
        pltpu.SemaphoreType.DMA((256,)),
        pltpu.SemaphoreType.DMA((256,)),
        pltpu.SemaphoreType.REGULAR((3,)),
    ]
    for kind in KINDS:
        scratch += [pltpu.VMEM((1, *shape), BF16) for shape in reduce_buffers(kind).values()]
    scratch += [pltpu.VMEM(block(TALL, c, [d for d in "xyz" if d != COLOURS[c][0][0]]), BF16) for c in range(3)]
    kept = [jax.ShapeDtypeStruct((1024, 2560), t) for t in (F32, F32, BF16)] + [jax.ShapeDtypeStruct((1024, 1024), BF16)] * 2
    return pl.pallas_call(
        step_kernel,
        out_shape=(
            jax.ShapeDtypeStruct((4, 2, 4, 1280), F32),
            jax.ShapeDtypeStruct((2, 40, 256), F32),
            jax.ShapeDtypeStruct((2, 4, 4, 1280), F32),
            jax.ShapeDtypeStruct((2, 4, 10, 2, 256), F32),
            *kept,
        ),
        in_specs=[pl.BlockSpec(memory_space=pl.ANY)] * 11,
        out_specs=(*[pl.BlockSpec(memory_space=pltpu.VMEM)] * 2, *[pl.BlockSpec(memory_space=pl.ANY)] * 7),
        scratch_shapes=scratch,
        compiler_params=pltpu.CompilerParams(
            collective_id=0, has_side_effects=True, vmem_limit_bytes=VMEM_LIMIT
        ),
        name="step",
    )(x, dy, w_gate, w_up, w_down, *m, *v)[:4]


def gather_colour(me, copies, key, kind, colour, ref):
    base = me.core * HALF[kind]
    fixed = dict(me.at)

    def part(at):
        return view(ref, kind, ("x", "y", "z"), at, colour, base, parts=GATHER_PART)

    phases = COLOURS[colour][::-1]
    for phase, (d, how) in enumerate(phases):
        n, lastly = SIZES[d], phase == len(phases) - 1
        rest = {e: v for e, v in fixed.items() if e != d}
        here = part(fixed)

        def across(name, at):
            if lastly:
                copies.start((key, colour, "across", name), lambda: (part(at), part(at), me.device(core=1 - me.core)))

        if how == RING:
            long, short = lengths(n)
            ways = ((me.sign, long, "l"), (-me.sign, short, "s"))
            for s in range(long):
                for sign, length, name in ways:
                    if s >= length:
                        continue
                    at = {**rest, d: me.off(d, -sign * s)}
                    if s:
                        copies.arrived((key, colour, phase, name, s - 1))
                    copies.start(
                        (key, colour, phase, name, s),
                        lambda at=at, d=d, sign=sign: (part(at), part(at), me.device(**{d: me.off(d, sign)})),
                    )
                    if s:
                        across((name, s - 1), at)
                if s == 0:
                    across("own", fixed)
                yield
            for sign, length, name in ways:
                if length:
                    copies.arrived((key, colour, phase, name, length - 1))
                    across((name, length - 1), {**rest, d: me.off(d, -sign * length)})
        else:
            copies.start_all(
                (key, colour, phase), n - 1, lambda i, d=d, here=here: (here, here, me.device(**{d: me.off(d, i + 1)}))
            )
            yield
            copies.arrived((key, colour, phase))
        fixed = rest
    yield
    names = ["own"]
    d, how = phases[-1]
    long, short = lengths(SIZES[d])
    names += [("l", s) for s in range(long)] + [("s", s) for s in range(short)]
    for name in names:
        copies.arrived((key, colour, "across", name))


def gather_kernel(*refs):
    sums_in, moments, given, weights = refs[:2], (refs[2:5], refs[5:8]), refs[8:10], refs[10:13]
    outs, new, rest = refs[13:19], (refs[19:22], refs[22:25]), refs[25:]
    sums, held, rows, after = by_kind(*rest[:2]), by_kind(*rest[2:4]), by_kind(*rest[4:6]), by_kind(*rest[6:8])
    tall_got, forty, load, send, recv = rest[8:13]
    me = Me()
    copies = Copies(send, recv)
    half = pl.ds(pl.multiple_of(me.core * 1280, 1280), 1280)
    mine = me.quarter()

    def which(i):
        kind, j = ORDER[i]
        return (2, j) if kind == TALL else (j // 2, j % 2)

    loads = []

    def take(src, dst):
        loads.append(pltpu.make_async_copy(src, dst, load.at[len(loads)]))
        loads[-1].start()

    for src, dst in zip(sums_in, rest[:2], strict=True):
        take(src, dst)
    for n in range(2):
        for w in (0, 1):
            take(moments[n][w].at[:, :, half], held[GATE].at[n, pl.ds(2 * w, 2), me.core])
        take(given[0].at[n], held[GATE].at[n, :, 1 - me.core])
        take(moments[n][2].at[:, :, quarter(me.at["z"], me.core)], held[TALL].at[n, mine])
        for z, core in me.others():
            q = 2 * lax.rem(z, 2) + core
            take(given[1].at[n, q], held[TALL].at[n, q])
    for i, (kind, j) in enumerate(ORDER):
        n, layer = which(i)
        z = me.at["z"] if kind != TALL else lax.div(me.at["z"], 2)
        first = ((me.at["x"] * SIZES["y"] + me.at["y"]) * dims(kind, "z")[0] + z) * ROWS[kind]
        columns = half if kind != TALL else quarter(me.at["z"], me.core)
        take(weights[n].at[layer, pl.ds(pl.multiple_of(first, 8), ROWS[kind]), columns], rows[kind].at[j])
    peers = me.arrive()
    for copy in loads:
        copy.wait()
    me.arrived(peers)

    def begin(i):
        kind, j = ORDER[i]
        w, layer = which(i)
        here = view(outs[i], kind, ("x", "y", "z"), me.at, None, me.core * HALF[kind])
        many = 2 if kind != TALL else 4
        size = ROWS[kind] // many
        old = rows[kind][j].astype(F32)
        parts = []
        for q in range(many):
            part = slice(q * size, q * size + size)
            if kind != TALL:
                m, v, g = held[kind][0, j, q], held[kind][1, j, q], sums[kind][j, q]
            else:
                m, v, g = held[TALL][0, q, :, layer], held[TALL][1, q, :, layer], sums[TALL][j, part]
            value, m, v = adamw(old[part], m, v, g)
            for n, t in enumerate((m, v)):
                after[kind][n, j, q] = t
            parts.append(value.astype(F32))
        if kind != TALL:
            here[...] = jnp.concatenate(parts, axis=0).astype(BF16)
        else:
            for q in range(4):
                forty[q * size : q * size + size, :] = parts[q]
            here[...] = forty[...].astype(BF16)
        for n in range(2):
            if kind != TALL:
                copies.start(
                    (i, "moments", n),
                    lambda n=n: (after[kind].at[n, j, 1 - me.core], new[n][w].at[layer, :, half], me.device(core=1 - me.core)),
                )
                new[n][w][layer, :, half] = jnp.where(me.core == 0, after[kind][n, j, 0], after[kind][n, j, 1])
            else:
                for o, (z, core) in enumerate(me.others()):
                    q = 2 * lax.rem(z, 2) + core
                    copies.start(
                        (i, "moments", n, o),
                        lambda n=n, q=q, z=z, core=core: (after[TALL].at[n, j, q], tall_got.at[n, j, mine], me.device(core=core, z=z)),
                    )

    def colour(i, c):
        if i in waiting:
            waiting.discard(i)
            begin(i)
        yield from gather_colour(me, copies, i, ORDER[i][0], c, outs[i])

    waiting = set(range(6))
    run({(i, c): colour(i, c) for i in range(6) for c in range(3)}, GATHER_ORDER)
    for i, (kind, j) in enumerate(ORDER):
        for n in range(2):
            if kind != TALL:
                copies.arrived((i, "moments", n))
            else:
                for o in range(3):
                    copies.arrived((i, "moments", n, o))
                for q in range(4):
                    columns = pl.ds((q % 2 * 2 + q // 2) * 256, 256)
                    new[n][2][:, j, columns] = jnp.where(q == mine, after[TALL][n, j, q], tall_got[n, j, q])
    copies.sent()


def all_gather(wide, tall, wide_moments, tall_moments, m, v, weights):
    moments = [pltpu.VMEM(t.shape, F32) for t in m]
    scratch = [
        pltpu.VMEM(wide.shape, F32),
        pltpu.VMEM(tall.shape, F32),
        pltpu.VMEM((2, 4, 2, 4, 1280), F32),
        pltpu.VMEM(tall_moments.shape, F32),
        pltpu.VMEM((4, ROWS[GATE], 1280), BF16),
        pltpu.VMEM((2, ROWS[TALL], 256), BF16),
        pltpu.VMEM((2, 4, 2, 4, 1280), F32),
        pltpu.VMEM((2, 2, 4, 10, 256), F32),
        pltpu.VMEM((2, 2, 4, 10, 256), F32),
        pltpu.VMEM((40, 256), F32),
        pltpu.SemaphoreType.DMA((24,)),
        pltpu.SemaphoreType.DMA((384,)),
        pltpu.SemaphoreType.DMA((384,)),
    ]
    matrices = [pltpu.VMEM((*dims(kind, ("x", "y", "z")), ROWS[kind], 2 * HALF[kind]), BF16) for kind, _ in ORDER]
    return pl.pallas_call(
        gather_kernel,
        out_shape=(*matrices, *moments, *moments),
        in_specs=[pl.BlockSpec(memory_space=pl.ANY)] * 13,
        out_specs=(pl.BlockSpec(memory_space=pltpu.VMEM),) * 12,
        scratch_shapes=scratch,
        compiler_params=pltpu.CompilerParams(collective_id=1, has_side_effects=True, vmem_limit_bytes=28 * 1024 * 1024),
        name="all_gather",
    )(wide, tall, *m, *v, wide_moments, tall_moments, *weights)


def spill_kernel(*refs):
    ins, moments, outs, sem = refs[:6], refs[6:12], refs[12:21], refs[21]
    copies = []
    for i, (kind, j) in enumerate(ORDER):
        which, layer = (2, j) if kind == TALL else (j // 2, j % 2)
        copies.append(pltpu.make_async_copy(ins[i], outs[which].at[layer], sem.at[i]))
    for i in range(6):
        copies.append(pltpu.make_async_copy(moments[i], outs[3 + i], sem.at[6 + i]))
    for copy in copies:
        copy.start()
    for copy in copies:
        copy.wait()


def spill(new):
    wide, tall = ((2, *dims(kind, ("x", "y", "z")), ROWS[kind], 2 * HALF[kind]) for kind in (GATE, TALL))
    return pl.pallas_call(
        spill_kernel,
        out_shape=(*(jax.ShapeDtypeStruct(shape, BF16) for shape in (wide, wide, tall)), *(jax.ShapeDtypeStruct(t.shape, F32) for t in new[6:])),
        in_specs=[pl.BlockSpec(memory_space=pltpu.VMEM)] * 12,
        out_specs=(pl.BlockSpec(memory_space=pl.ANY),) * 9,
        scratch_shapes=[pltpu.SemaphoreType.DMA((12,))],
        compiler_params=pltpu.CompilerParams(vmem_limit_bytes=1024 * 1024),
        name="spill",
    )(*new)


def adamw(w, m, v, g):
    m = 0.9 * m + 0.1 * g
    v = 0.95 * v + 0.05 * g * g
    step = m * lax.rsqrt(v + 1e-8) + 0.1 * w
    return (w - 0.02 * step).astype(BF16), m, v


def solution(mesh):
    def step(x, dy, *arrays):
        weights, m, v = (arrays[i : i + 3] for i in (0, 3, 6))
        m, v = ((*t[:2], t[2].transpose(1, 0, 2)) for t in (m, v))
        new = spill(all_gather(*summed(x[0], dy[0], *weights, m, v), m, v, weights))
        m, v = ((*t[:2], t[2].transpose(1, 0, 2)) for t in (new[3:6], new[6:9]))
        return (*(w.reshape(2, -1, w.shape[-1]) for w in new[:3]), *m, *v)

    batch, whole, rows = P(("rep", "dp")), P(), P(None, "dp")
    return jax.shard_map(
        step,
        mesh=mesh,
        in_specs=(batch, batch, *(whole,) * 3, *(rows,) * 6),
        out_specs=(*(P("rep"),) * 3, *(P("rep", "dp"),) * 6),
        check_vma=False,
    )
```

```python
import functools

import jax
import jax.numpy as jnp
from jax import lax
from jax.experimental import pallas as pl
from jax.experimental.pallas import tpu as pltpu
from jax.sharding import PartitionSpec as P

NAMES = ("w_gate", "w_up", "w_down")
MESH = pl.DeviceIdType.MESH
F32, BF16 = jnp.float32, jnp.bfloat16
SIZES = {"x": 4, "y": 4, "z": 8}
VMEM_LIMIT = 64 * 1024 * 1024 - 64 * 1024

TICKS = {
    "first": ["0h"],
    "wide1": ["1h", "020100", "1s121011", "2h0200"],
    "back": ["0112", "", "2202200010112112", "01", "2200", "", "021120", "1200212210020s"],
    "units": ["012202122010110021", "", "01022220", "12101121", "2022", "0103031221", "2210", "11131320", "", "212323"],
    "last": ["3h"],
    "wide0": ["4h", "323031", "4s424140", "5h3230"],
    "tail": ["42315052513241304042315251325041423040523151323042504041523151305032404241525150323133334252404143435152505353"],
}
GATHER_ORDER = "023120220100113012321040412152514250022212325242312002012220001211322030520042103101403011410020102131014051023011504110221200313220522120514201024022301150411231323110520142000111210250510011412240123221305242300210510222501012412232124041322152504240215152504251"


RING, DIRECT = "ring", "direct"
COLOURS = (
    (("x", RING), ("y", RING), ("z", DIRECT)),
    (("y", RING), ("x", RING), ("z", DIRECT)),
    (("z", RING), ("x", DIRECT), ("y", DIRECT)),
)
GATE, UP, TALL = KINDS = "gate", "up", "tall"
PART = {
    GATE: ((0, 512), (512, 384), (896, 384)),
    UP: ((0, 512), (512, 384), (896, 384)),
    TALL: ((0, 8), (8, 16), (24, 16)),
}
GATHER_PART = {
    GATE: ((0, 512), (512, 384), (896, 384)),
    UP: ((0, 256), (256, 384), (640, 640)),
    TALL: ((0, 16), (16, 16), (32, 8)),
}
HALF = {GATE: 1280, UP: 1280, TALL: 512}
ROWS = {GATE: 8, UP: 8, TALL: 40}
ORDER = ((TALL, 1), (GATE, 1), (UP, 3), (TALL, 0), (GATE, 0), (UP, 2))


def by_kind(wide, tall):
    return {GATE: wide, UP: wide, TALL: tall}


class Me:
    def __init__(self):
        index = lax.axis_index("dp")
        Me.zero = index * 0
        self.core = lax.rem(index, 2)
        chip = index // 2
        self.at = {
            "z": lax.rem(chip, SIZES["z"]),
            "y": lax.rem(chip // SIZES["z"], SIZES["y"]),
            "x": chip // (SIZES["z"] * SIZES["y"]),
        }
        self.sign = 1 - 2 * self.core

    def off(self, d, by):
        return lax.rem(self.at[d] + by + SIZES[d], SIZES[d])

    def device(self, core=None, **at):
        at = {**self.at, **at}
        core = self.core if core is None else core
        return (0, ((at["x"] * SIZES["y"] + at["y"]) * SIZES["z"] + at["z"]) * 2 + core)

    def arrive(self):
        sem = pltpu.get_barrier_semaphore()

        def signal(peer):
            pl.semaphore_signal(sem, inc=1, device_id=peer, device_id_type=MESH)

        for d, n in SIZES.items():
            each(n - 1, lambda i, d=d: signal(self.device(**{d: self.off(d, i + 1)})))
        signal(self.device(core=1 - self.core))
        signal(self.device(core=1 - self.core, z=self.pair()))
        return sem

    def arrived(self, sem):
        pl.semaphore_wait(sem, sum(SIZES.values()) - 1)

    def quarter(self):
        return 2 * lax.rem(self.at["z"], 2) + self.core

    def others(self):
        return (self.at["z"], 1 - self.core), (self.pair(), self.core), (self.pair(), 1 - self.core)

    def pair(self):
        return self.at["z"] + 1 - 2 * lax.rem(self.at["z"], 2)


def quarter(z, core):
    return pl.ds(pl.multiple_of(core * 512 + lax.rem(z, 2) * 256, 256), 256)


def dims(kind, free):
    return tuple(SIZES[d] // (2 if kind == TALL and d == "z" else 1) for d in free)


def view(ref, kind, free, fixed, colour=None, base=0, own=False, parts=PART):
    index = [(fixed[d] // 2 if kind == TALL and d == "z" else fixed[d]) if d in fixed else slice(None) for d in free]
    if own and not (kind == TALL and "z" in free and "z" in fixed):
        return ref.at[(*index, slice(None), slice(None))]
    if kind != TALL:
        first, size = (0, HALF[kind]) if colour is None else parts[kind][colour]
        rows, columns = slice(None), pl.ds(_at(base, first), size)
    else:
        rows = slice(None) if own or colour is None else pl.ds(*parts[TALL][colour])
        if "z" in free and "z" in fixed:
            columns = pl.ds(pl.multiple_of(base + lax.rem(fixed["z"], 2) * 256, 256), 256)
        else:
            columns = pl.ds(_at(base, 0), HALF[TALL])
    return ref.at[(*index, rows, columns)]


def _at(base, first):
    return first if isinstance(base, int) and base == 0 else pl.multiple_of(base + first, 128)


def block(kind, colour, free):
    first, size = PART[kind][colour]
    tail = (8, size) if kind != TALL else (size, HALF[TALL] if "z" in free else HALF[TALL] // 2)
    return dims(kind, free) + tail


def lengths(n):
    return n // 2, (n - 1) // 2


def reduce_buffers(kind):
    shapes = {}
    for c, phases in enumerate(COLOURS):
        free = ["x", "y", "z"]
        for p, (d, how) in enumerate(phases):
            free.remove(d)
            shape = block(kind, c, tuple(free))
            count = SIZES[d] - 1
            shapes[c, p] = (count, *shape)
    return shapes


class Copies:
    def __init__(self, send, recv):
        self.send, self.recv, self.all, self.used, self.left = send, recv, {}, 0, set()

    def start(self, key, make):
        self.start_all(key, 1, lambda i: make())

    def start_all(self, key, count, make):
        first = self.used
        self.used += count
        assert self.used <= self.send.shape[0]

        def copy(i):
            src, dst, to = make(i)
            return pltpu.make_async_remote_copy(
                src_ref=src, dst_ref=dst, send_sem=self.send.at[first + i], recv_sem=self.recv.at[first + i], device_id=to, device_id_type=MESH
            )

        self.all[key] = count, copy
        each(count, lambda i: copy(i).start())

    def arrived(self, key):
        count, copy = self.all[key]
        each(count, lambda i: copy(i).wait_recv())

    def sent(self, mine=lambda key: True):
        for key, (count, copy) in self.all.items():
            if key not in self.left and mine(key):
                self.left.add(key)
                each(count, lambda i, copy=copy: copy(i).wait_send())


def each(count, do):
    if count == 1:
        do(0)
    else:

        loop(count)(do)


def loop(count):
    def run(body):
        def step(carry, _):
            body(carry[0])
            return (carry[0] + 1, None), None

        lax.scan(step, (Me.zero, None), None, length=count)

    return run


def total(parts):
    return functools.reduce(jnp.add, [p[...].astype(F32) for p in parts])


def reduce_colour(me, copies, key, kind, colour, grads, received, last, keep=None):
    free, fixed = ("x", "y", "z"), {}
    parts = [lambda at, r=r: view(r(), kind, ("x", "y", "z"), at, colour) for r in grads]
    out = parts[0]

    def add(at, more):
        rest = [d for d in free if d not in at]
        if len(rest) >= 2:
            first = rest[0]

            @loop(SIZES[first])
            def _(i):
                now = {**at, first: i}
                out(now)[...] = total([p(now) for p in parts + more]).astype(BF16)
        else:
            out(at)[...] = total([p(at) for p in parts + more]).astype(BF16)

    for phase, (d, how) in enumerate(COLOURS[colour]):
        n, buffer = SIZES[d], functools.partial(received, colour, phase)
        left = tuple(e for e in ("x", "y", "z") if e not in fixed and e != d)

        def slot(i, buffer=buffer, left=left):
            return lambda at: view(buffer().at[i], kind, left, {e: v for e, v in at.items() if e in left}, colour, own=True)

        if how == RING:
            long, short = lengths(n)
            ways = ((1, long, 0, "l"), (-1, short, long, "s"))
            for s in range(long):
                for sign, length, base, name in ways:
                    if s >= length:
                        continue

                    def make(d=d, fixed=fixed, buffer=buffer, sign=sign, by=length - s, place=base + s):
                        at = {**fixed, d: me.off(d, me.sign * (sign * by))}
                        return out(at), buffer().at[place], me.device(**{d: me.off(d, me.sign * sign)})

                    if s:
                        copies.arrived((key, colour, phase, name, s - 1))
                    add({**fixed, d: me.off(d, me.sign * (sign * (length - s)))}, [slot(base + s - 1)] if s else [])
                    copies.start((key, colour, phase, name, s), make)
                yield
            for sign, length, base, name in ways:
                if length:
                    copies.arrived((key, colour, phase, name, length - 1))
            parts = parts + [slot(base + length - 1) for sign, length, base, name in ways if length]
        else:

            def make(i, d=d, fixed=fixed, buffer=buffer, add=add, out=out):
                to = me.off(d, i + 1)
                return out({**fixed, d: to}), buffer().at[i], me.device(**{d: to})

            each(n - 1, lambda i: add({**fixed, d: me.off(d, i + 1)}, []))
            copies.start_all((key, colour, phase), n - 1, make)
            yield
            copies.arrived((key, colour, phase))
            parts = parts + [slot(i) for i in range(n - 1)]
        fixed = {**fixed, d: me.at[d]}
        if keep is not None and phase == 0:
            copies.sent(lambda k: k[:3] == (key, colour, 0))
            stays = (lambda at, left=left: view(keep, kind, left, {e: v for e, v in at.items() if e in left}, colour, own=True))
            stays(fixed)[...] = out(fixed)[...]
            out = stays
            parts[0] = stays
    last(colour, total([p(fixed) for p in parts]).astype(BF16).astype(F32))


class Reduce:
    def __init__(self, me, own, theirs, halves, buffers, sums, send, recv, free, kept):
        self.me, self.own, self.theirs, self.halves, self.buffers = me, own, theirs, halves, buffers
        self.sums, self.free, self.kept = sums, free, kept
        self.copies = Copies(send, recv)
        self.waiting = set(range(6))
        self.streams = {(i, c): self.colour(i, c) for i in range(6) for c in range(3)} | {(i, 3): self.finish(i) for i in range(6)}

    def slot(self, i):
        kind, j = ORDER[i]
        return 0 if kind == TALL else j // 2

    def half(self, i):
        kind = ORDER[i][0]
        if i >= 3:
            pl.semaphore_wait(self.free.at[i - 3], sum(SIZES.values()) - len(SIZES) + 1)
        self.copies.start(
            (i, "half"), lambda: (self.halves[kind](), self.theirs[kind].at[self.slot(i)], self.me.device(core=1 - self.me.core))
        )

    def half_sent(self, i):
        self.copies.sent(lambda key: key == (i, "half"))

    def colour(self, i, c):
        kind, j = ORDER[i]
        slot = self.slot(i)
        if i in self.waiting:
            self.waiting.discard(i)
            self.copies.arrived((i, "half"))

        def last(colour, value):
            first, size = PART[kind][colour]
            if kind != TALL:
                self.sums[kind][j, 0, :, first : first + size] = value[:4]
                self.sums[kind][j, 1, :, first : first + size] = value[4:]
            else:
                self.sums[TALL][j, first : first + size, :] = value

        grads = (lambda: self.own[kind].at[slot]), (lambda: self.theirs[kind].at[slot])
        keep = self.kept[c] if i == 0 else None
        yield from reduce_colour(self.me, self.copies, i, kind, c, grads, lambda c, p: self.buffers[kind, (c, p)].at[0], last, keep)

    def finish(self, i):
        if i < 3:
            for d, n in SIZES.items():
                each(n - 1, lambda o, d=d: self.done(i, self.me.device(**{d: self.me.off(d, o + 1)})))
            self.done(i, self.me.device(core=1 - self.me.core))
        self.copies.sent(lambda key: key[0] == i)
        yield

    def done(self, i, device):
        pl.semaphore_signal(self.free.at[i], inc=1, device_id=device, device_id_type=MESH)

    def run(self, order):
        for i, c in zip(order[::2], order[1::2], strict=True):
            if c == "h":
                self.half(int(i))
            elif c == "s":
                self.half_sent(int(i))
            else:
                next(self.streams[int(i), int(c)], None)


def dot(a, b, ca=1, cb=0):
    return lax.dot_general(a, b, (((ca,), (cb,)), ((), ())), preferred_element_type=F32)


def rem(a, b):
    return a % b if isinstance(a, int) else lax.rem(a, b)


def at_tile(i, size):
    return pl.ds(pl.multiple_of(i * size, size), size)


def put_rows(ref, i, value):
    y, z, rows = ref.shape[1:4]
    for s in range(0, 256, 8):
        row = i * 256 + s
        group = lax.div(row, rows)
        ref[lax.div(group, y * z), rem(lax.div(group, z), y), rem(group, z), pl.ds(pl.multiple_of(rem(row, rows), 8), 8), :] = value[s : s + 8]


def put_all(ref, value):
    ref[...] = value.reshape(ref.shape)


def step_kernel(*refs):
    x_in, dy_in, w_gate, w_up, w_down = refs[:5]
    moments, outs, (wide_moments, tall_moments), rest = (refs[5:8], refs[8:11]), refs[11:13], refs[13:15], list(refs[15:])
    gate_kept, up_kept, hidden_kept, a0_kept, h1_kept = rest[:5]
    rest = rest[5:]
    take = lambda n: [rest.pop(0) for _ in range(n)]
    act, dy, turned, back, both, gates, ups = take(7)
    tile_g, tile_u, tile_d, rows_w, columns_w = take(5)
    wide_own, wide_theirs, tall_own, tall_half, tall_theirs = take(5)
    load, sem_g, sem_u, sem_d, sem_w, sem_c, sem_f, send, recv, free = take(10)
    buffers = {}
    for kind in KINDS:
        for k in reduce_buffers(kind):
            buffers[kind, k] = rest.pop(0)
    tall_kept = take(3)
    me = Me()

    def fetch(src, dst, sem):
        copy = pltpu.make_async_copy(src, dst, sem)
        copy.start()
        return copy

    class Stream:
        def __init__(self, tile, buffer, sem):
            self.tile, self.buffer, self.sem = tile, buffer, sem

        def copy(self, i):
            slot = rem(i, 2)
            return pltpu.make_async_copy(self.tile(i), self.buffer.at[slot], self.sem.at[slot])

    def stream(*streams, n):
        for s in streams:
            s.copy(0).start()

        def ahead(i):
            @pl.when(i + 1 < n)
            def _():
                for s in streams:
                    s.copy(i + 1).start()

            for s in streams:
                s.copy(i).wait()

        return ahead

    def columns(w, layer, buffer, sem):
        return Stream(lambda i: w.at[layer, :, at_tile(i, 256)], buffer, sem)

    loads = [fetch(x_in, back, load.at[0]), fetch(dy_in, dy, load.at[1])]
    zeroth = stream(columns(w_gate, 0, tile_g, sem_g), columns(w_up, 0, tile_u, sem_u), n=10)

    def half_columns(i, half):
        src = w_down.at[0, pl.ds(half * 1280, 1280), at_tile(i, 256)]
        return pltpu.make_async_copy(src, columns_w.at[half], sem_c.at[half])

    for half in (0, 1):
        half_columns(0, half).start()
    peers = me.arrive()
    own = by_kind(wide_own, tall_own)
    theirs = by_kind(wide_theirs, tall_theirs)
    halves = by_kind(lambda: wide_own.at[2], lambda: tall_half)
    reduce = Reduce(me, own, theirs, halves, buffers, by_kind(*outs), send, recv, free, tall_kept)

    def ticks(phase, i):
        orders = TICKS[phase]
        if any(orders):
            lax.switch(i, [functools.partial(reduce.run, order) for order in orders])

    def norm():
        @pl.loop(0, 8)
        def _(i):
            rows = at_tile(i, 128)
            h = back[rows, :].astype(F32)
            act[rows, :] = (h * lax.rsqrt(jnp.mean(h * h, -1, keepdims=True) + 1e-6)).astype(BF16)

    def turn(src, i):
        i = rem(i, 8)
        turned[:, at_tile(i, 128)] = src[at_tile(i, 128), :].T

    def silu_of(g):
        s = jax.nn.sigmoid(g)
        return g * s, s * (1 + g * (1 - s))

    def unit(i, silu, slope, hidden, d, dout):
        d = d.astype(BF16).astype(F32)
        both[1, :, at_tile(i, 256)] = (d * silu).astype(BF16)
        both[0, :, at_tile(i, 256)] = (d * slope).astype(BF16)
        for ref, core in ((tall_own.at[0], me.core), (tall_half, 1 - me.core)):
            put_rows(ref, i, dot(hidden, dout[:, at_tile(core, 512)]).astype(BF16))

    def wide_grads(phase):
        @pl.loop(0, 4)
        def _(k):
            which = lax.div(k, 2)
            mine = lax.rem(k + which, 2)
            core = mine * me.core + (1 - mine) * (1 - me.core)
            value = dot(turned[...], both[which, :, at_tile(core, 1280)]).astype(BF16)
            put_all(wide_own.at[lax.rem(2 - mine * (2 - which), 3)], value)
            ticks(phase, k)

    def kept(i, out):
        slot = rem(i, 2)
        pairs = (gates.at[slot], gate_kept.at[i]), (ups.at[slot], up_kept.at[i])
        return [pltpu.make_async_copy(*(p if out else p[::-1]), sem_f.at[n, slot]) for n, p in enumerate(pairs)]

    loads[0].wait()
    norm()
    keep = fetch(act, a0_kept, load.at[0])

    @pl.loop(0, 10)
    def _(i):
        zeroth(i)

        @pl.when(i >= 2)
        def _():
            for copy in kept(i - 2, True):
                copy.wait()

        slot = rem(i, 2)
        g, u = dot(act[...], tile_g[slot]), dot(act[...], tile_u[slot])
        silu, slope = silu_of(g)
        gates[slot] = silu
        ups[slot] = u * slope
        both[0, :, at_tile(i, 256)] = (silu * u).astype(BF16)
        for copy in kept(i, True):
            copy.start()

    keep_hidden = fetch(both.at[0], hidden_kept, load.at[2])
    first = stream(
        columns(w_gate, 1, tile_g, sem_g),
        columns(w_up, 1, tile_u, sem_u),
        Stream(lambda i: w_down.at[1, at_tile(i, 256), :], tile_d, sem_d),
        n=10,
    )

    @pl.loop(0, 4)
    def _(i):
        part = 0.0
        for half in (0, 1):
            half_columns(i, half).wait()
            part += dot(both[0, :, half * 1280 : half * 1280 + 1280], columns_w[half])

            @pl.when(i < 3)
            def _():
                half_columns(i + 1, half).start()

        part = part.astype(BF16).astype(F32)
        back[:, at_tile(i, 256)] = (back[:, at_tile(i, 256)].astype(F32) + part).astype(BF16)

    keep.wait()
    keep = fetch(back, h1_kept, load.at[0])
    norm()

    loads[1].wait()
    keep_hidden.wait()

    @pl.loop(0, 10)
    def _(i):
        first(i)
        turn(act, i)
        slot = rem(i, 2)
        silu, slope = silu_of(dot(act[...], tile_g[slot]))
        u = dot(act[...], tile_u[slot])
        unit(i, silu, u * slope, (silu * u).astype(BF16).T, dot(dy[...], tile_d[slot], 1, 1), dy)

    me.arrived(peers)
    for n, three in enumerate(moments):
        for which in (0, 1):

            def make(n=n, which=which, three=three):
                theirs = pl.ds(pl.multiple_of((1 - me.core) * 1280, 1280), 1280)
                return three[which].at[:, :, theirs], wide_moments.at[n, pl.ds(2 * which, 2)], me.device(core=1 - me.core)

            reduce.copies.start(("moments", n, which), make)
        for o in range(3):

            def make(n=n, o=o, three=three):
                z, core = me.others()[o]
                return three[2].at[:, :, quarter(z, core)], tall_moments.at[n, me.quarter()], me.device(core=core, z=z)

            reduce.copies.start(("moments", n, 2 + o), make)
    reduce.run(TICKS["first"][0])
    wide_grads("wide1")

    keep.wait()
    for i in (8, 9):
        for copy in kept(i, True):
            copy.wait()
    load_h = fetch(h1_kept, turned, load.at[0])

    def weight_rows(k, w):
        slot = rem(k, 2)
        rows = at_tile(k // 2 if isinstance(k, int) else lax.div(k, 2), 256)
        return pltpu.make_async_copy(w.at[1, rows, :], rows_w.at[slot], sem_w.at[slot])

    weight_rows(0, w_gate).start()

    @pl.loop(0, 8)
    def _(k):
        n, which = lax.div(k, 2), lax.rem(k, 2)

        @pl.when(which == 0)
        def _():
            weight_rows(k + 1, w_up).start()

        @pl.when((which == 1) & (k < 7))
        def _():
            weight_rows(k + 1, w_gate).start()

        weight_rows(k, w_gate).wait()
        part = dot(both[which], rows_w[which], 1, 1).astype(BF16).astype(F32)
        before = back[:, at_tile(n, 256)].astype(F32)
        back[:, at_tile(n, 256)] = (jnp.where(which == 0, 0.0, before) + part).astype(BF16)
        ticks("back", k)

    load_h.wait()

    @pl.loop(0, 8)
    def _(i):
        rows = at_tile(i, 128)
        h, d = turned[rows, :].astype(F32), back[rows, :].astype(F32)
        scale = lax.rsqrt(jnp.mean(h * h, -1, keepdims=True) + 1e-6)
        along = jnp.sum(d * h, -1, keepdims=True)
        d = (d * scale - h * (scale * scale * scale * along * (1 / 1024))).astype(BF16)
        act[rows, :] = (dy[rows, :].astype(F32) + d.astype(F32)).astype(BF16)

    load_a = fetch(a0_kept, back, load.at[1])
    second = stream(
        Stream(lambda i: w_down.at[0, at_tile(i, 256), :], tile_d, sem_d),
        Stream(lambda i: hidden_kept.at[:, at_tile(i, 256)], tile_g, sem_g),
        n=10,
    )
    for copy in kept(0, False):
        copy.start()
    load_a.wait()

    @pl.loop(0, 10)
    def _(i):
        @pl.when(i < 9)
        def _():
            for copy in kept(i + 1, False):
                copy.start()

        second(i)
        turn(back, i)
        for copy in kept(i, False):
            copy.wait()
        slot = rem(i, 2)
        unit(i, gates[slot], ups[slot], tile_g[slot].T, dot(act[...], tile_d[slot], 1, 1), act)
        ticks("units", i)

    reduce.run(TICKS["last"][0])
    wide_grads("wide0")
    reduce.run(TICKS["tail"][0])
    for stream_ in reduce.streams.values():
        assert next(stream_, 0) == 0, "not done"
    for n in range(2):
        for o in range(5):
            reduce.copies.arrived(("moments", n, o))
    reduce.copies.sent()


def run(streams, order):
    for i, c in zip(order[::2], order[1::2], strict=True):
        next(streams[int(i), int(c)], None)
    for stream in streams.values():
        assert next(stream, 0) == 0, "not done"


def full_shape(kind):
    return dims(kind, ("x", "y", "z")) + (ROWS[kind], HALF[kind])


def summed(x, dy, w_gate, w_up, w_down, m, v):
    square = pltpu.VMEM((1024, 1024), BF16)
    scratch = [square] * 4 + [pltpu.VMEM((2, 1024, 2560), BF16)]
    scratch += [pltpu.VMEM((2, 1024, 256), F32)] * 2
    scratch += [pltpu.VMEM((2, 1024, 256), BF16)] * 2 + [pltpu.VMEM((2, 256, 1024), BF16), pltpu.VMEM((2, 256, 2560), BF16)]
    scratch += [
        pltpu.VMEM((2, 1280, 256), BF16),
        pltpu.VMEM((3, *full_shape(GATE)), BF16),
        pltpu.VMEM((2, *full_shape(GATE)), BF16),
        pltpu.VMEM((1, *full_shape(TALL)), BF16),
        pltpu.VMEM(full_shape(TALL), BF16),
        pltpu.VMEM((1, *full_shape(TALL)), BF16),
        pltpu.SemaphoreType.DMA((3,)),
        *[pltpu.SemaphoreType.DMA((2,))] * 5,
        pltpu.SemaphoreType.DMA((2, 2)),
        pltpu.SemaphoreType.DMA((256,)),
        pltpu.SemaphoreType.DMA((256,)),
        pltpu.SemaphoreType.REGULAR((3,)),
    ]
    for kind in KINDS:
        scratch += [pltpu.VMEM((1, *shape), BF16) for shape in reduce_buffers(kind).values()]
    scratch += [pltpu.VMEM(block(TALL, c, [d for d in "xyz" if d != COLOURS[c][0][0]]), BF16) for c in range(3)]
    kept = [jax.ShapeDtypeStruct((10, 1024, 256), F32)] * 2 + [jax.ShapeDtypeStruct((1024, t), BF16) for t in (2560, 1024, 1024)]
    return pl.pallas_call(
        step_kernel,
        out_shape=(
            jax.ShapeDtypeStruct((4, 2, 4, 1280), F32),
            jax.ShapeDtypeStruct((2, 40, 256), F32),
            jax.ShapeDtypeStruct((2, 4, 4, 1280), F32),
            jax.ShapeDtypeStruct((2, 4, 10, 2, 256), F32),
            *kept,
        ),
        in_specs=[pl.BlockSpec(memory_space=pl.ANY)] * 11,
        out_specs=(*[pl.BlockSpec(memory_space=pltpu.VMEM)] * 2, *[pl.BlockSpec(memory_space=pl.ANY)] * 7),
        scratch_shapes=scratch,
        compiler_params=pltpu.CompilerParams(
            collective_id=0, has_side_effects=True, vmem_limit_bytes=VMEM_LIMIT
        ),
        name="step",
    )(x, dy, w_gate, w_up, w_down, *m, *v)[:4]


def gather_colour(me, copies, key, kind, colour, ref):
    base = me.core * HALF[kind]
    fixed = dict(me.at)

    def part(at):
        return view(ref, kind, ("x", "y", "z"), at, colour, base, parts=GATHER_PART)

    phases = COLOURS[colour][::-1]
    for phase, (d, how) in enumerate(phases):
        n, lastly = SIZES[d], phase == len(phases) - 1
        rest = {e: v for e, v in fixed.items() if e != d}
        here = part(fixed)

        def across(name, at):
            if lastly:
                copies.start((key, colour, "across", name), lambda: (part(at), part(at), me.device(core=1 - me.core)))

        if how == RING:
            long, short = lengths(n)
            ways = ((me.sign, long, "l"), (-me.sign, short, "s"))
            for s in range(long):
                for sign, length, name in ways:
                    if s >= length:
                        continue
                    at = {**rest, d: me.off(d, -sign * s)}
                    if s:
                        copies.arrived((key, colour, phase, name, s - 1))
                    copies.start(
                        (key, colour, phase, name, s),
                        lambda at=at, d=d, sign=sign: (part(at), part(at), me.device(**{d: me.off(d, sign)})),
                    )
                    if s:
                        across((name, s - 1), at)
                if s == 0:
                    across("own", fixed)
                yield
            for sign, length, name in ways:
                if length:
                    copies.arrived((key, colour, phase, name, length - 1))
                    across((name, length - 1), {**rest, d: me.off(d, -sign * length)})
        else:
            copies.start_all(
                (key, colour, phase), n - 1, lambda i, d=d, here=here: (here, here, me.device(**{d: me.off(d, i + 1)}))
            )
            yield
            copies.arrived((key, colour, phase))
        fixed = rest
    yield
    names = ["own"]
    d, how = phases[-1]
    long, short = lengths(SIZES[d])
    names += [("l", s) for s in range(long)] + [("s", s) for s in range(short)]
    for name in names:
        copies.arrived((key, colour, "across", name))


def gather_kernel(*refs):
    sums_in, moments, given, weights = refs[:2], (refs[2:5], refs[5:8]), refs[8:10], refs[10:13]
    outs, new, rest = refs[13:19], (refs[19:22], refs[22:25]), refs[25:]
    sums, held, rows, after = by_kind(*rest[:2]), by_kind(*rest[2:4]), by_kind(*rest[4:6]), by_kind(*rest[6:8])
    tall_got, forty, load, send, recv = rest[8:13]
    me = Me()
    copies = Copies(send, recv)
    half = pl.ds(pl.multiple_of(me.core * 1280, 1280), 1280)
    mine = me.quarter()

    def which(i):
        kind, j = ORDER[i]
        return (2, j) if kind == TALL else (j // 2, j % 2)

    loads = []

    def take(src, dst):
        loads.append(pltpu.make_async_copy(src, dst, load.at[len(loads)]))
        loads[-1].start()

    for src, dst in zip(sums_in, rest[:2], strict=True):
        take(src, dst)
    for n in range(2):
        for w in (0, 1):
            take(moments[n][w].at[:, :, half], held[GATE].at[n, pl.ds(2 * w, 2), me.core])
        take(given[0].at[n], held[GATE].at[n, :, 1 - me.core])
        take(moments[n][2].at[:, :, quarter(me.at["z"], me.core)], held[TALL].at[n, mine])
        for z, core in me.others():
            q = 2 * lax.rem(z, 2) + core
            take(given[1].at[n, q], held[TALL].at[n, q])
    for i, (kind, j) in enumerate(ORDER):
        n, layer = which(i)
        z = me.at["z"] if kind != TALL else lax.div(me.at["z"], 2)
        first = ((me.at["x"] * SIZES["y"] + me.at["y"]) * dims(kind, "z")[0] + z) * ROWS[kind]
        columns = half if kind != TALL else quarter(me.at["z"], me.core)
        take(weights[n].at[layer, pl.ds(pl.multiple_of(first, 8), ROWS[kind]), columns], rows[kind].at[j])
    peers = me.arrive()
    for copy in loads:
        copy.wait()
    me.arrived(peers)

    def begin(i):
        kind, j = ORDER[i]
        w, layer = which(i)
        here = view(outs[i], kind, ("x", "y", "z"), me.at, None, me.core * HALF[kind])
        many = 2 if kind != TALL else 4
        size = ROWS[kind] // many
        old = rows[kind][j].astype(F32)
        parts = []
        for q in range(many):
            part = slice(q * size, q * size + size)
            if kind != TALL:
                m, v, g = held[kind][0, j, q], held[kind][1, j, q], sums[kind][j, q]
            else:
                m, v, g = held[TALL][0, q, :, layer], held[TALL][1, q, :, layer], sums[TALL][j, part]
            value, m, v = adamw(old[part], m, v, g)
            for n, t in enumerate((m, v)):
                after[kind][n, j, q] = t
            parts.append(value.astype(F32))
        if kind != TALL:
            here[...] = jnp.concatenate(parts, axis=0).astype(BF16)
        else:
            for q in range(4):
                forty[q * size : q * size + size, :] = parts[q]
            here[...] = forty[...].astype(BF16)
        for n in range(2):
            if kind != TALL:
                copies.start(
                    (i, "moments", n),
                    lambda n=n: (after[kind].at[n, j, 1 - me.core], new[n][w].at[layer, :, half], me.device(core=1 - me.core)),
                )
                new[n][w][layer, :, half] = jnp.where(me.core == 0, after[kind][n, j, 0], after[kind][n, j, 1])
            else:
                for o, (z, core) in enumerate(me.others()):
                    q = 2 * lax.rem(z, 2) + core
                    copies.start(
                        (i, "moments", n, o),
                        lambda n=n, q=q, z=z, core=core: (after[TALL].at[n, j, q], tall_got.at[n, j, mine], me.device(core=core, z=z)),
                    )

    def colour(i, c):
        if i in waiting:
            waiting.discard(i)
            begin(i)
        yield from gather_colour(me, copies, i, ORDER[i][0], c, outs[i])

    waiting = set(range(6))
    run({(i, c): colour(i, c) for i in range(6) for c in range(3)}, GATHER_ORDER)
    for i, (kind, j) in enumerate(ORDER):
        for n in range(2):
            if kind != TALL:
                copies.arrived((i, "moments", n))
            else:
                for o in range(3):
                    copies.arrived((i, "moments", n, o))
                for q in range(4):
                    columns = pl.ds((q % 2 * 2 + q // 2) * 256, 256)
                    new[n][2][:, j, columns] = jnp.where(q == mine, after[TALL][n, j, q], tall_got[n, j, q])
    copies.sent()


def all_gather(wide, tall, wide_moments, tall_moments, m, v, weights):
    moments = [pltpu.VMEM(t.shape, F32) for t in m]
    scratch = [
        pltpu.VMEM(wide.shape, F32),
        pltpu.VMEM(tall.shape, F32),
        pltpu.VMEM((2, 4, 2, 4, 1280), F32),
        pltpu.VMEM(tall_moments.shape, F32),
        pltpu.VMEM((4, ROWS[GATE], 1280), BF16),
        pltpu.VMEM((2, ROWS[TALL], 256), BF16),
        pltpu.VMEM((2, 4, 2, 4, 1280), F32),
        pltpu.VMEM((2, 2, 4, 10, 256), F32),
        pltpu.VMEM((2, 2, 4, 10, 256), F32),
        pltpu.VMEM((40, 256), F32),
        pltpu.SemaphoreType.DMA((24,)),
        pltpu.SemaphoreType.DMA((384,)),
        pltpu.SemaphoreType.DMA((384,)),
    ]
    matrices = [pltpu.VMEM((*dims(kind, ("x", "y", "z")), ROWS[kind], 2 * HALF[kind]), BF16) for kind, _ in ORDER]
    return pl.pallas_call(
        gather_kernel,
        out_shape=(*matrices, *moments, *moments),
        in_specs=[pl.BlockSpec(memory_space=pl.ANY)] * 13,
        out_specs=(pl.BlockSpec(memory_space=pltpu.VMEM),) * 12,
        scratch_shapes=scratch,
        compiler_params=pltpu.CompilerParams(collective_id=1, has_side_effects=True, vmem_limit_bytes=28 * 1024 * 1024),
        name="all_gather",
    )(wide, tall, *m, *v, wide_moments, tall_moments, *weights)


def spill_kernel(*refs):
    ins, moments, outs, sem = refs[:6], refs[6:12], refs[12:21], refs[21]
    copies = []
    for i, (kind, j) in enumerate(ORDER):
        which, layer = (2, j) if kind == TALL else (j // 2, j % 2)
        copies.append(pltpu.make_async_copy(ins[i], outs[which].at[layer], sem.at[i]))
    for i in range(6):
        copies.append(pltpu.make_async_copy(moments[i], outs[3 + i], sem.at[6 + i]))
    for copy in copies:
        copy.start()
    for copy in copies:
        copy.wait()


def spill(new):
    wide, tall = ((2, *dims(kind, ("x", "y", "z")), ROWS[kind], 2 * HALF[kind]) for kind in (GATE, TALL))
    return pl.pallas_call(
        spill_kernel,
        out_shape=(*(jax.ShapeDtypeStruct(shape, BF16) for shape in (wide, wide, tall)), *(jax.ShapeDtypeStruct(t.shape, F32) for t in new[6:])),
        in_specs=[pl.BlockSpec(memory_space=pltpu.VMEM)] * 12,
        out_specs=(pl.BlockSpec(memory_space=pl.ANY),) * 9,
        scratch_shapes=[pltpu.SemaphoreType.DMA((12,))],
        compiler_params=pltpu.CompilerParams(vmem_limit_bytes=1024 * 1024),
        name="spill",
    )(*new)


def adamw(w, m, v, g):
    m = 0.9 * m + 0.1 * g
    v = 0.95 * v + 0.05 * g * g
    step = m * lax.rsqrt(v + 1e-8) + 0.1 * w
    return (w - 0.02 * step).astype(BF16), m, v


def solution(mesh):
    def step(x, dy, *arrays):
        weights, m, v = (arrays[i : i + 3] for i in (0, 3, 6))
        m, v = ((*t[:2], t[2].transpose(1, 0, 2)) for t in (m, v))
        new = spill(all_gather(*summed(x[0], dy[0], *weights, m, v), m, v, weights))
        m, v = ((*t[:2], t[2].transpose(1, 0, 2)) for t in (new[3:6], new[6:9]))
        return (*(w.reshape(2, -1, w.shape[-1]) for w in new[:3]), *m, *v)

    batch, whole, rows = P(("rep", "dp")), P(), P(None, "dp")
    return jax.shard_map(
        step,
        mesh=mesh,
        in_specs=(batch, batch, *(whole,) * 3, *(rows,) * 6),
        out_specs=(*(P("rep"),) * 3, *(P("rep", "dp"),) * 6),
        check_vma=False,
    )
```

```python
import functools

import jax
import jax.numpy as jnp
from jax import lax
from jax.experimental import pallas as pl
from jax.experimental.pallas import tpu as pltpu
from jax.sharding import PartitionSpec as P

NAMES = ("w_gate", "w_up", "w_down")
MESH = pl.DeviceIdType.MESH
F32, BF16 = jnp.float32, jnp.bfloat16
SIZES = {"x": 4, "y": 4, "z": 8}
VMEM_LIMIT = 64 * 1024 * 1024 - 64 * 1024

TICKS = {
    "first": ["0h"],
    "wide1": ["1h", "020100", "1s121011", "2h0200"],
    "back": ["0112", "", "2202200010112112", "01", "2200", "", "021120", "1200212210020s"],
    "units": ["012202122010110021", "", "01022220", "12101121", "2022", "0103031221", "2210", "11131320", "", "212323"],
    "last": ["3h"],
    "wide0": ["4h", "323031", "4s424140", "5h3230"],
    "tail": ["42315052513241304042315251325041423040523151323042504041523151305032404241525150323133334252404143435152505353"],
}
GATHER_ORDER = "023120220100113012321040412152514250022212325242312002012220001211322030520042103101403011410020102131014051023011504110221200313220522120514201024022301150411231323110520142000111210250510011412240123221305242300210510222501012412232124041322152504240215152504251"


RING, DIRECT = "ring", "direct"
COLOURS = (
    (("x", RING), ("y", RING), ("z", DIRECT)),
    (("y", RING), ("x", RING), ("z", DIRECT)),
    (("z", RING), ("x", DIRECT), ("y", DIRECT)),
)
GATE, UP, TALL = KINDS = "gate", "up", "tall"
PART = {
    GATE: ((0, 512), (512, 384), (896, 384)),
    UP: ((0, 512), (512, 384), (896, 384)),
    TALL: ((0, 8), (8, 16), (24, 16)),
}
GATHER_PART = {
    GATE: ((0, 512), (512, 384), (896, 384)),
    UP: ((0, 256), (256, 384), (640, 640)),
    TALL: ((0, 16), (16, 16), (32, 8)),
}
HALF = {GATE: 1280, UP: 1280, TALL: 512}
ROWS = {GATE: 8, UP: 8, TALL: 40}
ORDER = ((TALL, 1), (GATE, 1), (UP, 3), (TALL, 0), (GATE, 0), (UP, 2))


def by_kind(wide, tall):
    return {GATE: wide, UP: wide, TALL: tall}


class Me:
    def __init__(self):
        index = lax.axis_index("dp")
        Me.zero = index * 0
        self.core = lax.rem(index, 2)
        chip = index // 2
        self.at = {
            "z": lax.rem(chip, SIZES["z"]),
            "y": lax.rem(chip // SIZES["z"], SIZES["y"]),
            "x": chip // (SIZES["z"] * SIZES["y"]),
        }
        self.sign = 1 - 2 * self.core

    def off(self, d, by):
        return lax.rem(self.at[d] + by + SIZES[d], SIZES[d])

    def device(self, core=None, **at):
        at = {**self.at, **at}
        core = self.core if core is None else core
        return (0, ((at["x"] * SIZES["y"] + at["y"]) * SIZES["z"] + at["z"]) * 2 + core)

    def arrive(self):
        sem = pltpu.get_barrier_semaphore()

        def signal(peer):
            pl.semaphore_signal(sem, inc=1, device_id=peer, device_id_type=MESH)

        for d, n in SIZES.items():
            each(n - 1, lambda i, d=d: signal(self.device(**{d: self.off(d, i + 1)})))
        signal(self.device(core=1 - self.core))
        signal(self.device(core=1 - self.core, z=self.pair()))
        return sem

    def arrived(self, sem):
        pl.semaphore_wait(sem, sum(SIZES.values()) - 1)

    def quarter(self):
        return 2 * lax.rem(self.at["z"], 2) + self.core

    def others(self):
        return (self.at["z"], 1 - self.core), (self.pair(), self.core), (self.pair(), 1 - self.core)

    def pair(self):
        return self.at["z"] + 1 - 2 * lax.rem(self.at["z"], 2)


def quarter(z, core):
    return pl.ds(pl.multiple_of(core * 512 + lax.rem(z, 2) * 256, 256), 256)


def dims(kind, free):
    return tuple(SIZES[d] // (2 if kind == TALL and d == "z" else 1) for d in free)


def view(ref, kind, free, fixed, colour=None, base=0, own=False, parts=PART):
    index = [(fixed[d] // 2 if kind == TALL and d == "z" else fixed[d]) if d in fixed else slice(None) for d in free]
    if own and not (kind == TALL and "z" in free and "z" in fixed):
        return ref.at[(*index, slice(None), slice(None))]
    if kind != TALL:
        first, size = (0, HALF[kind]) if colour is None else parts[kind][colour]
        rows, columns = slice(None), pl.ds(_at(base, first), size)
    else:
        rows = slice(None) if own or colour is None else pl.ds(*parts[TALL][colour])
        if "z" in free and "z" in fixed:
            columns = pl.ds(pl.multiple_of(base + lax.rem(fixed["z"], 2) * 256, 256), 256)
        else:
            columns = pl.ds(_at(base, 0), HALF[TALL])
    return ref.at[(*index, rows, columns)]


def _at(base, first):
    return first if isinstance(base, int) and base == 0 else pl.multiple_of(base + first, 128)


def block(kind, colour, free):
    first, size = PART[kind][colour]
    tail = (8, size) if kind != TALL else (size, HALF[TALL] if "z" in free else HALF[TALL] // 2)
    return dims(kind, free) + tail


def lengths(n):
    return n // 2, (n - 1) // 2


def reduce_buffers(kind):
    shapes = {}
    for c, phases in enumerate(COLOURS):
        free = ["x", "y", "z"]
        for p, (d, how) in enumerate(phases):
            free.remove(d)
            shape = block(kind, c, tuple(free))
            count = SIZES[d] - 1
            shapes[c, p] = (count, *shape)
    return shapes


class Copies:
    def __init__(self, send, recv):
        self.send, self.recv, self.all, self.used, self.left = send, recv, {}, 0, set()

    def start(self, key, make):
        self.start_all(key, 1, lambda i: make())

    def start_all(self, key, count, make):
        first = self.used
        self.used += count
        assert self.used <= self.send.shape[0]

        def copy(i):
            src, dst, to = make(i)
            return pltpu.make_async_remote_copy(
                src_ref=src, dst_ref=dst, send_sem=self.send.at[first + i], recv_sem=self.recv.at[first + i], device_id=to, device_id_type=MESH
            )

        self.all[key] = count, copy
        each(count, lambda i: copy(i).start())

    def arrived(self, key):
        count, copy = self.all[key]
        each(count, lambda i: copy(i).wait_recv())

    def sent(self, mine=lambda key: True):
        for key, (count, copy) in self.all.items():
            if key not in self.left and mine(key):
                self.left.add(key)
                each(count, lambda i, copy=copy: copy(i).wait_send())


def each(count, do):
    if count == 1:
        do(0)
    else:

        loop(count)(do)


def loop(count):
    def run(body):
        def step(carry, _):
            body(carry[0])
            return (carry[0] + 1, None), None

        lax.scan(step, (Me.zero, None), None, length=count)

    return run


def total(parts):
    return functools.reduce(jnp.add, [p[...].astype(F32) for p in parts])


def reduce_colour(me, copies, key, kind, colour, grads, received, last, keep=None):
    free, fixed = ("x", "y", "z"), {}
    parts = [lambda at, r=r: view(r(), kind, ("x", "y", "z"), at, colour) for r in grads]
    out = parts[0]

    def add(at, more):
        rest = [d for d in free if d not in at]
        if len(rest) >= 2:
            first = rest[0]

            @loop(SIZES[first])
            def _(i):
                now = {**at, first: i}
                out(now)[...] = total([p(now) for p in parts + more]).astype(BF16)
        else:
            out(at)[...] = total([p(at) for p in parts + more]).astype(BF16)

    for phase, (d, how) in enumerate(COLOURS[colour]):
        n, buffer = SIZES[d], functools.partial(received, colour, phase)
        left = tuple(e for e in ("x", "y", "z") if e not in fixed and e != d)

        def slot(i, buffer=buffer, left=left):
            return lambda at: view(buffer().at[i], kind, left, {e: v for e, v in at.items() if e in left}, colour, own=True)

        if how == RING:
            long, short = lengths(n)
            ways = ((1, long, 0, "l"), (-1, short, long, "s"))
            for s in range(long):
                for sign, length, base, name in ways:
                    if s >= length:
                        continue

                    def make(d=d, fixed=fixed, buffer=buffer, sign=sign, by=length - s, place=base + s):
                        at = {**fixed, d: me.off(d, me.sign * (sign * by))}
                        return out(at), buffer().at[place], me.device(**{d: me.off(d, me.sign * sign)})

                    if s:
                        copies.arrived((key, colour, phase, name, s - 1))
                    add({**fixed, d: me.off(d, me.sign * (sign * (length - s)))}, [slot(base + s - 1)] if s else [])
                    copies.start((key, colour, phase, name, s), make)
                yield
            for sign, length, base, name in ways:
                if length:
                    copies.arrived((key, colour, phase, name, length - 1))
            parts = parts + [slot(base + length - 1) for sign, length, base, name in ways if length]
        else:

            def make(i, d=d, fixed=fixed, buffer=buffer, add=add, out=out):
                to = me.off(d, i + 1)
                return out({**fixed, d: to}), buffer().at[i], me.device(**{d: to})

            each(n - 1, lambda i: add({**fixed, d: me.off(d, i + 1)}, []))
            copies.start_all((key, colour, phase), n - 1, make)
            yield
            copies.arrived((key, colour, phase))
            parts = parts + [slot(i) for i in range(n - 1)]
        fixed = {**fixed, d: me.at[d]}
        if keep is not None and phase == 0:
            copies.sent(lambda k: k[:3] == (key, colour, 0))
            stays = (lambda at, left=left: view(keep, kind, left, {e: v for e, v in at.items() if e in left}, colour, own=True))
            stays(fixed)[...] = out(fixed)[...]
            out = stays
            parts[0] = stays
    last(colour, total([p(fixed) for p in parts]).astype(BF16).astype(F32))


class Reduce:
    def __init__(self, me, own, theirs, halves, buffers, sums, send, recv, free, kept):
        self.me, self.own, self.theirs, self.halves, self.buffers = me, own, theirs, halves, buffers
        self.sums, self.free, self.kept = sums, free, kept
        self.copies = Copies(send, recv)
        self.waiting = set(range(6))
        self.streams = {(i, c): self.colour(i, c) for i in range(6) for c in range(3)} | {(i, 3): self.finish(i) for i in range(6)}

    def slot(self, i):
        kind, j = ORDER[i]
        return 0 if kind == TALL else j // 2

    def half(self, i):
        kind = ORDER[i][0]
        if i >= 3:
            pl.semaphore_wait(self.free.at[i - 3], sum(SIZES.values()) - len(SIZES) + 1)
        self.copies.start(
            (i, "half"), lambda: (self.halves[kind](), self.theirs[kind].at[self.slot(i)], self.me.device(core=1 - self.me.core))
        )

    def half_sent(self, i):
        self.copies.sent(lambda key: key == (i, "half"))

    def colour(self, i, c):
        kind, j = ORDER[i]
        slot = self.slot(i)
        if i in self.waiting:
            self.waiting.discard(i)
            self.copies.arrived((i, "half"))

        def last(colour, value):
            first, size = PART[kind][colour]
            if kind != TALL:
                self.sums[kind][j, 0, :, first : first + size] = value[:4]
                self.sums[kind][j, 1, :, first : first + size] = value[4:]
            else:
                self.sums[TALL][j, first : first + size, :] = value

        grads = (lambda: self.own[kind].at[slot]), (lambda: self.theirs[kind].at[slot])
        keep = self.kept[c] if i == 0 else None
        yield from reduce_colour(self.me, self.copies, i, kind, c, grads, lambda c, p: self.buffers[kind, (c, p)].at[0], last, keep)

    def finish(self, i):
        if i < 3:
            for d, n in SIZES.items():
                each(n - 1, lambda o, d=d: self.done(i, self.me.device(**{d: self.me.off(d, o + 1)})))
            self.done(i, self.me.device(core=1 - self.me.core))
        self.copies.sent(lambda key: key[0] == i)
        yield

    def done(self, i, device):
        pl.semaphore_signal(self.free.at[i], inc=1, device_id=device, device_id_type=MESH)

    def run(self, order):
        for i, c in zip(order[::2], order[1::2], strict=True):
            if c == "h":
                self.half(int(i))
            elif c == "s":
                self.half_sent(int(i))
            else:
                next(self.streams[int(i), int(c)], None)


def dot(a, b, ca=1, cb=0):
    return lax.dot_general(a, b, (((ca,), (cb,)), ((), ())), preferred_element_type=F32)


def rem(a, b):
    return a % b if isinstance(a, int) else lax.rem(a, b)


def at_tile(i, size):
    return pl.ds(pl.multiple_of(i * size, size), size)


def put_rows(ref, i, value):
    y, z, rows = ref.shape[1:4]
    for s in range(0, 256, 8):
        row = i * 256 + s
        group = lax.div(row, rows)
        ref[lax.div(group, y * z), rem(lax.div(group, z), y), rem(group, z), pl.ds(pl.multiple_of(rem(row, rows), 8), 8), :] = value[s : s + 8]


def put_all(ref, value):
    ref[...] = value.reshape(ref.shape)


def step_kernel(*refs):
    x_in, dy_in, w_gate, w_up, w_down = refs[:5]
    moments, outs, (wide_moments, tall_moments), rest = (refs[5:8], refs[8:11]), refs[11:13], refs[13:15], list(refs[15:])
    gate_kept, up_kept, hidden_kept, a0_kept, h1_kept = rest[:5]
    rest = rest[5:]
    take = lambda n: [rest.pop(0) for _ in range(n)]
    act, dy, turned, back, both, gates, ups = take(7)
    tile_g, tile_u, tile_d, rows_w, columns_w = take(5)
    wide_own, wide_theirs, tall_own, tall_half, tall_theirs = take(5)
    load, sem_g, sem_u, sem_d, sem_w, sem_c, sem_f, send, recv, free = take(10)
    buffers = {}
    for kind in KINDS:
        for k in reduce_buffers(kind):
            buffers[kind, k] = rest.pop(0)
    tall_kept = take(3)
    me = Me()

    def fetch(src, dst, sem):
        copy = pltpu.make_async_copy(src, dst, sem)
        copy.start()
        return copy

    class Stream:
        def __init__(self, tile, buffer, sem):
            self.tile, self.buffer, self.sem = tile, buffer, sem

        def copy(self, i):
            slot = rem(i, 2)
            return pltpu.make_async_copy(self.tile(i), self.buffer.at[slot], self.sem.at[slot])

    def stream(*streams, n):
        for s in streams:
            s.copy(0).start()

        def ahead(i):
            @pl.when(i + 1 < n)
            def _():
                for s in streams:
                    s.copy(i + 1).start()

            for s in streams:
                s.copy(i).wait()

        return ahead

    def columns(w, layer, buffer, sem):
        return Stream(lambda i: w.at[layer, :, at_tile(i, 256)], buffer, sem)

    loads = [fetch(x_in, back, load.at[0]), fetch(dy_in, dy, load.at[1])]
    zeroth = stream(columns(w_gate, 0, tile_g, sem_g), columns(w_up, 0, tile_u, sem_u), n=10)

    def half_columns(i, half):
        src = w_down.at[0, pl.ds(half * 1280, 1280), at_tile(i, 256)]
        return pltpu.make_async_copy(src, columns_w.at[half], sem_c.at[half])

    for half in (0, 1):
        half_columns(0, half).start()
    peers = me.arrive()
    own = by_kind(wide_own, tall_own)
    theirs = by_kind(wide_theirs, tall_theirs)
    halves = by_kind(lambda: wide_own.at[2], lambda: tall_half)
    reduce = Reduce(me, own, theirs, halves, buffers, by_kind(*outs), send, recv, free, tall_kept)

    def ticks(phase, i):
        orders = TICKS[phase]
        if any(orders):
            lax.switch(i, [functools.partial(reduce.run, order) for order in orders])

    def norm():
        @pl.loop(0, 8)
        def _(i):
            rows = at_tile(i, 128)
            h = back[rows, :].astype(F32)
            act[rows, :] = (h * lax.rsqrt(jnp.mean(h * h, -1, keepdims=True) + 1e-6)).astype(BF16)

    def turn(src, i):
        i = rem(i, 8)
        turned[:, at_tile(i, 128)] = src[at_tile(i, 128), :].T

    def silu_of(g):
        s = jax.nn.sigmoid(g)
        return g * s, s * (1 + g * (1 - s))

    def unit(i, silu, slope, hidden, d, dout):
        d = d.astype(BF16).astype(F32)
        both[1, :, at_tile(i, 256)] = (d * silu).astype(BF16)
        both[0, :, at_tile(i, 256)] = (d * slope).astype(BF16)
        for ref, core in ((tall_own.at[0], me.core), (tall_half, 1 - me.core)):
            put_rows(ref, i, dot(hidden, dout[:, at_tile(core, 512)]).astype(BF16))

    def wide_grads(phase):
        @pl.loop(0, 4)
        def _(k):
            which = lax.div(k, 2)
            mine = lax.rem(k + which, 2)
            core = mine * me.core + (1 - mine) * (1 - me.core)
            value = dot(turned[...], both[which, :, at_tile(core, 1280)]).astype(BF16)
            put_all(wide_own.at[lax.rem(2 - mine * (2 - which), 3)], value)
            ticks(phase, k)

    def kept(i, out):
        slot = rem(i, 2)
        pairs = (gates.at[slot], gate_kept.at[i]), (ups.at[slot], up_kept.at[i])
        return [pltpu.make_async_copy(*(p if out else p[::-1]), sem_f.at[n, slot]) for n, p in enumerate(pairs)]

    loads[0].wait()
    norm()
    keep = fetch(act, a0_kept, load.at[0])

    @pl.loop(0, 10)
    def _(i):
        zeroth(i)

        @pl.when(i >= 2)
        def _():
            for copy in kept(i - 2, True):
                copy.wait()

        slot = rem(i, 2)
        g, u = dot(act[...], tile_g[slot]), dot(act[...], tile_u[slot])
        silu, slope = silu_of(g)
        gates[slot] = silu
        ups[slot] = u * slope
        both[0, :, at_tile(i, 256)] = (silu * u).astype(BF16)
        for copy in kept(i, True):
            copy.start()

    keep_hidden = pltpu.make_async_copy(both.at[0], hidden_kept, load.at[2])
    first = stream(
        columns(w_gate, 1, tile_g, sem_g),
        columns(w_up, 1, tile_u, sem_u),
        Stream(lambda i: w_down.at[1, at_tile(i, 256), :], tile_d, sem_d),
        n=10,
    )

    @pl.loop(0, 4)
    def _(i):
        @pl.when(i == 1)
        def _():
            keep_hidden.start()

        part = 0.0
        for half in (0, 1):
            half_columns(i, half).wait()
            part += dot(both[0, :, half * 1280 : half * 1280 + 1280], columns_w[half])

            @pl.when(i < 3)
            def _():
                half_columns(i + 1, half).start()

        part = part.astype(BF16).astype(F32)
        back[:, at_tile(i, 256)] = (back[:, at_tile(i, 256)].astype(F32) + part).astype(BF16)

    keep.wait()
    keep = fetch(back, h1_kept, load.at[0])
    norm()

    loads[1].wait()
    keep_hidden.wait()

    @pl.loop(0, 10)
    def _(i):
        first(i)
        turn(act, i)
        slot = rem(i, 2)
        silu, slope = silu_of(dot(act[...], tile_g[slot]))
        u = dot(act[...], tile_u[slot])
        unit(i, silu, u * slope, (silu * u).astype(BF16).T, dot(dy[...], tile_d[slot], 1, 1), dy)

    me.arrived(peers)
    for n, three in enumerate(moments):
        for which in (0, 1):

            def make(n=n, which=which, three=three):
                theirs = pl.ds(pl.multiple_of((1 - me.core) * 1280, 1280), 1280)
                return three[which].at[:, :, theirs], wide_moments.at[n, pl.ds(2 * which, 2)], me.device(core=1 - me.core)

            reduce.copies.start(("moments", n, which), make)
        for o in range(3):

            def make(n=n, o=o, three=three):
                z, core = me.others()[o]
                return three[2].at[:, :, quarter(z, core)], tall_moments.at[n, me.quarter()], me.device(core=core, z=z)

            reduce.copies.start(("moments", n, 2 + o), make)
    reduce.run(TICKS["first"][0])
    wide_grads("wide1")

    keep.wait()
    for i in (8, 9):
        for copy in kept(i, True):
            copy.wait()
    load_h = fetch(h1_kept, turned, load.at[0])

    def weight_rows(k, w):
        slot = rem(k, 2)
        rows = at_tile(k // 2 if isinstance(k, int) else lax.div(k, 2), 256)
        return pltpu.make_async_copy(w.at[1, rows, :], rows_w.at[slot], sem_w.at[slot])

    weight_rows(0, w_gate).start()

    @pl.loop(0, 8)
    def _(k):
        n, which = lax.div(k, 2), lax.rem(k, 2)

        @pl.when(which == 0)
        def _():
            weight_rows(k + 1, w_up).start()

        @pl.when((which == 1) & (k < 7))
        def _():
            weight_rows(k + 1, w_gate).start()

        weight_rows(k, w_gate).wait()
        part = dot(both[which], rows_w[which], 1, 1).astype(BF16).astype(F32)
        before = back[:, at_tile(n, 256)].astype(F32)
        back[:, at_tile(n, 256)] = (jnp.where(which == 0, 0.0, before) + part).astype(BF16)
        ticks("back", k)

    load_h.wait()

    @pl.loop(0, 8)
    def _(i):
        rows = at_tile(i, 128)
        h, d = turned[rows, :].astype(F32), back[rows, :].astype(F32)
        scale = lax.rsqrt(jnp.mean(h * h, -1, keepdims=True) + 1e-6)
        along = jnp.sum(d * h, -1, keepdims=True)
        d = (d * scale - h * (scale * scale * scale * along * (1 / 1024))).astype(BF16)
        act[rows, :] = (dy[rows, :].astype(F32) + d.astype(F32)).astype(BF16)

    load_a = fetch(a0_kept, back, load.at[1])
    second = stream(
        Stream(lambda i: w_down.at[0, at_tile(i, 256), :], tile_d, sem_d),
        Stream(lambda i: hidden_kept.at[:, at_tile(i, 256)], tile_g, sem_g),
        n=10,
    )
    for copy in kept(0, False):
        copy.start()
    load_a.wait()

    @pl.loop(0, 10)
    def _(i):
        @pl.when(i < 9)
        def _():
            for copy in kept(i + 1, False):
                copy.start()

        second(i)
        turn(back, i)
        for copy in kept(i, False):
            copy.wait()
        slot = rem(i, 2)
        unit(i, gates[slot], ups[slot], tile_g[slot].T, dot(act[...], tile_d[slot], 1, 1), act)
        ticks("units", i)

    reduce.run(TICKS["last"][0])
    wide_grads("wide0")
    reduce.run(TICKS["tail"][0])
    for stream_ in reduce.streams.values():
        assert next(stream_, 0) == 0, "not done"
    for n in range(2):
        for o in range(5):
            reduce.copies.arrived(("moments", n, o))
    reduce.copies.sent()


def run(streams, order):
    for i, c in zip(order[::2], order[1::2], strict=True):
        next(streams[int(i), int(c)], None)
    for stream in streams.values():
        assert next(stream, 0) == 0, "not done"


def full_shape(kind):
    return dims(kind, ("x", "y", "z")) + (ROWS[kind], HALF[kind])


def summed(x, dy, w_gate, w_up, w_down, m, v):
    square = pltpu.VMEM((1024, 1024), BF16)
    scratch = [square] * 4 + [pltpu.VMEM((2, 1024, 2560), BF16)]
    scratch += [pltpu.VMEM((2, 1024, 256), F32)] * 2
    scratch += [pltpu.VMEM((2, 1024, 256), BF16)] * 2 + [pltpu.VMEM((2, 256, 1024), BF16), pltpu.VMEM((2, 256, 2560), BF16)]
    scratch += [
        pltpu.VMEM((2, 1280, 256), BF16),
        pltpu.VMEM((3, *full_shape(GATE)), BF16),
        pltpu.VMEM((2, *full_shape(GATE)), BF16),
        pltpu.VMEM((1, *full_shape(TALL)), BF16),
        pltpu.VMEM(full_shape(TALL), BF16),
        pltpu.VMEM((1, *full_shape(TALL)), BF16),
        pltpu.SemaphoreType.DMA((3,)),
        *[pltpu.SemaphoreType.DMA((2,))] * 5,
        pltpu.SemaphoreType.DMA((2, 2)),
        pltpu.SemaphoreType.DMA((256,)),
        pltpu.SemaphoreType.DMA((256,)),
        pltpu.SemaphoreType.REGULAR((3,)),
    ]
    for kind in KINDS:
        scratch += [pltpu.VMEM((1, *shape), BF16) for shape in reduce_buffers(kind).values()]
    scratch += [pltpu.VMEM(block(TALL, c, [d for d in "xyz" if d != COLOURS[c][0][0]]), BF16) for c in range(3)]
    kept = [jax.ShapeDtypeStruct((10, 1024, 256), F32)] * 2 + [jax.ShapeDtypeStruct((1024, t), BF16) for t in (2560, 1024, 1024)]
    return pl.pallas_call(
        step_kernel,
        out_shape=(
            jax.ShapeDtypeStruct((4, 2, 4, 1280), F32),
            jax.ShapeDtypeStruct((2, 40, 256), F32),
            jax.ShapeDtypeStruct((2, 4, 4, 1280), F32),
            jax.ShapeDtypeStruct((2, 4, 10, 2, 256), F32),
            *kept,
        ),
        in_specs=[pl.BlockSpec(memory_space=pl.ANY)] * 11,
        out_specs=(*[pl.BlockSpec(memory_space=pltpu.VMEM)] * 2, *[pl.BlockSpec(memory_space=pl.ANY)] * 7),
        scratch_shapes=scratch,
        compiler_params=pltpu.CompilerParams(
            collective_id=0, has_side_effects=True, vmem_limit_bytes=VMEM_LIMIT
        ),
        name="step",
    )(x, dy, w_gate, w_up, w_down, *m, *v)[:4]


def gather_colour(me, copies, key, kind, colour, ref):
    base = me.core * HALF[kind]
    fixed = dict(me.at)

    def part(at):
        return view(ref, kind, ("x", "y", "z"), at, colour, base, parts=GATHER_PART)

    phases = COLOURS[colour][::-1]
    for phase, (d, how) in enumerate(phases):
        n, lastly = SIZES[d], phase == len(phases) - 1
        rest = {e: v for e, v in fixed.items() if e != d}
        here = part(fixed)

        def across(name, at):
            if lastly:
                copies.start((key, colour, "across", name), lambda: (part(at), part(at), me.device(core=1 - me.core)))

        if how == RING:
            long, short = lengths(n)
            ways = ((me.sign, long, "l"), (-me.sign, short, "s"))
            for s in range(long):
                for sign, length, name in ways:
                    if s >= length:
                        continue
                    at = {**rest, d: me.off(d, -sign * s)}
                    if s:
                        copies.arrived((key, colour, phase, name, s - 1))
                    copies.start(
                        (key, colour, phase, name, s),
                        lambda at=at, d=d, sign=sign: (part(at), part(at), me.device(**{d: me.off(d, sign)})),
                    )
                    if s:
                        across((name, s - 1), at)
                if s == 0:
                    across("own", fixed)
                yield
            for sign, length, name in ways:
                if length:
                    copies.arrived((key, colour, phase, name, length - 1))
                    across((name, length - 1), {**rest, d: me.off(d, -sign * length)})
        else:
            copies.start_all(
                (key, colour, phase), n - 1, lambda i, d=d, here=here: (here, here, me.device(**{d: me.off(d, i + 1)}))
            )
            yield
            copies.arrived((key, colour, phase))
        fixed = rest
    yield
    names = ["own"]
    d, how = phases[-1]
    long, short = lengths(SIZES[d])
    names += [("l", s) for s in range(long)] + [("s", s) for s in range(short)]
    for name in names:
        copies.arrived((key, colour, "across", name))


def gather_kernel(*refs):
    sums_in, moments, given, weights = refs[:2], (refs[2:5], refs[5:8]), refs[8:10], refs[10:13]
    outs, new, rest = refs[13:19], (refs[19:22], refs[22:25]), refs[25:]
    sums, held, rows, after = by_kind(*rest[:2]), by_kind(*rest[2:4]), by_kind(*rest[4:6]), by_kind(*rest[6:8])
    tall_got, forty, load, send, recv = rest[8:13]
    me = Me()
    copies = Copies(send, recv)
    half = pl.ds(pl.multiple_of(me.core * 1280, 1280), 1280)
    mine = me.quarter()

    def which(i):
        kind, j = ORDER[i]
        return (2, j) if kind == TALL else (j // 2, j % 2)

    peers = me.arrive()
    loads = []

    def take(src, dst):
        loads.append(pltpu.make_async_copy(src, dst, load.at[len(loads)]))
        loads[-1].start()

    for src, dst in zip(sums_in, rest[:2], strict=True):
        take(src, dst)
    for n in range(2):
        for w in (0, 1):
            take(moments[n][w].at[:, :, half], held[GATE].at[n, pl.ds(2 * w, 2), me.core])
        take(given[0].at[n], held[GATE].at[n, :, 1 - me.core])
        take(moments[n][2].at[:, :, quarter(me.at["z"], me.core)], held[TALL].at[n, mine])
        for z, core in me.others():
            q = 2 * lax.rem(z, 2) + core
            take(given[1].at[n, q], held[TALL].at[n, q])
    for i, (kind, j) in enumerate(ORDER):
        n, layer = which(i)
        z = me.at["z"] if kind != TALL else lax.div(me.at["z"], 2)
        first = ((me.at["x"] * SIZES["y"] + me.at["y"]) * dims(kind, "z")[0] + z) * ROWS[kind]
        columns = half if kind != TALL else quarter(me.at["z"], me.core)
        take(weights[n].at[layer, pl.ds(pl.multiple_of(first, 8), ROWS[kind]), columns], rows[kind].at[j])
    for copy in loads:
        copy.wait()
    me.arrived(peers)

    def begin(i):
        kind, j = ORDER[i]
        w, layer = which(i)
        here = view(outs[i], kind, ("x", "y", "z"), me.at, None, me.core * HALF[kind])
        many = 2 if kind != TALL else 4
        size = ROWS[kind] // many
        old = rows[kind][j].astype(F32)
        parts = []
        for q in range(many):
            part = slice(q * size, q * size + size)
            if kind != TALL:
                m, v, g = held[kind][0, j, q], held[kind][1, j, q], sums[kind][j, q]
            else:
                m, v, g = held[TALL][0, q, :, layer], held[TALL][1, q, :, layer], sums[TALL][j, part]
            value, m, v = adamw(old[part], m, v, g)
            for n, t in enumerate((m, v)):
                after[kind][n, j, q] = t
            parts.append(value.astype(F32))
        if kind != TALL:
            here[...] = jnp.concatenate(parts, axis=0).astype(BF16)
        else:
            for q in range(4):
                forty[q * size : q * size + size, :] = parts[q]
            here[...] = forty[...].astype(BF16)
        for n in range(2):
            if kind != TALL:
                copies.start(
                    (i, "moments", n),
                    lambda n=n: (after[kind].at[n, j, 1 - me.core], new[n][w].at[layer, :, half], me.device(core=1 - me.core)),
                )
                new[n][w][layer, :, half] = jnp.where(me.core == 0, after[kind][n, j, 0], after[kind][n, j, 1])
            else:
                for o, (z, core) in enumerate(me.others()):
                    q = 2 * lax.rem(z, 2) + core
                    copies.start(
                        (i, "moments", n, o),
                        lambda n=n, q=q, z=z, core=core: (after[TALL].at[n, j, q], tall_got.at[n, j, mine], me.device(core=core, z=z)),
                    )

    def colour(i, c):
        if i in waiting:
            waiting.discard(i)
            begin(i)
        yield from gather_colour(me, copies, i, ORDER[i][0], c, outs[i])

    waiting = set(range(6))
    run({(i, c): colour(i, c) for i in range(6) for c in range(3)}, GATHER_ORDER)
    for i, (kind, j) in enumerate(ORDER):
        for n in range(2):
            if kind != TALL:
                copies.arrived((i, "moments", n))
            else:
                for o in range(3):
                    copies.arrived((i, "moments", n, o))
                for q in range(4):
                    columns = pl.ds((q % 2 * 2 + q // 2) * 256, 256)
                    new[n][2][:, j, columns] = jnp.where(q == mine, after[TALL][n, j, q], tall_got[n, j, q])
    copies.sent()


def all_gather(wide, tall, wide_moments, tall_moments, m, v, weights):
    moments = [pltpu.VMEM(t.shape, F32) for t in m]
    scratch = [
        pltpu.VMEM(wide.shape, F32),
        pltpu.VMEM(tall.shape, F32),
        pltpu.VMEM((2, 4, 2, 4, 1280), F32),
        pltpu.VMEM(tall_moments.shape, F32),
        pltpu.VMEM((4, ROWS[GATE], 1280), BF16),
        pltpu.VMEM((2, ROWS[TALL], 256), BF16),
        pltpu.VMEM((2, 4, 2, 4, 1280), F32),
        pltpu.VMEM((2, 2, 4, 10, 256), F32),
        pltpu.VMEM((2, 2, 4, 10, 256), F32),
        pltpu.VMEM((40, 256), F32),
        pltpu.SemaphoreType.DMA((24,)),
        pltpu.SemaphoreType.DMA((384,)),
        pltpu.SemaphoreType.DMA((384,)),
    ]
    matrices = [pltpu.VMEM((*dims(kind, ("x", "y", "z")), ROWS[kind], 2 * HALF[kind]), BF16) for kind, _ in ORDER]
    return pl.pallas_call(
        gather_kernel,
        out_shape=(*matrices, *moments, *moments),
        in_specs=[pl.BlockSpec(memory_space=pl.ANY)] * 13,
        out_specs=(pl.BlockSpec(memory_space=pltpu.VMEM),) * 12,
        scratch_shapes=scratch,
        compiler_params=pltpu.CompilerParams(collective_id=1, has_side_effects=True, vmem_limit_bytes=28 * 1024 * 1024),
        name="all_gather",
    )(wide, tall, *m, *v, wide_moments, tall_moments, *weights)


def spill_kernel(*refs):
    ins, moments, outs, sem = refs[:6], refs[6:12], refs[12:21], refs[21]
    copies = []
    for i, (kind, j) in enumerate(ORDER):
        which, layer = (2, j) if kind == TALL else (j // 2, j % 2)
        copies.append(pltpu.make_async_copy(ins[i], outs[which].at[layer], sem.at[i]))
    for i in range(6):
        copies.append(pltpu.make_async_copy(moments[i], outs[3 + i], sem.at[6 + i]))
    for copy in copies:
        copy.start()
    for copy in copies:
        copy.wait()


def spill(new):
    wide, tall = ((2, *dims(kind, ("x", "y", "z")), ROWS[kind], 2 * HALF[kind]) for kind in (GATE, TALL))
    return pl.pallas_call(
        spill_kernel,
        out_shape=(*(jax.ShapeDtypeStruct(shape, BF16) for shape in (wide, wide, tall)), *(jax.ShapeDtypeStruct(t.shape, F32) for t in new[6:])),
        in_specs=[pl.BlockSpec(memory_space=pltpu.VMEM)] * 12,
        out_specs=(pl.BlockSpec(memory_space=pl.ANY),) * 9,
        scratch_shapes=[pltpu.SemaphoreType.DMA((12,))],
        compiler_params=pltpu.CompilerParams(vmem_limit_bytes=1024 * 1024),
        name="spill",
    )(*new)


def adamw(w, m, v, g):
    m = 0.9 * m + 0.1 * g
    v = 0.95 * v + 0.05 * g * g
    step = m * lax.rsqrt(v + 1e-8) + 0.1 * w
    return (w - 0.02 * step).astype(BF16), m, v


def solution(mesh):
    def step(x, dy, *arrays):
        weights, m, v = (arrays[i : i + 3] for i in (0, 3, 6))
        m, v = ((*t[:2], t[2].transpose(1, 0, 2)) for t in (m, v))
        new = spill(all_gather(*summed(x[0], dy[0], *weights, m, v), m, v, weights))
        m, v = ((*t[:2], t[2].transpose(1, 0, 2)) for t in (new[3:6], new[6:9]))
        return (*(w.reshape(2, -1, w.shape[-1]) for w in new[:3]), *m, *v)

    batch, whole, rows = P(("rep", "dp")), P(), P(None, "dp")
    return jax.shard_map(
        step,
        mesh=mesh,
        in_specs=(batch, batch, *(whole,) * 3, *(rows,) * 6),
        out_specs=(*(P("rep"),) * 3, *(P("rep", "dp"),) * 6),
        check_vma=False,
    )
```
